32 devices in a mesh: gx: 4 (over z), gy: 4 (over x, core), gz: 2 (over y).
Axes of the slice: x: 2, y: 2, z: 4, core: 2. Of those that a mesh axis runs over, the one named last changes fastest.
Arguments:
- x_a: bfloat16 [32, 8, 64, 256], P(None, 'gx', 'gy', 'gz'), may hold values from -12 to 12
- x_b: bfloat16 [32, 8, 64, 256], P(None, 'gx', 'gy', 'gz'), may hold values from -12 to 12
- w_first: bfloat16 [3, 3, 3, 32, 32], replicated, may hold values from -0.21875 to 0.21875
- w_second: bfloat16 [3, 3, 3, 32, 32], replicated, may hold values from -0.21875 to 0.21875
- gain_first: float32 [32], replicated, may hold values from 0.1 to 1.9
- bias_first: float32 [32], replicated, may hold values from -2 to 2
- gain_second: float32 [32], replicated, may hold values from 0.1 to 1.9
- bias_second: float32 [32], replicated, may hold values from -2 to 2
- grad_out: bfloat16 [32, 8, 64, 256], P(None, 'gx', 'gy', 'gz'), may hold values from -6 to 6
Outputs:
- y_a: bfloat16 [32, 8, 64, 256], P(None, 'gx', 'gy', 'gz')
- dx_b: bfloat16 [32, 8, 64, 256], P(None, 'gx', 'gy', 'gz')
- grad_w_first: float32 [3, 3, 3, 32, 32], replicated
- grad_w_second: float32 [3, 3, 3, 32, 32], replicated
- grad_norm: float32 [4, 32], replicated
The draws below stay inside these ranges and needn't reach their ends.
All inputs are finite; a program needn't handle non-finite values.
Results may differ from the reference program's by a relative error of at most 0.0063.
Values may be sent and summed in bfloat16 or wider, within the bound.
No kernel may reach another device: no remote copies, remote signals or barrier semaphores. Data moves between devices by JAX's collectives and lax.ppermute only.
A program may use at most 128 MiB of HBM per device.

```python
import math
import jax
import jax.numpy as jnp
from jax import lax

C = 32
NX = 8
NY = 64
NZ = 256
VOXELS = 131072


def draw_volume(key, salt):
    folded = jax.random.fold_in(key, salt)
    depth = jnp.arange(NX, dtype=jnp.float32) / max(NX - 1, 1)
    base = jnp.clip(jax.random.normal(folded, (C, NX, NY, NZ), jnp.float32), -4.0, 4.0)
    ramp = 1.0 + 2.0 * depth
    value = base * ramp[None, :, None, None]
    return value.astype(jnp.bfloat16)


def draw_x_a(key, part):
    return draw_volume(key, 11)


def draw_x_b(key, part):
    return draw_volume(key, 23)


def block_levels(key, extent, cuts, smallest, high):
    level = 1.0
    for axis_at, blocks in cuts:
        draws = jax.random.uniform(jax.random.fold_in(jax.random.fold_in(key, 6), axis_at), (blocks,), jnp.float32, smallest / len(cuts), high / len(cuts))
        level = level * jnp.repeat(jnp.exp(draws), extent[axis_at] // blocks).reshape((-1,) + (1,) * (len(extent) - 1 - axis_at))
    return level


def bell_draw(own_key, extent, scale, bound, cuts=(), kind=jnp.bfloat16):
    result = jax.random.normal(own_key, extent, jnp.float32) * scale
    if len(cuts) > 0:
        result = block_levels(own_key, extent, cuts, -0.22, 0.18) * result
    return jnp.clip(result, min=-bound, max=bound).astype(kind)


def setup_inputs(seed: int = 0) -> dict:
    arg_keys = jax.random.split(jax.random.key(seed), 10)
    return {
        "x_a": draw_x_a(jax.random.fold_in(arg_keys[9], 71), 0),
        "x_b": draw_x_b(jax.random.fold_in(arg_keys[9], 71), 0),
        "w_first": bell_draw(arg_keys[2], (3, 3, 3, C, C), (27 * C) ** -0.5, 0.21875),
        "w_second": bell_draw(arg_keys[3], (3, 3, 3, C, C), (27 * C) ** -0.5, 0.21875),
        "gain_first": jnp.clip(1.0 + 0.18 * jax.random.normal(arg_keys[4], (C,), jnp.float32), 0.1, 1.9),
        "bias_first": bell_draw(arg_keys[5], (C,), 0.5, 2.0, (), jnp.float32),
        "gain_second": jnp.clip(1.0 + 0.18 * jax.random.normal(arg_keys[6], (C,), jnp.float32), 0.1, 1.9),
        "bias_second": bell_draw(arg_keys[7], (C,), 0.5, 2.0, (), jnp.float32),
        "grad_out": bell_draw(arg_keys[8], (C, NX, NY, NZ), 1.0, 6.0, ((1, 4), (2, 4), (3, 2))),
    }


EPSILON = 1e-05

def spread(values):
    return values[:, None, None, None]

def silu_slope(value):
    sigma = jax.nn.sigmoid(value)
    return sigma * (1.0 + value * (1.0 - sigma))

def pad_volume(volume):
    return jnp.pad(volume, ((0, 0), (1, 1), (1, 1), (1, 1)))

def convolve(padded, weight):
    in_chan = padded.shape[0]
    out_chan = weight.shape[3]
    span_x = padded.shape[1] - 2
    span_y = padded.shape[2] - 2
    span_z = padded.shape[3] - 2
    total = jnp.zeros((out_chan, span_x * span_y * span_z), jnp.float32)
    for shift_x in range(3):
        for shift_y in range(3):
            pieces = [padded[:, shift_x:shift_x + span_x, shift_y:shift_y + span_y, shift_z:shift_z + span_z] for shift_z in range(3)]
            stacked = jnp.concatenate(pieces, axis=0).reshape(3 * in_chan, -1)
            matrix = weight[shift_x, shift_y].transpose(1, 0, 2).reshape(out_chan, 3 * in_chan)
            total = total + jnp.dot(matrix, stacked, preferred_element_type=jnp.float32)
    return total.reshape(out_chan, span_x, span_y, span_z)

def kernel_grad(padded, upstream):
    in_chan = padded.shape[0]
    out_chan = upstream.shape[0]
    span_x, span_y, span_z = (upstream.shape[1], upstream.shape[2], upstream.shape[3])
    flat = upstream.reshape(out_chan, -1)
    rows = []
    for shift_x in range(3):
        for shift_y in range(3):
            pieces = [padded[:, shift_x:shift_x + span_x, shift_y:shift_y + span_y, shift_z:shift_z + span_z] for shift_z in range(3)]
            stacked = jnp.concatenate(pieces, axis=0).reshape(3 * in_chan, -1)
            product = lax.dot_general(flat, stacked, (((1,), (1,)), ((), ())), preferred_element_type=jnp.float32)
            rows.append(product.reshape(out_chan, 3, in_chan).transpose(1, 0, 2))
    return jnp.stack(rows).reshape(3, 3, 3, out_chan, in_chan)

def flipped(weight):
    return jnp.flip(weight, (0, 1, 2)).transpose(0, 1, 2, 4, 3)

def forward_layer(features, weight, gain, bias):
    conv_out = convolve(pad_volume(features), weight)
    means = lax.optimization_barrier(jnp.sum(conv_out, axis=(1, 2, 3))) / VOXELS
    variance = lax.optimization_barrier(jnp.sum(jnp.square(conv_out - spread(means)), axis=(1, 2, 3))) / VOXELS
    scales = lax.rsqrt(variance + EPSILON)
    normed = (conv_out - spread(means)) * spread(scales)
    preact = spread(gain) * normed + spread(bias)
    output = (preact * jax.nn.sigmoid(preact)).astype(jnp.bfloat16)
    return (output, preact, normed, scales)

def backward_layer(upstream, preact, normed, scales, gain):
    slope = upstream * silu_slope(preact)
    sum_d = lax.optimization_barrier(jnp.sum(slope, axis=(1, 2, 3)))
    sum_dx = lax.optimization_barrier(jnp.sum(slope * normed, axis=(1, 2, 3)))
    delta = spread(gain * scales) * (slope - spread(sum_d / VOXELS) - normed * spread(sum_dx / VOXELS))
    return (delta.astype(jnp.bfloat16), sum_d, sum_dx)

def reference(x_a, x_b, w_first, w_second, gain_first, bias_first, gain_second, bias_second, grad_out):
    hidden_a = forward_layer(x_a, w_first, gain_first, bias_first)[0]
    y_a = forward_layer(hidden_a, w_second, gain_second, bias_second)[0]
    hidden_b, pre_one, norm_one, scale_one = forward_layer(x_b, w_first, gain_first, bias_first)
    unused, pre_two, norm_two, scale_two = forward_layer(hidden_b, w_second, gain_second, bias_second)
    factor = 1.0 / math.sqrt(VOXELS)
    delta_two, sum_d2, sum_x2 = backward_layer(grad_out.astype(jnp.float32), pre_two, norm_two, scale_two, gain_second)
    grad_w_second = kernel_grad(pad_volume(hidden_b), delta_two) * factor
    upstream_one = convolve(pad_volume(delta_two), flipped(w_second))
    delta_one, sum_d1, sum_x1 = backward_layer(upstream_one, pre_one, norm_one, scale_one, gain_first)
    grad_w_first = kernel_grad(pad_volume(x_b), delta_one) * factor
    dx_b = convolve(pad_volume(delta_one), flipped(w_first)).astype(jnp.bfloat16)
    grad_norm = jnp.stack([sum_x1, sum_d1, sum_x2, sum_d2]) * factor
    return (y_a, dx_b, grad_w_first, grad_w_second, grad_norm)
```

```python
import math

import jax
import jax.numpy as jnp
from jax import lax
from jax.experimental import pallas as pl
from jax.experimental.pallas import tpu as pltpu
from jax.sharding import PartitionSpec as P

EPSILON = 1e-05
AXES = ("gx", "gy", "gz")
LANES = 128
BF = jnp.bfloat16
F32 = jnp.float32
VM = pl.BlockSpec(memory_space=pltpu.VMEM)
SM = pl.BlockSpec(memory_space=pltpu.SMEM)


def kernel_call(body, name, out_shape, args, scratch=(), smem=0):
    return pl.pallas_call(
        body,
        out_shape=out_shape,
        in_specs=[SM] * smem + [VM] * (len(args) - smem),
        out_specs=[VM] * len(out_shape),
        scratch_shapes=list(scratch),
        name=name,
    )(*args)


def shape(dims, kind):
    return jax.ShapeDtypeStruct(dims, kind)


def shift_pair(low_source, high_source, axis):
    count = lax.axis_size(axis)
    if count == 2:
        at = lax.axis_index(axis)
        got = lax.ppermute(jnp.where(at == 0, low_source, high_source), axis, [(0, 1), (1, 0)])
        zero = jnp.zeros_like(got)
        return jnp.where(at == 1, got, zero), jnp.where(at == 0, got, zero)
    forward = [(i, i + 1) for i in range(count - 1)]
    backward = [(t, s) for s, t in forward]
    return lax.ppermute(low_source, axis, forward), lax.ppermute(high_source, axis, backward)


def extended(block, sides):
    for axis, dim, width in sides:
        size = block.shape[dim]
        low, high = shift_pair(
            lax.slice_in_dim(block, size - width, size, axis=dim),
            lax.slice_in_dim(block, 0, width, axis=dim),
            axis,
        )
        block = jnp.concatenate([low, block, high], axis=dim)
    return block


def exchange(spread_rows):
    return lax.all_to_all(spread_rows, AXES, 0, 0)


def order_matrix(chan, rows):
    size = chan * rows
    k = lax.broadcasted_iota(jnp.int32, (size, size), 0)
    n = lax.broadcasted_iota(jnp.int32, (size, size), 1)
    return (n == (k % rows) * chan + k // rows).astype(BF)


def band_conv(src, weight, group, planes, pitch):
    size = planes * pitch
    at = pl.multiple_of(group * LANES, LANES)
    parts = [src[pl.ds(d * pitch, size), pl.ds(at, 2 * LANES)] for d in range(3)]
    out = jnp.dot(jnp.concatenate(parts, axis=1), weight[...], preferred_element_type=F32)
    return (
        out[:, :LANES]
        + pltpu.roll(out[:, LANES : 2 * LANES], size - 1, 0)
        + pltpu.roll(out[:, 2 * LANES :], size - 2, 0)
    )


def tap_products(d_rows, h_ref, start, group, pitch, acc):
    size = d_rows.shape[0]
    three = jnp.concatenate([d_rows, pltpu.roll(d_rows, 1, 0), pltpu.roll(d_rows, 2, 0)], axis=1)
    left = three.T.astype(BF)
    at = pl.multiple_of(group * LANES, LANES)
    for d in range(3):
        right = h_ref[pl.ds(start + d * pitch, size), pl.ds(at, 2 * LANES)]
        acc[d] = acc[d] + jnp.dot(left, right, preferred_element_type=F32)


def fold_taps(acc, chan):
    rows = []
    for d in range(3):
        for t in range(3):
            base = t * LANES
            rows.append(
                sum(
                    acc[d, base + j * chan : base + (j + 1) * chan, j * chan : (j + 3) * chan]
                    for j in range(LANES // chan)
                )
            )
    return jnp.concatenate(rows, axis=0)


def fold_lanes(value, chan):
    step = chan
    while step < LANES:
        value = value + pltpu.roll(value, step, 1)
        step *= 2
    return value


def gathered(ref, row, chan):
    return fold_lanes(jnp.sum(ref[:, row, :], axis=0, keepdims=True), chan)


def sigmoid(value):
    return 0.5 + 0.5 * jnp.tanh(0.5 * value)


def body_maker(mesh):
    def body(x_a, x_b, w_first, w_second, gain_first, bias_first, gain_second, bias_second, grad_out):
        chan, span_x, span_y, span_z = x_a.shape
        world = lax.axis_size("gx") * lax.axis_size("gy") * lax.axis_size("gz")
        voxels = float(span_x * span_y * span_z * world)
        factor = 1.0 / math.sqrt(voxels)
        per = LANES // chan
        line = span_y * chan
        pitch = -(-(span_z + 4) // 16) * 16
        inner_groups = span_y // per
        outer_groups = -(-(span_y + 2) // per)
        wide = (outer_groups + 1) * LANES
        mid = outer_groups * LANES
        po, pi = span_x + 2, span_x
        so, si = po * pitch, pi * pitch

        def band(weight):
            turned = weight.transpose(0, 1, 4, 2, 3)
            parts = [
                jnp.pad(turned, ((0, 0), (j, 2 * per - 3 - j), (0, 0), (0, 0), (0, 0)))
                for j in range(per)
            ]
            return jnp.stack(parts, axis=4).reshape(3 * 2 * LANES, 3 * LANES)

        def flipped(weight):
            return jnp.flip(weight, (0, 1, 2)).transpose(0, 1, 2, 4, 3)

        band_one, band_two = band(w_first), band(w_second)
        back_one, back_two = band(flipped(w_first)), band(flipped(w_second))
        params = jnp.stack(
            [jnp.tile(v, per) for v in (gain_first, bias_first, gain_second, bias_second)]
        )

        def limits(axis, size):
            at, count = lax.axis_index(axis), lax.axis_size(axis)
            return [jnp.where(at == 0, 1, 0), jnp.where(at == count - 1, size + 1, size + 2)]

        bounds = jnp.stack(
            limits("gx", span_x) + limits("gy", span_y) + limits("gz", span_z)
        ).astype(jnp.int32)

        def inside(bound, group):
            row = lax.broadcasted_iota(jnp.int32, (so, LANES), 0)
            lane = lax.broadcasted_iota(jnp.int32, (so, LANES), 1) + group * LANES
            plane = row // pitch
            z = row - plane * pitch
            y = lane // chan
            ok = (plane >= bound[0]) & (plane < bound[1]) & (y >= bound[2]) & (y < bound[3])
            return ok & (z >= bound[4]) & (z < bound[5])

        def own(group):
            row = lax.broadcasted_iota(jnp.int32, (si, LANES), 0)
            lane = lax.broadcasted_iota(jnp.int32, (si, LANES), 1) + group * LANES
            z = row % pitch
            return (z >= 1) & (z <= span_z) & (lane >= chan) & (lane < chan + line)

        def own_rows():
            row = lax.broadcasted_iota(jnp.int32, (si, LANES), 0)
            return row % pitch < span_z

        def turn_in(a_ref, b_ref, g_ref, v_ref, o_ref):
            order = order_matrix(chan, span_y)
            for at, ref in enumerate((a_ref, b_ref)):
                for x in range(span_x):
                    block = ref[:, x].reshape(chan * span_y, span_z)
                    v_ref[at, x] = lax.dot_general(
                        block, order, (((0,), (0,)), ((), ())), preferred_element_type=F32
                    ).astype(BF)
            for x in range(span_x):
                block = g_ref[:, x].reshape(chan * span_y, span_z)
                o_ref[x * pitch : x * pitch + span_z, :] = lax.dot_general(
                    block, order, (((0,), (0,)), ((), ())), preferred_element_type=F32
                ).astype(BF)
                o_ref[x * pitch + span_z : (x + 1) * pitch, :] = jnp.zeros(
                    (pitch - span_z, line), BF
                )

        vols, cot = kernel_call(
            turn_in,
            "turn_in",
            [shape((2, span_x, span_z, line), BF), shape((si, line), BF)],
            [x_a, x_b, grad_out],
        )

        def two_wide(block):
            block = extended(block, (("gz", 2, 2), ("gy", 3, 2 * chan), ("gx", 1, 2)))
            fill = (0, pitch - block.shape[2]), (0, wide - block.shape[3])
            block = jnp.pad(block, ((0, 0), (0, 0)) + fill)
            return block.reshape(block.shape[0], (span_x + 4) * pitch, wide)

        padded = two_wide(vols)

        def first_conv(x_ref, w_ref, c_ref, st_ref):
            rows = []
            for v in range(2):

                def step(g, sums):
                    out = band_conv(x_ref.at[v], w_ref, g, po, pitch)
                    c_ref[v, :, pl.ds(pl.multiple_of(g * LANES, LANES), LANES)] = out
                    mine = jnp.where(own(g), out[pitch : pitch + si], 0.0)
                    return (
                        sums[0] + jnp.sum(mine, axis=0, keepdims=True),
                        sums[1] + jnp.sum(mine * mine, axis=0, keepdims=True),
                    )

                zero = jnp.zeros((1, LANES), F32)
                rows += list(lax.fori_loop(0, outer_groups, step, (zero, zero)))
            rows.append(jnp.zeros((4, LANES), F32))
            st_ref[...] = jnp.broadcast_to(jnp.concatenate(rows, axis=0)[None], st_ref.shape)

        stat_shape = shape((world, 8, LANES), F32)
        conv_one, stats = kernel_call(
            first_conv, "first_conv", [shape((2, so, mid), F32), stat_shape], [padded, band_one]
        )
        stats_one = exchange(stats)

        def moments(st_ref, v):
            mean = gathered(st_ref, 2 * v, chan) / voxels
            var = gathered(st_ref, 2 * v + 1, chan) / voxels - mean * mean
            return mean, lax.rsqrt(var + EPSILON)

        def second_conv(bound, c_ref, w_ref, st_in, p_ref, h_ref, c2_ref, st_ref, a_ref):
            rows = []
            for v in range(2):
                mean, rstd = moments(st_in, v)
                gain, bias = p_ref[0:1, :], p_ref[1:2, :]
                dest = a_ref if v == 0 else h_ref

                def act(g, carry):
                    at = pl.ds(pl.multiple_of(g * LANES, LANES), LANES)
                    z = gain * ((c_ref[v, :, at] - mean) * rstd) + bias
                    dest[:, at] = jnp.where(inside(bound, g), z * sigmoid(z), 0.0).astype(BF)
                    return carry

                lax.fori_loop(0, outer_groups, act, 0)

                def step(g, sums):
                    out = band_conv(dest, w_ref, g, pi, pitch)
                    c2_ref[v, :, pl.ds(pl.multiple_of(g * LANES, LANES), LANES)] = out
                    mine = jnp.where(own_rows(), out, 0.0)
                    return (
                        sums[0] + jnp.sum(mine, axis=0, keepdims=True),
                        sums[1] + jnp.sum(mine * mine, axis=0, keepdims=True),
                    )

                zero = jnp.zeros((1, LANES), F32)
                rows += list(lax.fori_loop(0, inner_groups, step, (zero, zero)))
            rows.append(jnp.zeros((4, LANES), F32))
            st_ref[...] = jnp.broadcast_to(jnp.concatenate(rows, axis=0)[None], st_ref.shape)

        hidden_b, conv_two, stats = kernel_call(
            second_conv,
            "second_conv",
            [shape((so, mid), BF), shape((2, si, line), F32), stat_shape],
            [bounds, conv_one, band_two, stats_one, params],
            scratch=[pltpu.VMEM((so, mid), BF)],
            smem=1,
        )
        stats_two = exchange(stats)

        def slope_two(c_ref, st_in, p_ref, go_ref, g):
            at = pl.ds(pl.multiple_of(g * LANES, LANES), LANES)
            mean, rstd = moments(st_in, 1)
            xhat = (c_ref[1, :, at] - mean) * rstd
            z = p_ref[2:3, :] * xhat + p_ref[3:4, :]
            s = sigmoid(z)
            d = go_ref[:, at].astype(F32) * (s * (1.0 + z * (1.0 - s)))
            return jnp.where(own_rows(), d, 0.0), xhat, rstd, at

        def sum_rows(ref, sums):
            rows = list(sums) + [jnp.zeros((6, LANES), F32)]
            ref[...] = jnp.broadcast_to(jnp.concatenate(rows, axis=0)[None], ref.shape)

        def native(value, order):
            return lax.dot_general(
                order, value, (((1,), (1,)), ((), ())), preferred_element_type=F32
            ).astype(BF).reshape(chan, span_y, span_z)

        def second_slope(c_ref, st_in, p_ref, go_ref, y_ref, st_ref):
            order = order_matrix(chan, span_y)
            mean, rstd = moments(st_in, 0)
            reps = line // LANES
            wide_mean, wide_rstd = jnp.tile(mean, (1, reps)), jnp.tile(rstd, (1, reps))
            gain, bias = jnp.tile(p_ref[2:3, :], (1, reps)), jnp.tile(p_ref[3:4, :], (1, reps))
            for x in range(span_x):
                c = c_ref[0, x * pitch : x * pitch + span_z, :]
                z = gain * ((c - wide_mean) * wide_rstd) + bias
                y_ref[:, x] = native((z * sigmoid(z)).astype(BF), order)

            def step(g, sums):
                d, xhat, _, _ = slope_two(c_ref, st_in, p_ref, go_ref, g)
                return (
                    sums[0] + jnp.sum(d, axis=0, keepdims=True),
                    sums[1] + jnp.sum(d * xhat, axis=0, keepdims=True),
                )

            zero = jnp.zeros((1, LANES), F32)
            sum_rows(st_ref, lax.fori_loop(0, inner_groups, step, (zero, zero)))

        y_a, stats = kernel_call(
            second_slope,
            "second_slope",
            [shape(x_a.shape, BF), stat_shape],
            [conv_two, stats_two, params, cot],
        )
        sums_two = exchange(stats)

        def second_delta(c_ref, st_in, p_ref, go_ref, sums_in, d_ref):
            sum_d, sum_x = gathered(sums_in, 0, chan) / voxels, gathered(sums_in, 1, chan) / voxels

            def step(g, carry):
                d, xhat, rstd, at = slope_two(c_ref, st_in, p_ref, go_ref, g)
                out = (p_ref[2:3, :] * rstd) * (d - sum_d - xhat * sum_x)
                d_ref[:, at] = jnp.where(own_rows(), out, 0.0).astype(BF)
                return carry

            lax.fori_loop(0, inner_groups, step, 0)

        (delta_two,) = kernel_call(
            second_delta,
            "second_delta",
            [shape((si, line), BF)],
            [conv_two, stats_two, params, cot, sums_two],
        )
        delta_pad = two_wide(delta_two.reshape(1, span_x, pitch, line)[:, :, :span_z])[0]

        def slope_one(c_ref, st_in, p_ref, g):
            at = pl.ds(pl.multiple_of(g * LANES, LANES), LANES)
            mean, rstd = moments(st_in, 1)
            xhat = (c_ref[:, at] - mean) * rstd
            z = p_ref[0:1, :] * xhat + p_ref[1:2, :]
            s = sigmoid(z)
            return s * (1.0 + z * (1.0 - s)), xhat, rstd, at

        def first_slope(dp_ref, w_ref, c_ref, st_in, p_ref, d2_ref, h_ref, d1_ref, st_ref, gw_ref, acc):
            acc[...] = jnp.zeros(acc.shape, F32)

            def step(g, sums):
                slope, xhat, _, at = slope_one(c_ref, st_in, p_ref, g)
                d = band_conv(dp_ref, w_ref, g, po, pitch) * slope
                d1_ref[:, at] = d
                mine = jnp.where(own(g), d[pitch : pitch + si], 0.0)
                return (
                    sums[0] + jnp.sum(mine, axis=0, keepdims=True),
                    sums[1] + jnp.sum(mine * xhat[pitch : pitch + si], axis=0, keepdims=True),
                )

            zero = jnp.zeros((1, LANES), F32)
            sum_rows(st_ref, lax.fori_loop(0, outer_groups, step, (zero, zero)))

            def taps(g, carry):
                at = pl.ds(pl.multiple_of(g * LANES, LANES), LANES)
                tap_products(d2_ref[:, at].astype(F32), h_ref, 0, g, pitch, acc)
                return carry

            lax.fori_loop(0, inner_groups, taps, 0)
            gw_ref[...] = fold_taps(acc, chan)

        taps_shape = shape((9 * chan, 3 * chan), F32)
        taps_scratch = [pltpu.VMEM((3, 3 * LANES, 2 * LANES), F32)]
        conv_one_b = conv_one[1]
        slope, stats, taps_two = kernel_call(
            first_slope,
            "first_slope",
            [shape((so, mid), F32), stat_shape, taps_shape],
            [delta_pad, back_two, conv_one_b, stats_one, params, delta_two, hidden_b],
            scratch=taps_scratch,
        )
        sums_one = exchange(stats)

        def first_delta(bound, s_ref, c_ref, st_in, p_ref, sums_in, w_ref, x_ref, dx_ref, gw_ref, d_ref, o_ref, acc):
            acc[...] = jnp.zeros(acc.shape, F32)
            sum_d, sum_x = gathered(sums_in, 0, chan) / voxels, gathered(sums_in, 1, chan) / voxels
            mean, rstd = moments(st_in, 1)

            def step(g, carry):
                at = pl.ds(pl.multiple_of(g * LANES, LANES), LANES)
                xhat = (c_ref[:, at] - mean) * rstd
                out = (p_ref[0:1, :] * rstd) * (s_ref[:, at] - sum_d - xhat * sum_x)
                out = jnp.where(inside(bound, g), out, 0.0).astype(BF)
                d_ref[:, at] = out
                mine = jnp.where(own(g), out[pitch : pitch + si].astype(F32), 0.0)
                tap_products(mine, x_ref, pitch, g, pitch, acc)
                return carry

            lax.fori_loop(0, outer_groups, step, 0)
            gw_ref[...] = fold_taps(acc, chan)

            def conv(g, carry):
                out = band_conv(d_ref, w_ref, g, pi, pitch)
                o_ref[:, pl.ds(pl.multiple_of(g * LANES, LANES), LANES)] = out.astype(BF)
                return carry

            lax.fori_loop(0, inner_groups, conv, 0)
            order = order_matrix(chan, span_y)
            for x in range(span_x):
                dx_ref[:, x] = native(o_ref[x * pitch : x * pitch + span_z, :], order)

        dx_b, taps_one = kernel_call(
            first_delta,
            "first_delta",
            [shape(x_a.shape, BF), taps_shape],
            [bounds, slope, conv_one_b, stats_one, params, sums_one, back_one, padded[1]],
            scratch=[pltpu.VMEM((so, mid), BF), pltpu.VMEM((si, line), BF)] + taps_scratch,
            smem=1,
        )

        both = jnp.stack([taps_one, taps_two]) * factor
        size = both.size
        share = -(-size // (world * 8 * LANES)) * 8
        flat = jnp.pad(both.reshape(-1), (0, share * world * LANES - size))
        part = jnp.sum(exchange(flat.reshape(world, share, LANES)), axis=0)
        whole = exchange(jnp.broadcast_to(part[None], (world, share, LANES)))
        whole = whole.reshape(-1)[:size].reshape(2, 3, 3, chan, 3, chan).transpose(0, 1, 4, 2, 3, 5)

        def channel_sums(got, row):
            return jnp.sum(jnp.sum(got[:, row], axis=0).reshape(per, chan), axis=0)

        grad_norm = factor * jnp.stack(
            [
                channel_sums(sums_one, 1),
                channel_sums(sums_one, 0),
                channel_sums(sums_two, 1),
                channel_sums(sums_two, 0),
            ]
        )
        return (y_a, dx_b, whole[0], whole[1], grad_norm)

    return body


def solution(mesh):
    block = P(None, "gx", "gy", "gz")
    placed = (block, block, P(), P(), P(), P(), P(), P(), block)
    return jax.shard_map(
        body_maker(mesh),
        mesh=mesh,
        in_specs=placed,
        out_specs=(block, block, P(), P(), P()),
        check_vma=False,
    )
```

```python
import math

import jax
import jax.numpy as jnp
from jax import lax
from jax.experimental import pallas as pl
from jax.experimental.pallas import tpu as pltpu
from jax.sharding import PartitionSpec as P

EPSILON = 1e-05
AXES = ("gx", "gy", "gz")
LANES = 128
SEAM = 16
BF = jnp.bfloat16
F32 = jnp.float32
VM = pl.BlockSpec(memory_space=pltpu.VMEM)
SM = pl.BlockSpec(memory_space=pltpu.SMEM)


def kernel_call(body, name, out_shape, args, scratch=(), smem=0, work=0):
    return pl.pallas_call(
        body,
        out_shape=out_shape,
        in_specs=[SM] * smem + [VM] * (len(args) - smem),
        out_specs=[VM] * len(out_shape),
        scratch_shapes=list(scratch),
        cost_estimate=pl.CostEstimate(flops=work, bytes_accessed=1 << 20, transcendentals=0),
        compiler_params=pltpu.CompilerParams(vmem_limit_bytes=8 << 20),
        name=name,
    )(*args)


def shape(dims, kind):
    return jax.ShapeDtypeStruct(dims, kind)


def exchange(spread_rows):
    return lax.all_to_all(spread_rows, AXES, 0, 0)


def neighbours(axis):
    count = lax.axis_size(axis)
    forward = [(i, i + 1) for i in range(count - 1)]
    return forward, [(t, s) for s, t in forward]


def order_matrix(chan, rows):
    size = chan * rows
    k = lax.broadcasted_iota(jnp.int32, (size, size), 0)
    n = lax.broadcasted_iota(jnp.int32, (size, size), 1)
    return (n == (k % rows) * chan + k // rows).astype(BF)


def lane_at(group):
    return pl.ds(pl.multiple_of(group * LANES, LANES), LANES)


def band_conv(src, weight, group, planes, pitch):
    size = planes * pitch + SEAM
    at = pl.multiple_of(group * LANES, LANES)
    parts = [src[pl.ds(d * pitch, size), pl.ds(at, 2 * LANES)] for d in range(3)]
    out = jnp.dot(jnp.concatenate(parts, axis=1), weight[...], preferred_element_type=F32)
    return (
        pltpu.roll(out[:, :LANES], 1, 0)
        + out[:, LANES : 2 * LANES]
        + pltpu.roll(out[:, 2 * LANES :], size - 1, 0)
    )


def tap_products(d_rows, h_ref, start, group, pitch, acc):
    size = d_rows.shape[0]
    three = jnp.concatenate(
        [pltpu.roll(d_rows, size - 1, 0), d_rows, pltpu.roll(d_rows, 1, 0)], axis=1
    )
    left = three.T.astype(BF)
    at = pl.multiple_of(group * LANES, LANES)
    for d in range(3):
        right = h_ref[pl.ds(start + d * pitch, size), pl.ds(at, 2 * LANES)]
        acc[d] = acc[d] + jnp.dot(left, right, preferred_element_type=F32)


def fold_taps(acc, out, first, chan, offset):
    per = LANES // chan
    for d in range(3):
        for t in range(3):
            rows = sum(
                acc[
                    d,
                    t * LANES + j * chan : t * LANES + (j + 1) * chan,
                    (j + offset) * chan : (j + offset + 3) * chan,
                ]
                for j in range(per)
            )
            for y in range(3):
                row, lane = divmod((d * 3 + y) * 3 + t, per)
                out[
                    first + row * chan : first + (row + 1) * chan, lane * chan : (lane + 1) * chan
                ] = rows[:, y * chan : (y + 1) * chan].astype(out.dtype)


def fold_lanes(value, chan):
    step = chan
    while step < LANES:
        value = value + pltpu.roll(value, step, 1)
        step *= 2
    return value


def gathered(ref, row, chan):
    return fold_lanes(jnp.sum(ref[:, row, :], axis=0, keepdims=True), chan)


def sigmoid(value):
    return 0.5 + 0.5 * jnp.tanh(0.5 * value)


def body(x_a, x_b, w_first, w_second, gain_first, bias_first, gain_second, bias_second, grad_out):
    chan, span_x, span_y, span_z = x_a.shape
    world = lax.axis_size("gx") * lax.axis_size("gy") * lax.axis_size("gz")
    voxels = float(span_x * span_y * span_z * world)
    factor = 1.0 / math.sqrt(voxels)
    per = LANES // chan
    line = span_y * chan
    tiles = line // LANES
    pitch = span_z + SEAM
    inner_groups = span_y // per
    outer_groups = inner_groups + 1
    wide = line + 2 * LANES
    mid = outer_groups * LANES
    po, pi = span_x + 2, span_x
    so, si, sw = po * pitch + SEAM, pi * pitch + SEAM, (span_x + 4) * pitch + SEAM
    flat_rows = span_x * span_z
    seams = (span_x + 1) * SEAM
    strip = si + tiles * seams
    swap = lax.axis_size("gz") == 2
    edges = 1 if swap else 2

    def limits(axis, low, high):
        at, count = lax.axis_index(axis), lax.axis_size(axis)
        return [jnp.where(at == 0, low + 1, low), jnp.where(at == count - 1, high - 1, high)]

    bounds = jnp.stack(
        limits("gx", 0, span_x + 2)
        + limits("gy", 0, span_y + 2)
        + limits("gz", -1, span_z + 1)
        + [lax.axis_index("gz"), lax.axis_index("gy") % 2]
    ).astype(jnp.int32)

    def fill_inside(bound, ref):
        row = lax.broadcasted_iota(jnp.int32, (so, LANES), 0) + (pitch - SEAM + 2)
        plane = row // pitch - 1
        z = row % pitch - 2
        ok = (plane >= bound[0]) & (plane < bound[1]) & (z >= bound[4]) & (z < bound[5])
        ref[...] = ok.astype(F32)

    def inside(bound, ref, group):
        lane = lax.broadcasted_iota(jnp.int32, (so, LANES), 1) + group * LANES
        y = lane // chan
        return (ref[...] > 0.5) & (y >= bound[2]) & (y < bound[3])

    def fill_own(ref):
        row = lax.broadcasted_iota(jnp.int32, (si, LANES), 0)
        ref[...] = ((row >= SEAM) & ((row - SEAM + pitch) % pitch < span_z)).astype(F32)

    def own(ref, group):
        lane = lax.broadcasted_iota(jnp.int32, (si, LANES), 1) + group * LANES
        return (ref[...] > 0.5) & (lane >= chan) & (lane < chan + line)

    own_scratch = pltpu.VMEM((si, LANES), F32)
    in_scratch = pltpu.VMEM((so, LANES), F32)


    def fill_bands(work):
        for out, w_ref, back, offset in work:
            out[...] = jnp.zeros(out.shape, BF)
            for dx in range(3):
                for dy in range(3):
                    for dz in range(3):
                        if back:
                            block = w_ref[2 - dx, 2 - dy, 2 - dz]
                        else:
                            block = w_ref[dx, dy, dz].astype(F32).T.astype(BF)
                        for j in range(per):
                            row = (dx * 2 * per + dy + j + offset) * chan
                            lane = dz * LANES + j * chan
                            out[row : row + chan, lane : lane + chan] = block

    def bands(w1_ref, w2_ref, g1_ref, b1_ref, g2_ref, b2_ref, one_ref, two_ref, p_ref):
        fill_bands(((one_ref, w1_ref, False, 2), (two_ref, w2_ref, False, 0)))
        p_ref[...] = jnp.zeros(p_ref.shape, F32)
        for row, ref in enumerate((g1_ref, b1_ref, g2_ref, b2_ref)):
            for j in range(per):
                p_ref[row : row + 1, j * chan : (j + 1) * chan] = ref[...]

    def back_bands(w1_ref, w2_ref, token, two_ref, one_ref):
        del token
        fill_bands(((two_ref, w2_ref, True, 2), (one_ref, w1_ref, True, 0)))

    band_shape = shape((6 * LANES, 3 * LANES), BF)
    token_shape = shape((8, LANES), F32)
    vectors = (gain_first, bias_first, gain_second, bias_second)
    band_one, band_two, params = kernel_call(
        bands,
        "bands",
        [band_shape, band_shape, token_shape],
        [w_first, w_second] + [v.reshape(1, chan) for v in vectors],
        work=1 << 31,
    )


    def turned(block, order):
        return lax.dot_general(
            block.reshape(chan * span_y, span_z),
            order,
            (((0,), (0,)), ((), ())),
            preferred_element_type=F32,
        ).astype(BF)

    def native(value, order):
        return lax.dot_general(
            order, value, (((1,), (1,)), ((), ())), preferred_element_type=F32
        ).astype(BF).reshape(chan, span_y, span_z)

    def z_tiles(bound, ref, at, v, z_ref):
        first = ref[at * span_z : at * span_z + SEAM, :]
        last = ref[(at + 1) * span_z - SEAM : (at + 1) * span_z, :]
        rows = slice(at * SEAM, (at + 1) * SEAM)
        if swap:
            pick = jnp.full(first.shape, bound[6], jnp.int32) == 0
            z_ref[0, rows] = jnp.where(pick, last.astype(F32), first.astype(F32)).astype(BF)
        else:
            z_ref[0, rows] = last
            z_ref[1, rows] = first

    def turn_in(bound, a_ref, b_ref, t_ref, z_ref):
        order = order_matrix(chan, span_y)
        for v, ref in enumerate((a_ref, b_ref)):
            for x in range(span_x):
                at = v * span_x + x
                t_ref[at * span_z : (at + 1) * span_z, :] = turned(ref[:, x], order)
                z_tiles(bound, t_ref, at, v, z_ref)

    def turn_cot(g_ref, o_ref):
        order = order_matrix(chan, span_y)
        o_ref[...] = jnp.zeros(o_ref.shape, BF)
        for x in range(span_x):
            at = SEAM + x * pitch
            o_ref[at : at + span_z, :] = turned(g_ref[:, x], order)


    def halo(block, tiles_z, count, token):
        forward_x, backward_x = neighbours("gx")
        rows_y = lax.axis_size("gy")
        pairs_y = [
            [p for i in range(first, rows_y - 1, 2) for p in ((i, i + 1), (i + 1, i))]
            for first in range(2)
        ]
        forward_z, backward_z = neighbours("gz")
        if swap:
            got_z = [lax.ppermute(tiles_z[0], "gz", [(0, 1), (1, 0)])]
        else:
            got_z = [
                lax.ppermute(tiles_z[0], "gz", forward_z),
                lax.ppermute(tiles_z[1], "gz", backward_z),
            ]

        def edge(bound, t_ref, *refs):
            got, (a_ref, b_ref, s_ref) = refs[:edges], refs[edges:]
            even = jnp.full((SEAM, LANES), bound[7], jnp.int32) == 0
            even_block = jnp.full((span_z, LANES), bound[7], jnp.int32) == 0

            def send(rows, low, high, ok):
                low, high = low.astype(F32), high.astype(F32)
                a_ref[rows, :] = jnp.where(ok, high, low).astype(BF)
                b_ref[rows, :] = jnp.where(ok, low, high).astype(BF)

            row = lax.broadcasted_iota(jnp.int32, (SEAM, line), 0)
            for v in range(count):
                parts = []
                for x in range(span_x + 1):
                    tile = jnp.zeros((SEAM, line), F32)
                    if x < span_x:
                        at = (v * span_x + x) * SEAM
                        value = got[0][at : at + SEAM, :].astype(F32)
                        ok = row >= SEAM - 2
                        if swap:
                            ok = ok & (jnp.full(row.shape, bound[6], jnp.int32) == 1)
                        tile = jnp.where(ok, value, tile)
                    if x > 0:
                        at = (v * span_x + x - 1) * SEAM
                        value = got[-1][at : at + SEAM, :].astype(F32)
                        ok = row < 2
                        if swap:
                            ok = ok & (jnp.full(row.shape, bound[6], jnp.int32) == 0)
                        tile = jnp.where(ok, value, tile)
                    parts.append(tile.astype(BF))
                for x in range(span_x + 1):
                    s_ref[v * seams + x * SEAM : v * seams + (x + 1) * SEAM, :] = parts[x]
                    base = v * si + x * pitch
                    send(
                        slice(base, base + SEAM),
                        parts[x][:, :LANES],
                        parts[x][:, line - LANES :],
                        even,
                    )
                    if x < span_x:
                        own_rows = slice((v * span_x + x) * span_z, (v * span_x + x + 1) * span_z)
                        rows = slice(base + SEAM, base + pitch)
                        send(
                            rows,
                            t_ref[own_rows, :LANES],
                            t_ref[own_rows, line - LANES :],
                            even_block,
                        )

        send_a, send_b, seam_rows = kernel_call(
            edge,
            "edge",
            [shape((count * si, LANES), BF)] * 2 + [shape((count * seams, line), BF)],
            [bounds, block] + got_z,
            smem=1,
        )
        got_a = lax.ppermute(send_a, "gy", pairs_y[0])
        got_b = lax.ppermute(send_b, "gy", pairs_y[1])

        def strips(bound, a_ref, b_ref, s_ref, token_ref, o_ref):
            del token_ref
            lane = lax.broadcasted_iota(jnp.int32, (si, LANES), 1)
            from_a = (lane < 2 * chan) == (jnp.full(lane.shape, bound[7], jnp.int32) == 0)
            for v in range(count):
                rows = slice(v * si, (v + 1) * si)
                o_ref[v * strip : v * strip + si, :] = jnp.where(
                    from_a, a_ref[rows, :].astype(F32), b_ref[rows, :].astype(F32)
                ).astype(BF)
                for t in range(tiles):
                    at = v * strip + si + t * seams
                    o_ref[at : at + seams, :] = s_ref[
                        v * seams : (v + 1) * seams, t * LANES : (t + 1) * LANES
                    ]

        (mine,) = kernel_call(
            strips,
            "strips",
            [shape((count * strip, LANES), BF)],
            [bounds, got_a, got_b, seam_rows, token],
            smem=1,
        )
        return [
            lax.ppermute(block, "gx", forward_x),
            block,
            lax.ppermute(block, "gx", backward_x),
            lax.ppermute(mine, "gx", forward_x),
            mine,
            lax.ppermute(mine, "gx", backward_x),
        ]

    def assemble(dest, v, pieces):
        blocks, strip_refs = pieces[:3], pieces[3:]
        lane = lax.broadcasted_iota(jnp.int32, (si, LANES), 1)
        edge_tiles = {}

        def put(seam, columns, value):
            if seam in edge_tiles and columns in edge_tiles[seam]:
                value = edge_tiles[seam].pop(columns) + value
                dest[seam : seam + SEAM, columns[0] : columns[1]] = value
            else:
                edge_tiles.setdefault(seam, {})[columns] = value

        for b in range(3):
            base = b * span_x * pitch
            for x in range(span_x):
                at = base + SEAM + x * pitch
                rows = slice((v * span_x + x) * span_z, (v * span_x + x + 1) * span_z)
                dest[at : at + span_z, LANES : LANES + line] = blocks[b][rows, :]
            ys = strip_refs[b][v * strip : v * strip + si, :].astype(F32)
            low = jnp.where(lane >= 2 * chan, ys, 0.0).astype(BF)
            high = jnp.where(lane < 2 * chan, ys, 0.0).astype(BF)
            last = si - SEAM
            for columns, value in (((0, LANES), low), ((LANES + line, wide), high)):
                dest[base + SEAM : base + last, columns[0] : columns[1]] = value[SEAM:last]
                put(base, columns, value[:SEAM])
                put(base + last, columns, value[last:])
            for t in range(tiles):
                at = v * strip + si + t * seams
                columns = (LANES * (t + 1), LANES * (t + 2))
                for x in range(span_x + 1):
                    value = strip_refs[b][at + x * SEAM : at + (x + 1) * SEAM, :]
                    seam = base + x * pitch
                    if 0 < x < span_x:
                        dest[seam : seam + SEAM, columns[0] : columns[1]] = value
                    else:
                        put(seam, columns, value)
        for seam, left in edge_tiles.items():
            for columns, value in left.items():
                dest[seam : seam + SEAM, columns[0] : columns[1]] = value


    stat_shape = shape((world, 4, LANES), F32)

    def send_rows(ref, rows):
        rows = list(rows)
        spare = ref.shape[1] - sum(r.shape[0] for r in rows)
        if spare:
            rows.append(jnp.zeros((spare, LANES), F32))
        ref[...] = jnp.broadcast_to(jnp.concatenate(rows, axis=0)[None], ref.shape)

    def moments(st_ref, row):
        mean = gathered(st_ref, row, chan) / voxels
        var = gathered(st_ref, row + 1, chan) / voxels - mean * mean
        return mean, lax.rsqrt(var + EPSILON)

    def add_up(sums, value, other):
        return (
            sums[0] + jnp.sum(value, axis=0, keepdims=True),
            sums[1] + jnp.sum(value * other, axis=0, keepdims=True),
        )

    def conv_one_of(v, w_ref, pieces, dest, c_ref, own_ref):
        fill_own(own_ref)
        assemble(dest, v, pieces)

        def step(g, sums):
            out = band_conv(dest, w_ref, g, po, pitch)
            c_ref[:, lane_at(g)] = out
            mine = jnp.where(own(own_ref, g), out[pitch : pitch + si], 0.0)
            return add_up(sums, mine, mine)

        return lax.fori_loop(0, outer_groups, step, (zero(), zero()))

    def zero():
        return jnp.zeros((1, LANES), F32)

    def first_conv_b(w_ref, *refs):
        pieces, (c_ref, x_ref, st_ref, own_ref) = refs[:6], refs[6:]
        send_rows(st_ref, conv_one_of(1, w_ref, pieces, x_ref, c_ref, own_ref))

    def first_conv_a(w_ref, *refs):
        pieces, (c_ref, st_ref, x_ref, own_ref) = refs[:6], refs[6:]
        rows = list(conv_one_of(0, w_ref, pieces, x_ref, c_ref, own_ref))
        st_ref[...] = jnp.concatenate(rows + [jnp.zeros((6, LANES), F32)], axis=0)

    def conv_two_of(bound, c_ref, w_ref, st_in, row, p_ref, h_ref, c2_ref, own_ref, in_ref):
        fill_own(own_ref)
        fill_inside(bound, in_ref)
        mean, rstd = moments(st_in, row)
        gain, bias = p_ref[0:1, :], p_ref[1:2, :]

        def act(g, carry):
            at = lane_at(g)
            z = gain * ((c_ref[:, at] - mean) * rstd) + bias
            h_ref[:, at] = jnp.where(inside(bound, in_ref, g), z * sigmoid(z), 0.0).astype(BF)
            return carry

        lax.fori_loop(0, outer_groups, act, 0)

        def step(g, sums):
            out = band_conv(h_ref, w_ref, g, pi, pitch)
            c2_ref[:, lane_at(g)] = out
            mine = jnp.where(own_ref[...] > 0.5, out, 0.0)
            return add_up(sums, mine, mine)

        return lax.fori_loop(0, inner_groups, step, (zero(), zero()))

    def second_conv_b(bound, c_ref, w_ref, st_in, p_ref, more, h_ref, c2_ref, st_ref, token_ref, own_ref, in_ref):
        token_ref[...] = jnp.zeros(token_ref.shape, F32)
        rows = conv_two_of(bound, c_ref, w_ref, st_in, 0, p_ref, h_ref, c2_ref, own_ref, in_ref)
        send_rows(st_ref, list(rows) + [more[0:2, :]])

    def second_conv_a(bound, c_ref, w_ref, st_in, p_ref, after, c2_ref, st_ref, h_ref, own_ref, in_ref):
        del after
        rows = conv_two_of(bound, c_ref, w_ref, st_in, 2, p_ref, h_ref, c2_ref, own_ref, in_ref)
        st_ref[...] = jnp.concatenate(list(rows) + [jnp.zeros((6, LANES), F32)], axis=0)

    def slope_two(c_ref, moment, p_ref, go_ref, own_ref, at):
        mean, rstd = moment
        xhat = (c_ref[:, at] - mean) * rstd
        z = p_ref[2:3, :] * xhat + p_ref[3:4, :]
        s = sigmoid(z)
        d = go_ref[:, at].astype(F32) * (s * (1.0 + z * (1.0 - s)))
        return jnp.where(own_ref[...] > 0.5, d, 0.0), xhat

    def second_slope(c_ref, st_in, p_ref, go_ref, st_ref, token_ref, own_ref):
        token_ref[...] = jnp.zeros(token_ref.shape, F32)
        fill_own(own_ref)
        moment = moments(st_in, 0)

        def step(g, sums):
            d, xhat = slope_two(c_ref, moment, p_ref, go_ref, own_ref, lane_at(g))
            return add_up(sums, d, xhat)

        send_rows(st_ref, lax.fori_loop(0, inner_groups, step, (zero(), zero())))

    def second_delta(bound, c_ref, st_in, p_ref, go_ref, sums_in, after, d_ref, t_ref, z_ref, own_ref):
        del after
        fill_own(own_ref)
        moment = moments(st_in, 0)
        scale = p_ref[2:3, :] * moment[1]
        sum_d, sum_x = gathered(sums_in, 0, chan) / voxels, gathered(sums_in, 1, chan) / voxels

        def step(g, carry):
            at = lane_at(g)
            d, xhat = slope_two(c_ref, moment, p_ref, go_ref, own_ref, at)
            out = scale * (d - sum_d - xhat * sum_x)
            d_ref[:, at] = jnp.where(own_ref[...] > 0.5, out, 0.0).astype(BF)
            return carry

        lax.fori_loop(0, inner_groups, step, 0)
        for x in range(span_x):
            base = SEAM + x * pitch
            t_ref[x * span_z : (x + 1) * span_z, :] = d_ref[base : base + span_z, :]
            z_tiles(bound, t_ref, x, 0, z_ref)

    def second_taps(d_ref, h_ref, after, gw_ref, acc):
        del after
        acc[...] = jnp.zeros(acc.shape, F32)

        def taps(g, carry):
            tap_products(d_ref[:, lane_at(g)].astype(F32), h_ref, 0, g, pitch, acc)
            return carry

        lax.fori_loop(0, inner_groups, taps, 0)
        gw_ref[...] = jnp.zeros(gw_ref.shape, F32)
        fold_taps(acc, gw_ref, 0, chan, 0)

    def first_slope(w_ref, c_ref, st_in, p_ref, more, *refs):
        pieces, (d1_ref, st_ref, token_ref, pad_ref, own_ref) = refs[:6], refs[6:]
        token_ref[...] = jnp.zeros(token_ref.shape, F32)
        fill_own(own_ref)
        assemble(pad_ref, 0, pieces)
        mean, rstd = moments(st_in, 0)

        def step(g, sums):
            at = lane_at(g)
            xhat = (c_ref[:, at] - mean) * rstd
            z = p_ref[0:1, :] * xhat + p_ref[1:2, :]
            s = sigmoid(z)
            d = band_conv(pad_ref, w_ref, g, po, pitch) * (s * (1.0 + z * (1.0 - s)))
            d1_ref[:, at] = d
            mine = jnp.where(own(own_ref, g), d[pitch : pitch + si], 0.0)
            return add_up(sums, mine, xhat[pitch : pitch + si])

        rows = lax.fori_loop(0, outer_groups, step, (zero(), zero()))
        send_rows(st_ref, list(rows) + [more[0:2, :]])

    def first_delta(bound, s_ref, c_ref, st_in, p_ref, sums_in, x_ref, more, d_ref, gw_ref, acc, own_ref, in_ref):
        fill_own(own_ref)
        fill_inside(bound, in_ref)
        acc[...] = jnp.zeros(acc.shape, F32)
        sum_d, sum_x = gathered(sums_in, 0, chan) / voxels, gathered(sums_in, 1, chan) / voxels
        mean, rstd = moments(st_in, 0)
        scale = p_ref[0:1, :] * rstd

        def step(g, carry):
            at = lane_at(g)
            xhat = (c_ref[:, at] - mean) * rstd
            out = scale * (s_ref[:, at] - sum_d - xhat * sum_x)
            out = jnp.where(inside(bound, in_ref, g), out, 0.0).astype(BF)
            d_ref[:, at] = out
            mine = jnp.where(own(own_ref, g), out[pitch : pitch + si].astype(F32), 0.0)
            tap_products(mine, x_ref, pitch, g, pitch, acc)
            return carry

        lax.fori_loop(0, outer_groups, step, 0)
        gw_ref[...] = jnp.zeros(gw_ref.shape, F32)
        fold_taps(acc, gw_ref, 0, chan, 2)
        gw_ref[tap_rows : 2 * tap_rows, :] = more[...]

    def mix(got_ref, after, out_ref):
        del after
        whole = jnp.sum(got_ref[...], axis=0, keepdims=True) * factor
        out_ref[...] = jnp.broadcast_to(whole.astype(BF), out_ref.shape)

    def last(got_ref, one_ref, two_ref):
        for out, first in ((one_ref, 0), (two_ref, tap_rows)):
            for at in range(27):
                row, lane = divmod(at, per)
                begin = first + row * chan
                block = got_ref[begin : begin + chan, lane * chan : (lane + 1) * chan]
                out[at // 9, at // 3 % 3, at % 3] = block.astype(F32)

    def last_conv(d_ref, w_ref, dx_ref, o_ref):
        def conv(g, carry):
            o_ref[:, lane_at(g)] = band_conv(d_ref, w_ref, g, pi, pitch).astype(BF)
            return carry

        lax.fori_loop(0, inner_groups, conv, 0)
        order = order_matrix(chan, span_y)
        for x in range(span_x):
            at = SEAM + x * pitch
            dx_ref[:, x] = native(o_ref[at : at + span_z, :], order)

    def out_a(c_ref, st_in, st_two, p_ref, y_ref, n_ref, h_ref):
        for row, (ref, at) in enumerate(((st_in, 1), (st_in, 0), (st_two, 1), (st_two, 0))):
            n_ref[row : row + 1, :] = factor * gathered(ref, at, chan)[:, :chan]
        order = order_matrix(chan, span_y)
        mean, rstd = moments(st_in, 2)

        def act(g, carry):
            at = lane_at(g)
            z = p_ref[2:3, :] * ((c_ref[:, at] - mean) * rstd) + p_ref[3:4, :]
            h_ref[:, at] = (z * sigmoid(z)).astype(BF)
            return carry

        lax.fori_loop(0, inner_groups, act, 0)
        for x in range(span_x):
            at = SEAM + x * pitch
            y_ref[:, x] = native(h_ref[at : at + span_z, :], order)


    vols, tiles_z = kernel_call(
        turn_in,
        "turn_in",
        [shape((2 * flat_rows, line), BF), shape((edges, 2 * span_x * SEAM, line), BF)],
        [bounds, x_a, x_b],
        smem=1,
    )
    pieces = halo(vols, tiles_z, 2, params)
    (cot,) = kernel_call(
        turn_cot, "turn_cot", [shape((si, line), BF)], [grad_out], work=1 << 27
    )
    c1_b, pad_b, stats = kernel_call(
        first_conv_b,
        "first_conv_b",
        [shape((so, mid), F32), shape((sw, wide), BF), stat_shape],
        [band_one] + pieces,
        scratch=[own_scratch],
        work=1 << 30,
    )
    stats_one = exchange(stats)
    c1_a, local_a = kernel_call(
        first_conv_a,
        "first_conv_a",
        [shape((so, mid), F32), shape((8, LANES), F32)],
        [band_one] + pieces,
        scratch=[pltpu.VMEM((sw, wide), BF), own_scratch],
        work=1 << 32,
    )
    hidden_b, c2_b, stats, token = kernel_call(
        second_conv_b,
        "second_conv_b",
        [shape((so, mid), BF), shape((si, line), F32), stat_shape, token_shape],
        [bounds, c1_b, band_two, stats_one, params, local_a],
        scratch=[own_scratch, in_scratch],
        smem=1,
        work=1 << 30,
    )
    stats_two = exchange(stats)
    back_two, back_one = kernel_call(
        back_bands,
        "back_bands",
        [band_shape, band_shape],
        [w_first, w_second, token],
        work=1 << 31,
    )
    stats, token = kernel_call(
        second_slope,
        "second_slope",
        [stat_shape, token_shape],
        [c2_b, stats_two, params, cot],
        scratch=[own_scratch],
        work=1 << 27,
    )
    sums_two = exchange(stats)
    c2_a, local_a = kernel_call(
        second_conv_a,
        "second_conv_a",
        [shape((si, line), F32), shape((8, LANES), F32)],
        [bounds, c1_a, band_two, stats_two, params, token],
        scratch=[pltpu.VMEM((so, mid), BF), own_scratch, in_scratch],
        smem=1,
        work=1 << 32,
    )
    delta_two, block, tiles_z = kernel_call(
        second_delta,
        "second_delta",
        [
            shape((si, line), BF),
            shape((flat_rows, line), BF),
            shape((edges, span_x * SEAM, line), BF),
        ],
        [bounds, c2_b, stats_two, params, cot, sums_two, local_a],
        scratch=[own_scratch],
        smem=1,
        work=1 << 27,
    )
    pieces = halo(block, tiles_z, 1, local_a)
    tap_rows = -(-27 // per) * chan
    taps_shape = shape((tap_rows, LANES), F32)
    acc_scratch = pltpu.VMEM((3, 3 * LANES, 2 * LANES), F32)
    slope, stats, token = kernel_call(
        first_slope,
        "first_slope",
        [shape((so, mid), F32), stat_shape, token_shape],
        [back_two, c1_b, stats_one, params, local_a] + pieces,
        scratch=[pltpu.VMEM((sw, wide), BF), own_scratch],
        work=1 << 30,
    )
    sums_one = exchange(stats)
    (taps_two,) = kernel_call(
        second_taps,
        "second_taps",
        [taps_shape],
        [delta_two, hidden_b, token],
        scratch=[acc_scratch],
        work=1 << 32,
    )
    share = -(-2 * tap_rows // (world * 8)) * 8
    delta_one, taps = kernel_call(
        first_delta,
        "first_delta",
        [shape((so, mid), BF), shape((share * world, LANES), F32)],
        [bounds, slope, c1_b, stats_one, params, sums_one, pad_b, taps_two],
        scratch=[acc_scratch, own_scratch, in_scratch],
        smem=1,
        work=1 << 30,
    )
    (dx_b,) = kernel_call(
        last_conv,
        "last_conv",
        [shape(x_a.shape, BF)],
        [delta_one, back_one],
        scratch=[pltpu.VMEM((si, line), BF)],
        work=1 << 32,
    )
    y_a, grad_norm = kernel_call(
        out_a,
        "out_a",
        [shape(x_a.shape, BF), shape((4, chan), F32)],
        [c2_a, sums_one, sums_two, params],
        scratch=[pltpu.VMEM((si, line), BF)],
        work=1 << 32,
    )

    part = exchange(taps.reshape(world, share, LANES))
    (whole,) = kernel_call(mix, "mix", [shape(part.shape, BF)], [part, grad_norm])
    whole = exchange(whole).reshape(world * share, LANES)
    weight_shape = shape((3, 3, 3, chan, chan), F32)
    grad_one, grad_two = kernel_call(last, "last", [weight_shape, weight_shape], [whole])
    return (y_a, dx_b, grad_one, grad_two, grad_norm)


def solution(mesh):
    block = P(None, "gx", "gy", "gz")
    placed = (block, block, P(), P(), P(), P(), P(), P(), block)
    return jax.shard_map(
        body,
        mesh=mesh,
        in_specs=placed,
        out_specs=(block, block, P(), P(), P()),
        check_vma=False,
    )
```

```python
import math

import jax
import jax.numpy as jnp
from jax import lax
from jax.experimental import pallas as pl
from jax.experimental.pallas import tpu as pltpu
from jax.sharding import PartitionSpec as P

EPSILON = 1e-05
AXES = ("gx", "gy", "gz")
LANES = 128
SEAM = 16
BF = jnp.bfloat16
F32 = jnp.float32
VM = pl.BlockSpec(memory_space=pltpu.VMEM)
SM = pl.BlockSpec(memory_space=pltpu.SMEM)
HB = pl.BlockSpec(memory_space=pltpu.HBM)


def kernel_call(body, name, out_shape, args, scratch=(), smem=0, work=0, far=(), far_out=()):
    args = [
        pltpu.with_memory_space_constraint(a, pltpu.HBM) if i in far else a
        for i, a in enumerate(args)
    ]
    out_shape = [
        pltpu.HBM(o.shape, o.dtype) if i in far_out else o for i, o in enumerate(out_shape)
    ]
    return pl.pallas_call(
        body,
        out_shape=out_shape,
        in_specs=[SM if i < smem else HB if i in far else VM for i in range(len(args))],
        out_specs=[HB if i in far_out else VM for i in range(len(out_shape))],
        scratch_shapes=list(scratch),
        cost_estimate=pl.CostEstimate(flops=work, bytes_accessed=1 << 20, transcendentals=0),
        compiler_params=pltpu.CompilerParams(vmem_limit_bytes=12 << 20),
        name=name,
    )(*args)


def shape(dims, kind):
    return jax.ShapeDtypeStruct(dims, kind)


def exchange(spread_rows):
    return lax.all_to_all(spread_rows, AXES, 0, 0)


def neighbours(axis):
    count = lax.axis_size(axis)
    forward = [(i, i + 1) for i in range(count - 1)]
    return forward, [(t, s) for s, t in forward]


def order_matrix(chan, rows):
    size = chan * rows
    k = lax.broadcasted_iota(jnp.int32, (size, size), 0)
    n = lax.broadcasted_iota(jnp.int32, (size, size), 1)
    return (n == (k % rows) * chan + k // rows).astype(BF)


def lane_at(group):
    return pl.ds(pl.multiple_of(group * LANES, LANES), LANES)


def band_conv(src, weight, group, planes, pitch):
    size = planes * pitch + SEAM
    at = pl.multiple_of(group * LANES, LANES)
    parts = [src[pl.ds(d * pitch, size), pl.ds(at, 2 * LANES)] for d in range(3)]
    out = jnp.dot(jnp.concatenate(parts, axis=1), weight[...], preferred_element_type=F32)
    return (
        pltpu.roll(out[:, :LANES], 1, 0)
        + out[:, LANES : 2 * LANES]
        + pltpu.roll(out[:, 2 * LANES :], size - 1, 0)
    )


def tap_products(d_rows, h_ref, start, group, pitch, acc):
    size = d_rows.shape[0]
    three = jnp.concatenate(
        [pltpu.roll(d_rows, size - 1, 0), d_rows, pltpu.roll(d_rows, 1, 0)], axis=1
    )
    left = three.T.astype(BF)
    at = pl.multiple_of(group * LANES, LANES)
    for d in range(3):
        right = h_ref[pl.ds(start + d * pitch, size), pl.ds(at, 2 * LANES)]
        acc[d] = acc[d] + jnp.dot(left, right, preferred_element_type=F32)


def fold_taps(acc, out, first, chan, offset):
    per = LANES // chan
    for d in range(3):
        for t in range(3):
            rows = sum(
                acc[
                    d,
                    t * LANES + j * chan : t * LANES + (j + 1) * chan,
                    (j + offset) * chan : (j + offset + 3) * chan,
                ]
                for j in range(per)
            )
            for y in range(3):
                row, lane = divmod((d * 3 + y) * 3 + t, per)
                out[
                    first + row * chan : first + (row + 1) * chan, lane * chan : (lane + 1) * chan
                ] = rows[:, y * chan : (y + 1) * chan].astype(out.dtype)


def fold_lanes(value, chan):
    step = chan
    while step < LANES:
        value = value + pltpu.roll(value, step, 1)
        step *= 2
    return value


def packed(sums, chan):
    lane = lax.broadcasted_iota(jnp.int32, (1, LANES), 1)
    out = jnp.zeros((1, LANES), F32)
    for k, value in enumerate(sums):
        out = jnp.where(lane // chan == k, fold_lanes(value, chan), out)
    return out


def gathered(ref, k, chan):
    total = jnp.sum(ref[:, 0, :], axis=0, keepdims=True)
    lane = lax.broadcasted_iota(jnp.int32, (1, LANES), 1)
    return fold_lanes(jnp.where(lane // chan == k, total, 0.0), chan)


def sigmoid(value):
    return 0.5 + 0.5 * jnp.tanh(0.5 * value)


def body(x_a, x_b, w_first, w_second, gain_first, bias_first, gain_second, bias_second, grad_out):
    chan, span_x, span_y, span_z = x_a.shape
    world = lax.axis_size("gx") * lax.axis_size("gy") * lax.axis_size("gz")
    voxels = float(span_x * span_y * span_z * world)
    factor = 1.0 / math.sqrt(voxels)
    per = LANES // chan
    line = span_y * chan
    tiles = line // LANES
    pitch = span_z + SEAM
    inner_groups = span_y // per
    outer_groups = inner_groups + 1
    wide = line + 2 * LANES
    mid = outer_groups * LANES
    po, pi = span_x + 2, span_x
    so, si, sw = po * pitch + SEAM, pi * pitch + SEAM, (span_x + 4) * pitch + SEAM
    flat_rows = span_x * span_z
    seams = (span_x + 1) * SEAM
    strip = si + tiles * seams
    swap = lax.axis_size("gz") == 2
    tap_rows = -(-27 // per) * chan
    hold = -(-tap_rows // world)
    edges = 1 if swap else 2

    def limits(axis, low, high):
        at, count = lax.axis_index(axis), lax.axis_size(axis)
        return [jnp.where(at == 0, low + 1, low), jnp.where(at == count - 1, high - 1, high)]

    bounds = jnp.stack(
        limits("gx", 0, span_x + 2)
        + limits("gy", 0, span_y + 2)
        + limits("gz", -1, span_z + 1)
        + [lax.axis_index("gz"), lax.axis_index("gy") % 2, lax.axis_index(AXES)]
    ).astype(jnp.int32)

    def fill_inside(bound, ref):
        row = lax.broadcasted_iota(jnp.int32, (so, LANES), 0) + (pitch - SEAM + 2)
        plane = row // pitch - 1
        z = row % pitch - 2
        ok = (plane >= bound[0]) & (plane < bound[1]) & (z >= bound[4]) & (z < bound[5])
        ref[...] = ok.astype(F32)

    def inside(bound, ref, group):
        lane = lax.broadcasted_iota(jnp.int32, (so, LANES), 1) + group * LANES
        y = lane // chan
        return (ref[...] > 0.5) & (y >= bound[2]) & (y < bound[3])

    def fill_own(ref):
        row = lax.broadcasted_iota(jnp.int32, (si, LANES), 0)
        ref[...] = ((row >= SEAM) & ((row - SEAM + pitch) % pitch < span_z)).astype(F32)

    def own(ref, group):
        lane = lax.broadcasted_iota(jnp.int32, (si, LANES), 1) + group * LANES
        return (ref[...] > 0.5) & (lane >= chan) & (lane < chan + line)

    own_scratch = pltpu.VMEM((si, LANES), F32)
    in_scratch = pltpu.VMEM((so, LANES), F32)


    def prepare(w1_ref, w2_ref, g1_ref, b1_ref, g2_ref, b2_ref, c_ref, p_ref, w1, w2, v, sems):
        copies = [
            pltpu.make_async_copy(source, dest, sems.at[i])
            for i, (source, dest) in enumerate(
                ((w1_ref, w1), (w2_ref, w2))
                + tuple((r, v.at[i : i + 1]) for i, r in enumerate((g1_ref, b1_ref, g2_ref, b2_ref)))
            )
        ]
        for copy in copies:
            copy.start()
        c_ref[...] = jnp.zeros(c_ref.shape, BF)
        p_ref[...] = jnp.zeros(p_ref.shape, F32)
        for copy in copies:
            copy.wait()
        for j in range(per):
            p_ref[0:4, j * chan : (j + 1) * chan] = v[0:4, 0:chan]
        for kind, (w, back) in enumerate(((w1, False), (w2, False), (w2, True), (w1, True))):
            for dx in range(3):
                for dy in range(3):
                    for dz in range(3):
                        if back:
                            block = w[2 - dx, 2 - dy, 2 - dz]
                        else:
                            block = w[dx, dy, dz].astype(F32).T.astype(BF)
                        row = ((kind * 3 + dx) * 3 + dy) * chan
                        c_ref[row : row + chan, dz * chan : (dz + 1) * chan] = block

    def fill_band(band, c_ref, kind, offset):
        band[...] = jnp.zeros(band.shape, BF)
        for dx in range(3):
            at = (kind * 3 + dx) * 3 * chan
            for dz in range(3):
                block = c_ref[at : at + 3 * chan, dz * chan : (dz + 1) * chan]
                for j in range(per):
                    row = (dx * 2 * per + j + offset) * chan
                    lane = dz * LANES + j * chan
                    band[row : row + 3 * chan, lane : lane + chan] = block

    band_scratch = pltpu.VMEM((6 * LANES, 3 * LANES), BF)
    token_shape = shape((8, LANES), F32)
    vectors = (gain_first, bias_first, gain_second, bias_second)
    weights, params = kernel_call(
        prepare,
        "prepare",
        [shape((4 * 9 * chan, LANES), BF), token_shape],
        [w_first, w_second] + [v.reshape(1, chan) for v in vectors],
        scratch=[
            pltpu.VMEM(w_first.shape, BF),
            pltpu.VMEM(w_second.shape, BF),
            pltpu.VMEM((8, chan), F32),
            pltpu.SemaphoreType.DMA((6,)),
        ],
        far=range(6),
        work=1 << 31,
    )


    def turned(block, order):
        return lax.dot_general(
            block.reshape(chan * span_y, span_z),
            order,
            (((0,), (0,)), ((), ())),
            preferred_element_type=F32,
        ).astype(BF)

    def native(value, order):
        return lax.dot_general(
            order, value, (((1,), (1,)), ((), ())), preferred_element_type=F32
        ).astype(BF).reshape(chan, span_y, span_z)

    def z_tiles(bound, ref, at, v, z_ref):
        first = ref[at * span_z : at * span_z + SEAM, :]
        last = ref[(at + 1) * span_z - SEAM : (at + 1) * span_z, :]
        rows = slice(at * SEAM, (at + 1) * SEAM)
        if swap:
            pick = jnp.full(first.shape, bound[6], jnp.int32) == 0
            z_ref[0, rows] = jnp.where(pick, last.astype(F32), first.astype(F32)).astype(BF)
        else:
            z_ref[0, rows] = last
            z_ref[1, rows] = first

    def turn_in(bound, a_ref, b_ref, t_ref, z_ref, buf, sems):
        copies = [
            pltpu.make_async_copy(ref.at[:, x], buf.at[v * span_x + x], sems.at[v * span_x + x])
            for v, ref in enumerate((a_ref, b_ref))
            for x in range(span_x)
        ]
        for copy in copies:
            copy.start()
        order = order_matrix(chan, span_y)
        for v in range(2):
            for x in range(span_x):
                at = v * span_x + x
                copies[at].wait()
                t_ref[at * span_z : (at + 1) * span_z, :] = turned(buf[at], order)
                z_tiles(bound, t_ref, at, v, z_ref)

    def turn_cot(g_ref, o_ref):
        order = order_matrix(chan, span_y)
        o_ref[...] = jnp.zeros(o_ref.shape, BF)
        for x in range(span_x):
            at = SEAM + x * pitch
            o_ref[at : at + span_z, :] = turned(g_ref[:, x], order)


    def halo(block, tiles_z, count, token):
        forward_x, backward_x = neighbours("gx")
        rows_y = lax.axis_size("gy")
        pairs_y = [
            [p for i in range(first, rows_y - 1, 2) for p in ((i, i + 1), (i + 1, i))]
            for first in range(2)
        ]
        forward_z, backward_z = neighbours("gz")
        if swap:
            got_z = [lax.ppermute(tiles_z[0], "gz", [(0, 1), (1, 0)])]
        else:
            got_z = [
                lax.ppermute(tiles_z[0], "gz", forward_z),
                lax.ppermute(tiles_z[1], "gz", backward_z),
            ]

        def edge(bound, t_ref, *refs):
            got, (a_ref, b_ref, s_ref) = refs[:edges], refs[edges:]
            even = jnp.full((SEAM, LANES), bound[7], jnp.int32) == 0
            even_block = jnp.full((span_z, LANES), bound[7], jnp.int32) == 0

            def choose(rows, low, high, ok):
                low, high = low.astype(F32), high.astype(F32)
                a_ref[rows, :] = jnp.where(ok, high, low).astype(BF)
                b_ref[rows, :] = jnp.where(ok, low, high).astype(BF)

            row = lax.broadcasted_iota(jnp.int32, (SEAM, line), 0)
            for v in range(count):
                parts = []
                for x in range(span_x + 1):
                    tile = jnp.zeros((SEAM, line), F32)
                    if x < span_x:
                        at = (v * span_x + x) * SEAM
                        value = got[0][at : at + SEAM, :].astype(F32)
                        ok = row >= SEAM - 2
                        if swap:
                            ok = ok & (jnp.full(row.shape, bound[6], jnp.int32) == 1)
                        tile = jnp.where(ok, value, tile)
                    if x > 0:
                        at = (v * span_x + x - 1) * SEAM
                        value = got[-1][at : at + SEAM, :].astype(F32)
                        ok = row < 2
                        if swap:
                            ok = ok & (jnp.full(row.shape, bound[6], jnp.int32) == 0)
                        tile = jnp.where(ok, value, tile)
                    parts.append(tile.astype(BF))
                for x in range(span_x + 1):
                    s_ref[v * seams + x * SEAM : v * seams + (x + 1) * SEAM, :] = parts[x]
                    base = v * si + x * pitch
                    choose(
                        slice(base, base + SEAM),
                        parts[x][:, :LANES],
                        parts[x][:, line - LANES :],
                        even,
                    )
                    if x < span_x:
                        own_rows = slice((v * span_x + x) * span_z, (v * span_x + x + 1) * span_z)
                        rows = slice(base + SEAM, base + pitch)
                        choose(
                            rows,
                            t_ref[own_rows, :LANES],
                            t_ref[own_rows, line - LANES :],
                            even_block,
                        )

        send_a, send_b, seam_rows = kernel_call(
            edge,
            "edge",
            [shape((count * si, LANES), BF)] * 2 + [shape((count * seams, line), BF)],
            [bounds, block] + got_z,
            smem=1,
        )
        got_a = lax.ppermute(send_a, "gy", pairs_y[0])
        got_b = lax.ppermute(send_b, "gy", pairs_y[1])

        def strips(bound, a_ref, b_ref, s_ref, token_ref, o_ref):
            del token_ref
            lane = lax.broadcasted_iota(jnp.int32, (si, LANES), 1)
            from_a = (lane < 2 * chan) == (jnp.full(lane.shape, bound[7], jnp.int32) == 0)
            for v in range(count):
                rows = slice(v * si, (v + 1) * si)
                o_ref[v * strip : v * strip + si, :] = jnp.where(
                    from_a, a_ref[rows, :].astype(F32), b_ref[rows, :].astype(F32)
                ).astype(BF)
                for t in range(tiles):
                    at = v * strip + si + t * seams
                    o_ref[at : at + seams, :] = s_ref[
                        v * seams : (v + 1) * seams, t * LANES : (t + 1) * LANES
                    ]

        (mine,) = kernel_call(
            strips,
            "strips",
            [shape((count * strip, LANES), BF)],
            [bounds, got_a, got_b, seam_rows, token],
            smem=1,
        )
        return [
            lax.ppermute(block, "gx", forward_x),
            block,
            lax.ppermute(block, "gx", backward_x),
            lax.ppermute(mine, "gx", forward_x),
            mine,
            lax.ppermute(mine, "gx", backward_x),
        ]

    def assemble(dest, v, pieces):
        blocks, strip_refs = pieces[:3], pieces[3:]
        lane = lax.broadcasted_iota(jnp.int32, (si, LANES), 1)
        edge_tiles = {}

        def put(seam, columns, value):
            if seam in edge_tiles and columns in edge_tiles[seam]:
                value = edge_tiles[seam].pop(columns) + value
                dest[seam : seam + SEAM, columns[0] : columns[1]] = value
            else:
                edge_tiles.setdefault(seam, {})[columns] = value

        for b in range(3):
            base = b * span_x * pitch
            for x in range(span_x):
                at = base + SEAM + x * pitch
                rows = slice((v * span_x + x) * span_z, (v * span_x + x + 1) * span_z)
                dest[at : at + span_z, LANES : LANES + line] = blocks[b][rows, :]
            ys = strip_refs[b][v * strip : v * strip + si, :].astype(F32)
            low = jnp.where(lane >= 2 * chan, ys, 0.0).astype(BF)
            high = jnp.where(lane < 2 * chan, ys, 0.0).astype(BF)
            last = si - SEAM
            for columns, value in (((0, LANES), low), ((LANES + line, wide), high)):
                dest[base + SEAM : base + last, columns[0] : columns[1]] = value[SEAM:last]
                put(base, columns, value[:SEAM])
                put(base + last, columns, value[last:])
            for t in range(tiles):
                at = v * strip + si + t * seams
                columns = (LANES * (t + 1), LANES * (t + 2))
                for x in range(span_x + 1):
                    value = strip_refs[b][at + x * SEAM : at + (x + 1) * SEAM, :]
                    seam = base + x * pitch
                    if 0 < x < span_x:
                        dest[seam : seam + SEAM, columns[0] : columns[1]] = value
                    else:
                        put(seam, columns, value)
        for seam, left in edge_tiles.items():
            for columns, value in left.items():
                dest[seam : seam + SEAM, columns[0] : columns[1]] = value


    def stat_shape(rows):
        return shape((world, rows, LANES), F32)

    def send(ref, sums, *parts):
        ref[:, 0:1, :] = jnp.broadcast_to(packed(sums, chan)[None], (world, 1, LANES))
        for i, part in enumerate(parts):
            for d in range(world):
                ref[d, 1 + i * hold : 1 + (i + 1) * hold, :] = part[d * hold : (d + 1) * hold, :]

    def moments(st_ref, row):
        mean = gathered(st_ref, row, chan) / voxels
        var = gathered(st_ref, row + 1, chan) / voxels - mean * mean
        return mean, lax.rsqrt(var + EPSILON)

    def add_up(sums, value, other):
        return (
            sums[0] + jnp.sum(value, axis=0, keepdims=True),
            sums[1] + jnp.sum(value * other, axis=0, keepdims=True),
        )

    def conv_one_of(v, w_ref, pieces, dest, c_ref, own_ref, band, after=None, to=None):
        fill_own(own_ref)
        assemble(dest, v, pieces)
        if after is not None:
            after.start()
        fill_band(band, w_ref, 0, 2)

        def step(g, sums):
            out = band_conv(dest, band, g, po, pitch)
            c_ref[:, lane_at(g)] = out
            if to is not None:
                column(c_ref, to[0], to[1], g).start()
            mine = jnp.where(own(own_ref, g), out[pitch : pitch + si], 0.0)
            return add_up(sums, mine, mine)

        return lax.fori_loop(0, outer_groups, step, (zero(), zero()))

    def zero():
        return jnp.zeros((1, LANES), F32)

    def first_conv_b(w_ref, *refs):
        pieces, rest = refs[:6], refs[6:]
        c_ref, x_out, st_ref, m_ref, x_ref, own_ref, band, sem = rest
        copy = pltpu.make_async_copy(x_ref, x_out, sem)
        send(st_ref, conv_one_of(1, w_ref, pieces, x_ref, c_ref, own_ref, band, copy))
        plain_taps(x_ref, m_ref)
        copy.wait()

    def first_conv_a(w_ref, after, *refs):
        del after
        pieces, (c_out, st_ref, x_ref, c_ref, own_ref, band, sems) = refs[:6], refs[6:]
        st_ref[...] = jnp.zeros(st_ref.shape, F32)
        rows = conv_one_of(0, w_ref, pieces, x_ref, c_ref, own_ref, band, None, (c_out, sems))
        for k in range(2):
            st_ref[k : k + 1, :] = rows[k]
        columns(c_ref, c_out, sems)

    def column(source, dest, sems, g):
        return pltpu.make_async_copy(source.at[:, lane_at(g)], dest.at[:, lane_at(g)], sems.at[g])

    def columns(source, dest, sems):
        def wait(g, carry):
            column(source, dest, sems, g).wait()
            return carry

        lax.fori_loop(0, outer_groups, wait, 0)

    def conv_two_of(bound, c_ref, w_ref, st_in, row, p_ref, h_ref, c2_ref, own_ref, in_ref, band, after=None):
        fill_own(own_ref)
        fill_inside(bound, in_ref)
        mean, rstd = moments(st_in, row)
        gain, bias = p_ref[0:1, :], p_ref[1:2, :]

        def act(g, carry):
            at = lane_at(g)
            z = gain * ((c_ref[:, at] - mean) * rstd) + bias
            h_ref[:, at] = jnp.where(inside(bound, in_ref, g), z * sigmoid(z), 0.0).astype(BF)
            return carry

        lax.fori_loop(0, outer_groups, act, 0)
        if after is not None:
            after.start()
        fill_band(band, w_ref, 1, 0)

        def step(g, sums):
            out = band_conv(h_ref, band, g, pi, pitch)
            c2_ref[:, lane_at(g)] = out
            mine = jnp.where(own_ref[...] > 0.5, out, 0.0)
            return add_up(sums, mine, mine)

        return lax.fori_loop(0, inner_groups, step, (zero(), zero()))

    def second_conv_b(bound, c_ref, w_ref, st_in, p_ref, more, m_ref, h_out, c2_ref, st_ref, token_ref, h_ref, own_ref, in_ref, band, sem):
        token_ref[...] = jnp.zeros(token_ref.shape, F32)
        copy = pltpu.make_async_copy(h_ref, h_out, sem)
        rows = conv_two_of(bound, c_ref, w_ref, st_in, 0, p_ref, h_ref, c2_ref, own_ref, in_ref, band, copy)
        send(st_ref, list(rows) + [more[0:1, :], more[1:2, :]])
        for d in range(world):
            for k in range(2):
                row = min(d * hold // chan + k, m_ref.shape[0] - 1)
                st_ref[d, 1 + k : 2 + k, :] = m_ref[row : row + 1, :]
        copy.wait()

    def second_conv_a(bound, c_far, w_ref, st_in, p_ref, after, c2_ref, st_ref, c_ref, h_ref, own_ref, in_ref, band, sem):
        del after
        copy = pltpu.make_async_copy(c_far, c_ref, sem)
        copy.start()
        copy.wait()
        rows = conv_two_of(bound, c_ref, w_ref, st_in, 2, p_ref, h_ref, c2_ref, own_ref, in_ref, band)
        st_ref[...] = jnp.concatenate(list(rows) + [jnp.zeros((6, LANES), F32)], axis=0)

    def early_taps(c_ref, st_in, x_far, after, t_ref, x_ref, acc, own_ref, sem):
        del after
        copy = pltpu.make_async_copy(x_far, x_ref, sem)
        copy.start()
        fill_own(own_ref)
        mean, rstd = moments(st_in, 0)
        acc[...] = jnp.zeros(acc.shape, F32)
        copy.wait()

        def step(g, carry):
            xhat = (c_ref[pl.ds(pitch, si), lane_at(g)] - mean) * rstd
            tap_products(jnp.where(own(own_ref, g), xhat, 0.0), x_ref, pitch, g, pitch, acc)
            return carry

        lax.fori_loop(0, outer_groups, step, 0)
        t_ref[...] = jnp.zeros(t_ref.shape, F32)
        fold_taps(acc, t_ref, 0, chan, 2)

    def plain_taps(x_ref, m_ref):
        m_ref[...] = jnp.zeros(m_ref.shape, F32)
        row = lax.broadcasted_iota(jnp.int32, (8, si), 0)
        at = lax.broadcasted_iota(jnp.int32, (8, si), 1)
        pick = jnp.zeros((8, si), F32)
        for x in range(span_x):
            for t in range(3):
                low = SEAM + x * pitch + t - 1
                pick = jnp.where((row == t) & (at >= low) & (at < low + span_z), 1.0, pick)
        pick = pick.astype(BF)
        for d in range(3):
            cols = jnp.dot(
                pick, x_ref[pl.ds((1 + d) * pitch, si), :], preferred_element_type=F32
            )
            for y in range(3):
                begin = LANES + (y - 1) * chan
                own_cols = cols[:, begin : begin + line]
                total = sum(own_cols[:, k * LANES : (k + 1) * LANES] for k in range(tiles))
                total = fold_lanes(total, chan)
                for t in range(3):
                    group, place = divmod((d * 3 + y) * 3 + t, per)
                    m_ref[group : group + 1, place * chan : (place + 1) * chan] = total[
                        t : t + 1, place * chan : (place + 1) * chan
                    ]

    def slope_two(c_ref, moment, p_ref, go_ref, own_ref, at):
        mean, rstd = moment
        xhat = (c_ref[:, at] - mean) * rstd
        z = p_ref[2:3, :] * xhat + p_ref[3:4, :]
        s = sigmoid(z)
        d = go_ref[:, at].astype(F32) * (s * (1.0 + z * (1.0 - s)))
        return jnp.where(own_ref[...] > 0.5, d, 0.0), xhat

    def second_slope(c_ref, st_in, p_ref, go_ref, t_ref, st_ref, token_ref, own_ref):
        token_ref[...] = jnp.zeros(token_ref.shape, F32)
        fill_own(own_ref)
        moment = moments(st_in, 0)

        def step(g, sums):
            d, xhat = slope_two(c_ref, moment, p_ref, go_ref, own_ref, lane_at(g))
            return add_up(sums, d, xhat)

        rows = lax.fori_loop(0, inner_groups, step, (zero(), zero()))
        send(st_ref, rows, t_ref)

    def second_delta(bound, c_ref, st_in, p_ref, go_ref, sums_in, after, d_ref, t_ref, z_ref, own_ref):
        del after
        fill_own(own_ref)
        moment = moments(st_in, 0)
        scale = p_ref[2:3, :] * moment[1]
        sum_d, sum_x = gathered(sums_in, 0, chan) / voxels, gathered(sums_in, 1, chan) / voxels

        def step(g, carry):
            at = lane_at(g)
            d, xhat = slope_two(c_ref, moment, p_ref, go_ref, own_ref, at)
            out = scale * (d - sum_d - xhat * sum_x)
            d_ref[:, at] = jnp.where(own_ref[...] > 0.5, out, 0.0).astype(BF)
            return carry

        lax.fori_loop(0, inner_groups, step, 0)
        for x in range(span_x):
            base = SEAM + x * pitch
            t_ref[x * span_z : (x + 1) * span_z, :] = d_ref[base : base + span_z, :]
            z_tiles(bound, t_ref, x, 0, z_ref)

    def second_taps(d_ref, h_far, gw_ref, h_ref, acc, sem):
        copy = pltpu.make_async_copy(h_far, h_ref, sem)
        copy.start()
        acc[...] = jnp.zeros(acc.shape, F32)
        gw_ref[...] = jnp.zeros(gw_ref.shape, F32)
        copy.wait()

        def taps(g, carry):
            tap_products(d_ref[:, lane_at(g)].astype(F32), h_ref, 0, g, pitch, acc)
            return carry

        lax.fori_loop(0, inner_groups, taps, 0)
        fold_taps(acc, gw_ref, 0, chan, 0)

    def first_slope(w_ref, c_ref, st_in, p_ref, more, gw_two, x_far, *refs):
        pieces, rest = refs[:6], refs[6:]
        d1_out, st_ref, pad_ref, own_ref, band, x_ref, acc, gw_ref, d1_ref, sem, sems = rest
        copy = pltpu.make_async_copy(x_far, x_ref, sem)
        copy.start()
        fill_own(own_ref)
        assemble(pad_ref, 0, pieces)
        fill_band(band, w_ref, 2, 2)
        mean, rstd = moments(st_in, 0)
        acc[...] = jnp.zeros(acc.shape, F32)
        gw_ref[...] = jnp.zeros(gw_ref.shape, F32)
        copy.wait()

        def step(g, sums):
            at = lane_at(g)
            xhat = (c_ref[:, at] - mean) * rstd
            z = p_ref[0:1, :] * xhat + p_ref[1:2, :]
            s = sigmoid(z)
            d = band_conv(pad_ref, band, g, po, pitch) * (s * (1.0 + z * (1.0 - s)))
            d1_ref[:, at] = d
            column(d1_ref, d1_out, sems, g).start()
            mine = jnp.where(own(own_ref, g), d[pitch : pitch + si], 0.0)
            tap_products(mine, x_ref, pitch, g, pitch, acc)
            return add_up(sums, mine, xhat[pitch : pitch + si])

        rows = lax.fori_loop(0, outer_groups, step, (zero(), zero()))
        fold_taps(acc, gw_ref, 0, chan, 2)
        send(st_ref, list(rows) + [more[0:1, :], more[1:2, :]], gw_ref, gw_two)
        columns(d1_ref, d1_out, sems)

    def first_delta(bound, s_far, c_ref, st_in, p_ref, sums_in, w_ref, after, dx_ref, s_ref, d_ref, o_ref, in_ref, band, sem):
        del after
        copy = pltpu.make_async_copy(s_far, s_ref, sem)
        copy.start()
        fill_inside(bound, in_ref)
        fill_band(band, w_ref, 3, 0)
        copy.wait()
        sum_d, sum_x = gathered(sums_in, 0, chan) / voxels, gathered(sums_in, 1, chan) / voxels
        mean, rstd = moments(st_in, 0)
        scale = p_ref[0:1, :] * rstd

        def step(g, carry):
            at = lane_at(g)
            xhat = (c_ref[:, at] - mean) * rstd
            out = scale * (s_ref[:, at] - sum_d - xhat * sum_x)
            d_ref[:, at] = jnp.where(inside(bound, in_ref, g), out, 0.0).astype(BF)
            return carry

        lax.fori_loop(0, outer_groups, step, 0)

        def conv(g, carry):
            o_ref[:, lane_at(g)] = band_conv(d_ref, band, g, pi, pitch).astype(BF)
            return carry

        lax.fori_loop(0, inner_groups, conv, 0)
        order = order_matrix(chan, span_y)
        for x in range(span_x):
            at = SEAM + x * pitch
            dx_ref[:, x] = native(o_ref[at : at + span_z, :], order)

    def mix(bound, st_in, p_ref, plain_ref, early_ref, late_ref, out_ref, token_ref):
        token_ref[...] = jnp.zeros(token_ref.shape, F32)
        sum_d, sum_x = gathered(late_ref, 0, chan) / voxels, gathered(late_ref, 1, chan) / voxels
        scale = p_ref[0:1, :] * moments(st_in, 0)[1]
        row = lax.broadcasted_iota(jnp.int32, (hold, LANES), 0) + bound[8] * hold
        lane = lax.broadcasted_iota(jnp.int32, (hold, LANES), 1)

        def of_row(value):
            return jnp.sum(jnp.where(lane == row % chan, value, 0.0), axis=1, keepdims=True)

        def part(ref, i):
            return jnp.sum(ref[:, 1 + i * hold : 1 + (i + 1) * hold, :], axis=0)

        plain = jnp.sum(plain_ref[:, 1:3, :], axis=0)
        plain = jnp.where(row // chan == bound[8] * hold // chan, plain[0:1, :], plain[1:2, :])
        one = of_row(scale) * (
            part(late_ref, 0) - of_row(sum_d) * plain - of_row(sum_x) * part(early_ref, 0)
        )
        out = jnp.concatenate([one, part(late_ref, 1)], axis=0) * factor
        spare = out_ref.shape[1] - out.shape[0]
        if spare:
            out = jnp.concatenate([out, jnp.zeros((spare, LANES), F32)], axis=0)
        out_ref[...] = jnp.broadcast_to(out.astype(BF)[None], out_ref.shape)

    def last(got_ref, one_ref, two_ref, flat):
        for i, out in enumerate((one_ref, two_ref)):
            for d in range(world):
                flat[d * hold : (d + 1) * hold, :] = got_ref[d, i * hold : (i + 1) * hold, :].astype(F32)
            for at in range(27):
                row, lane = divmod(at, per)
                block = flat[row * chan : (row + 1) * chan, lane * chan : (lane + 1) * chan]
                out[at // 9, at // 3 % 3, at % 3] = block

    def out_a(c_ref, st_in, st_two, p_ref, after, y_ref, n_ref, h_ref):
        del after
        for row, (ref, at) in enumerate(((st_in, 1), (st_in, 0), (st_two, 1), (st_two, 0))):
            n_ref[row : row + 1, :] = factor * gathered(ref, at, chan)[:, :chan]
        order = order_matrix(chan, span_y)
        mean, rstd = moments(st_in, 2)

        def act(g, carry):
            at = lane_at(g)
            z = p_ref[2:3, :] * ((c_ref[:, at] - mean) * rstd) + p_ref[3:4, :]
            h_ref[:, at] = (z * sigmoid(z)).astype(BF)
            return carry

        lax.fori_loop(0, inner_groups, act, 0)
        for x in range(span_x):
            at = SEAM + x * pitch
            y_ref[:, x] = native(h_ref[at : at + span_z, :], order)


    vols, tiles_z = kernel_call(
        turn_in,
        "turn_in",
        [shape((2 * flat_rows, line), BF), shape((edges, 2 * span_x * SEAM, line), BF)],
        [bounds, x_a, x_b],
        scratch=[
            pltpu.VMEM((2 * span_x, chan, span_y, span_z), BF),
            pltpu.SemaphoreType.DMA((2 * span_x,)),
        ],
        smem=1,
        far=(1, 2),
    )
    pieces = halo(vols, tiles_z, 2, params)
    (cot,) = kernel_call(
        turn_cot, "turn_cot", [shape((si, line), BF)], [grad_out], work=1 << 27
    )
    wide_scratch = pltpu.VMEM((sw, wide), BF)
    one_copy = pltpu.SemaphoreType.DMA
    mid_scratch = pltpu.VMEM((so, mid), F32)
    group_copies = pltpu.SemaphoreType.DMA((outer_groups,))
    acc_scratch = pltpu.VMEM((3, 3 * LANES, 2 * LANES), F32)
    c1_b, pad_b, stats, plain = kernel_call(
        first_conv_b,
        "first_conv_b",
        [shape((so, mid), F32), shape((sw, wide), BF), stat_shape(1), token_shape],
        [weights] + pieces,
        scratch=[wide_scratch, own_scratch, band_scratch, one_copy],
        far_out=(1,),
        work=1 << 30,
    )
    stats_one = exchange(stats)
    c1_a, local_a = kernel_call(
        first_conv_a,
        "first_conv_a",
        [shape((so, mid), F32), shape((8, LANES), F32)],
        [weights, plain] + pieces,
        scratch=[wide_scratch, mid_scratch, own_scratch, band_scratch, group_copies],
        far_out=(0,),
        work=1 << 32,
    )
    hidden_b, c2_b, stats, token = kernel_call(
        second_conv_b,
        "second_conv_b",
        [shape((so, mid), BF), shape((si, line), F32), stat_shape(3), token_shape],
        [bounds, c1_b, weights, stats_one, params, local_a, plain],
        scratch=[pltpu.VMEM((so, mid), BF), own_scratch, in_scratch, band_scratch, one_copy],
        smem=1,
        far_out=(0,),
        work=1 << 30,
    )
    stats_two = exchange(stats)
    (taps_early,) = kernel_call(
        early_taps,
        "early_taps",
        [shape((world * hold, LANES), F32)],
        [c1_b, stats_one, pad_b, token],
        scratch=[wide_scratch, acc_scratch, own_scratch, one_copy],
        far=(2,),
        work=1 << 32,
    )
    stats, token = kernel_call(
        second_slope,
        "second_slope",
        [stat_shape(1 + hold), token_shape],
        [c2_b, stats_two, params, cot, taps_early],
        scratch=[own_scratch],
        work=1 << 27,
    )
    sums_two = exchange(stats)
    c2_a, local_a = kernel_call(
        second_conv_a,
        "second_conv_a",
        [shape((si, line), F32), shape((8, LANES), F32)],
        [bounds, c1_a, weights, stats_two, params, token],
        scratch=[mid_scratch, pltpu.VMEM((so, mid), BF), own_scratch, in_scratch, band_scratch, one_copy],
        smem=1,
        far=(1,),
        work=1 << 32,
    )
    delta_two, block, tiles_z = kernel_call(
        second_delta,
        "second_delta",
        [
            shape((si, line), BF),
            shape((flat_rows, line), BF),
            shape((edges, span_x * SEAM, line), BF),
        ],
        [bounds, c2_b, stats_two, params, cot, sums_two, local_a],
        scratch=[own_scratch],
        smem=1,
        work=1 << 27,
    )
    (taps_two,) = kernel_call(
        second_taps,
        "second_taps",
        [shape((world * hold, LANES), F32)],
        [delta_two, hidden_b],
        scratch=[pltpu.VMEM((so, mid), BF), acc_scratch, one_copy],
        far=(1,),
        work=1 << 32,
    )
    pieces = halo(block, tiles_z, 1, local_a)
    slope, stats = kernel_call(
        first_slope,
        "first_slope",
        [shape((so, mid), F32), stat_shape(1 + 2 * hold)],
        [weights, c1_b, stats_one, params, local_a, taps_two, pad_b] + pieces,
        scratch=[
            wide_scratch,
            own_scratch,
            band_scratch,
            wide_scratch,
            acc_scratch,
            pltpu.VMEM((world * hold, LANES), F32),
            mid_scratch,
            one_copy,
            group_copies,
        ],
        far=(6,),
        far_out=(0,),
        work=1 << 30,
    )
    sums_one = exchange(stats)
    whole, token = kernel_call(
        mix,
        "mix",
        [shape((world, -(-2 * hold // 8) * 8, LANES), BF), token_shape],
        [bounds, stats_one, params, stats_two, sums_two, sums_one],
        smem=1,
    )
    whole = exchange(whole)
    (dx_b,) = kernel_call(
        first_delta,
        "first_delta",
        [shape(x_a.shape, BF)],
        [bounds, slope, c1_b, stats_one, params, sums_one, weights, token],
        scratch=[
            mid_scratch,
            pltpu.VMEM((so, mid), BF),
            pltpu.VMEM((si, line), BF),
            in_scratch,
            band_scratch,
            one_copy,
        ],
        smem=1,
        far=(1,),
        work=1 << 31,
    )
    y_a, grad_norm = kernel_call(
        out_a,
        "out_a",
        [shape(x_a.shape, BF), shape((4, chan), F32)],
        [c2_a, sums_one, sums_two, params, token],
        scratch=[pltpu.VMEM((si, line), BF)],
        work=1 << 31,
    )
    weight_shape = shape((3, 3, 3, chan, chan), F32)
    grad_one, grad_two = kernel_call(
        last,
        "last",
        [weight_shape, weight_shape],
        [whole],
        scratch=[pltpu.VMEM((world * hold, LANES), F32)],
    )
    return (y_a, dx_b, grad_one, grad_two, grad_norm)


def solution(mesh):
    block = P(None, "gx", "gy", "gz")
    placed = (block, block, P(), P(), P(), P(), P(), P(), block)
    return jax.shard_map(
        body,
        mesh=mesh,
        in_specs=placed,
        out_specs=(block, block, P(), P(), P()),
        check_vma=False,
    )
```

```python
import math

import jax
import jax.numpy as jnp
from jax import lax
from jax.experimental import pallas as pl
from jax.experimental.pallas import tpu as pltpu
from jax.sharding import PartitionSpec as P


EPSILON = 1e-05
AXES = ("gx", "gy", "gz")
LANES = 128
SEAM = 16
BF = jnp.bfloat16
F32 = jnp.float32
VM = pl.BlockSpec(memory_space=pltpu.VMEM)
SM = pl.BlockSpec(memory_space=pltpu.SMEM)
HB = pl.BlockSpec(memory_space=pltpu.HBM)


def kernel_call(body, out_shape, args, scratch=(), smem=0, work=0, far=(), far_out=(), home=()):
    args = [
        pltpu.with_memory_space_constraint(a, pltpu.HBM) if i in far else a
        for i, a in enumerate(args)
    ]
    out_shape = [
        pltpu.HBM(o.shape, o.dtype) if i in far_out or i in home else o
        for i, o in enumerate(out_shape)
    ]
    return pl.pallas_call(
        body,
        out_shape=out_shape,
        in_specs=[SM if i < smem else HB if i in far else VM for i in range(len(args))],
        out_specs=[HB if i in far_out else VM for i in range(len(out_shape))],
        scratch_shapes=list(scratch),
        cost_estimate=pl.CostEstimate(flops=work, bytes_accessed=1 << 20, transcendentals=0),
        compiler_params=pltpu.CompilerParams(vmem_limit_bytes=12 << 20),
    )(*args)


def shape(dims, kind):
    return jax.ShapeDtypeStruct(dims, kind)


def exchange(spread_rows):
    return lax.all_to_all(spread_rows, AXES, 0, 0)


def neighbours(axis):
    count = lax.axis_size(axis)
    forward = [(i, i + 1) for i in range(count - 1)]
    return forward, [(t, s) for s, t in forward]


def order_matrix(chan, rows, start, lanes):
    k = lax.broadcasted_iota(jnp.int32, (chan * rows, lanes), 0)
    n = lax.broadcasted_iota(jnp.int32, (chan * rows, lanes), 1)
    return (n == (k % rows) * chan + k // rows + start).astype(BF)


def lane_at(group):
    return pl.ds(pl.multiple_of(group * LANES, LANES), LANES)


def band_conv(src, weight, group, planes, pitch):
    size = planes * pitch + SEAM
    at = pl.multiple_of(group * LANES, LANES)
    parts = [src[pl.ds(d * pitch, size), pl.ds(at, 2 * LANES)] for d in range(3)]
    out = jnp.dot(jnp.concatenate(parts, axis=1), weight[...], preferred_element_type=F32)
    return (
        pltpu.roll(out[:, :LANES], 1, 0)
        + out[:, LANES : 2 * LANES]
        + pltpu.roll(out[:, 2 * LANES :], size - 1, 0)
    )


def tap_products(d_rows, h_ref, start, group, pitch, acc):
    size = d_rows.shape[0]
    three = jnp.concatenate(
        [pltpu.roll(d_rows, size - 1, 0), d_rows, pltpu.roll(d_rows, 1, 0)], axis=1
    )
    left = three.T.astype(BF)
    at = pl.multiple_of(group * LANES, LANES)
    for d in range(3):
        right = h_ref[pl.ds(start + d * pitch, size), pl.ds(at, 2 * LANES)]
        acc[d] = acc[d] + jnp.dot(left, right, preferred_element_type=F32)


def fold_taps(acc, out, first, chan, offset):
    per = LANES // chan
    for d in range(3):
        for t in range(3):
            rows = sum(
                acc[
                    d,
                    t * LANES + j * chan : t * LANES + (j + 1) * chan,
                    (j + offset) * chan : (j + offset + 3) * chan,
                ]
                for j in range(per)
            )
            for y in range(3):
                row, lane = divmod((d * 3 + y) * 3 + t, per)
                out[
                    first + row * chan : first + (row + 1) * chan, lane * chan : (lane + 1) * chan
                ] = rows[:, y * chan : (y + 1) * chan].astype(out.dtype)


def fold_lanes(value, chan):
    step = chan
    while step < LANES:
        value = value + pltpu.roll(value, step, 1)
        step *= 2
    return value


def packed(sums, chan):
    lane = lax.broadcasted_iota(jnp.int32, (1, LANES), 1)
    out = jnp.zeros((1, LANES), F32)
    for k, value in enumerate(sums):
        out = jnp.where(lane // chan == k, fold_lanes(value, chan), out)
    return out


def gathered(ref, k, chan):
    total = jnp.sum(ref[:, 0, :], axis=0, keepdims=True)
    lane = lax.broadcasted_iota(jnp.int32, (1, LANES), 1)
    return fold_lanes(jnp.where(lane // chan == k, total, 0.0), chan)


def sigmoid(value):
    return 0.5 + 0.5 * jnp.tanh(0.5 * value)


def body(x_a, x_b, w_first, w_second, gain_first, bias_first, gain_second, bias_second, grad_out):
    chan, span_x, span_y, span_z = x_a.shape
    world = lax.axis_size("gx") * lax.axis_size("gy") * lax.axis_size("gz")
    voxels = float(span_x * span_y * span_z * world)
    factor = 1.0 / math.sqrt(voxels)
    per = LANES // chan
    line = span_y * chan
    tiles = line // LANES
    pitch = span_z + SEAM
    inner_groups = span_y // per
    outer_groups = inner_groups + 1
    b_groups = inner_groups + 2
    wide = line + 3 * LANES
    begin = 2 * LANES
    mid = outer_groups * LANES
    mid_b = b_groups * LANES
    base_b, base_a, base_two, base_one = -5, -1, -2, -1
    po, pi = span_x + 2, span_x
    so, si, sw = po * pitch + SEAM, pi * pitch + SEAM, (span_x + 4) * pitch + SEAM
    flat_rows = span_x * span_z
    seams = (span_x + 1) * SEAM
    strip_at = (0, si + tiles * seams)
    strip_rows = strip_at[1] + 2 * si + tiles * seams
    swap = lax.axis_size("gz") == 2
    tap_rows = -(-27 // per) * chan
    hold = -(-tap_rows // world)
    edges = 1 if swap else 2

    def limits(axis, low, high, reach):
        at, count = lax.axis_index(axis), lax.axis_size(axis)
        return [
            jnp.where(at == 0, low, low - reach),
            jnp.where(at == count - 1, high, high + reach),
        ]

    bounds = jnp.stack(
        limits("gx", 1, span_x + 1, 1)
        + limits("gy", 0, span_y, 3)
        + limits("gz", 0, span_z, 3)
        + [lax.axis_index("gz"), lax.axis_index("gy") % 2, lax.axis_index(AXES)]
    ).astype(jnp.int32)


    def fill_inside(bound, ref, planes):
        row = lax.broadcasted_iota(jnp.int32, ref.shape, 0) + (pitch - SEAM + 4)
        plane = row // pitch - 1
        z = row % pitch - 4
        ok = (plane >= planes[0]) & (plane < planes[1]) & (z >= bound[4]) & (z < bound[5])
        ref[...] = ok.astype(F32)

    def inside(bound, ref, group, base):
        lane = lax.broadcasted_iota(jnp.int32, ref.shape, 1) + group * LANES
        y = lane // chan + base
        return (ref[...] > 0.5) & (y >= bound[2]) & (y < bound[3])

    def fill_own(ref):
        row = lax.broadcasted_iota(jnp.int32, (si, LANES), 0)
        ref[...] = ((row >= SEAM) & ((row - SEAM + pitch) % pitch < span_z)).astype(F32)

    def own(ref, group, base):
        lane = lax.broadcasted_iota(jnp.int32, (si, LANES), 1) + group * LANES
        y = lane // chan + base
        return (ref[...] > 0.5) & (y >= 0) & (y < span_y)

    own_scratch = pltpu.VMEM((si, LANES), F32)
    in_scratch = pltpu.VMEM((so, LANES), F32)


    def prepare(w1_ref, w2_ref, g1_ref, b1_ref, g2_ref, b2_ref, c_ref, p_ref, w1, w2, v, sems):
        copies = [
            pltpu.make_async_copy(source, dest, sems.at[i])
            for i, (source, dest) in enumerate(
                ((w1_ref, w1), (w2_ref, w2))
                + tuple((r, v.at[i : i + 1]) for i, r in enumerate((g1_ref, b1_ref, g2_ref, b2_ref)))
            )
        ]
        for copy in copies:
            copy.start()
        c_ref[...] = jnp.zeros(c_ref.shape, BF)
        p_ref[...] = jnp.zeros(p_ref.shape, F32)
        for copy in copies:
            copy.wait()
        for j in range(per):
            p_ref[0:4, j * chan : (j + 1) * chan] = v[0:4, 0:chan]
        for kind, (w, back) in enumerate(((w1, False), (w2, False), (w2, True), (w1, True))):
            for dx in range(3):
                for dy in range(3):
                    for dz in range(3):
                        if back:
                            block = w[2 - dx, 2 - dy, 2 - dz]
                        else:
                            block = w[dx, dy, dz].astype(F32).T.astype(BF)
                        row = ((kind * 3 + dx) * 3 + dy) * chan
                        c_ref[row : row + chan, dz * chan : (dz + 1) * chan] = block

    class Band:
        def __init__(self, band, part, sem, far, kind):
            self.band, self.part = band, part
            rows = 9 * chan
            self.copy = pltpu.make_async_copy(far.at[pl.ds(kind * rows, rows)], part, sem)
            self.copy.start()

        def fill(self, offset):
            self.band[...] = jnp.zeros(self.band.shape, BF)
            self.copy.wait()
            fill_band(self.band, self.part, offset)
            return self.band

    def fill_band(band, c_ref, offset):
        for dx in range(3):
            at = dx * 3 * chan
            for dz in range(3):
                block = c_ref[at : at + 3 * chan, dz * chan : (dz + 1) * chan]
                for j in range(per):
                    row = (dx * 2 * per + j + offset) * chan
                    lane = dz * LANES + j * chan
                    band[row : row + 3 * chan, lane : lane + chan] = block

    band_scratch = (
        pltpu.VMEM((6 * LANES, 3 * LANES), BF),
        pltpu.VMEM((9 * chan, LANES), BF),
        pltpu.SemaphoreType.DMA,
    )
    token_shape = shape((8, LANES), F32)
    vectors = (gain_first, bias_first, gain_second, bias_second)
    weights, params = kernel_call(
        prepare,
        [shape((4 * 9 * chan, LANES), BF), token_shape],
        [w_first, w_second] + [v.reshape(1, chan) for v in vectors],
        scratch=[
            pltpu.VMEM(w_first.shape, BF),
            pltpu.VMEM(w_second.shape, BF),
            pltpu.VMEM((8, chan), F32),
            pltpu.SemaphoreType.DMA((6,)),
        ],
        far=range(6),
        home=(0,),
        work=1 << 31,
    )


    def turned(block, order):
        return lax.dot_general(
            block.reshape(chan * span_y, span_z),
            order,
            (((0,), (0,)), ((), ())),
            preferred_element_type=F32,
        ).astype(BF)

    def native(value, order):
        return lax.dot_general(
            order, value, (((1,), (1,)), ((), ())), preferred_element_type=F32
        ).astype(BF).reshape(chan, span_y, span_z)

    def turn_in(bound, a_ref, b_ref, go_ref, t_ref, g_ref, z_ref, buf, sems):
        copies = [
            pltpu.make_async_copy(ref.at[:, x], buf.at[v * span_x + x], sems.at[v * span_x + x])
            for v, ref in enumerate((a_ref, b_ref, go_ref))
            for x in range(span_x)
        ]
        for copy in copies:
            copy.start()
        order = order_matrix(chan, span_y, 0, line)
        moved = order_matrix(chan, span_y, 2 * chan, mid)
        z_ref[...] = jnp.zeros(z_ref.shape, BF)
        for v in range(3):
            dest, lanes = (t_ref, line) if v < 2 else (g_ref, mid)
            for x in range(span_x):
                at = v * span_x + x
                row = (at % (2 * span_x)) * span_z
                copies[at].wait()
                dest[row : row + span_z, :] = turned(buf[at], order if v < 2 else moved)
                first = dest[row : row + SEAM, :]
                last = dest[row + span_z - SEAM : row + span_z, :]
                rows = slice(at * SEAM, (at + 1) * SEAM)
                if swap:
                    pick = jnp.full(first.shape, bound[6], jnp.int32) == 0
                    z_ref[0, rows, :lanes] = jnp.where(
                        pick, last.astype(F32), first.astype(F32)
                    ).astype(BF)
                else:
                    z_ref[0, rows, :lanes] = last
                    z_ref[1, rows, :lanes] = first


    def halo(block, cot_block, tiles_z, token):
        forward_x, backward_x = neighbours("gx")
        forward_z, backward_z = neighbours("gz")
        rows_y = lax.axis_size("gy")
        pairs_y = [
            [p for i in range(first, rows_y - 1, 2) for p in ((i, i + 1), (i + 1, i))]
            for first in range(2)
        ]
        if swap:
            got_z = [lax.ppermute(tiles_z[0], "gz", [(0, 1), (1, 0)])]
        else:
            got_z = [
                lax.ppermute(tiles_z[0], "gz", forward_z),
                lax.ppermute(tiles_z[1], "gz", backward_z),
            ]
        from_low = lax.ppermute(block, "gx", forward_x)
        from_high = lax.ppermute(block, "gx", backward_x)

        def edge(bound, t_ref, g_ref, *refs):
            got, (a_ref, b_ref, s_ref) = refs[:edges], refs[edges:]
            row = lax.broadcasted_iota(jnp.int32, (SEAM, mid), 0)
            even = jnp.full((SEAM, LANES), bound[7], jnp.int32) == 0
            even_block = jnp.full((span_z, LANES), bound[7], jnp.int32) == 0

            def choose(rows, low, high, ok):
                low, high = low.astype(F32), high.astype(F32)
                a_ref[rows, :] = jnp.where(ok, high, low).astype(BF)
                b_ref[rows, :] = jnp.where(ok, low, high).astype(BF)

            for v in range(3):
                source, lanes = (t_ref, line) if v < 2 else (g_ref, mid)
                for x in range(span_x + 1):
                    tile = jnp.zeros((SEAM, mid), F32)
                    if x < span_x:
                        at = (v * span_x + x) * SEAM
                        value = got[0][at : at + SEAM, :].astype(F32)
                        ok = row >= SEAM - 4
                        if swap:
                            ok = ok & (jnp.full(row.shape, bound[6], jnp.int32) == 1)
                        tile = jnp.where(ok, value, tile)
                    if x > 0:
                        at = (v * span_x + x - 1) * SEAM
                        value = got[-1][at : at + SEAM, :].astype(F32)
                        ok = row < 4
                        if swap:
                            ok = ok & (jnp.full(row.shape, bound[6], jnp.int32) == 0)
                        tile = jnp.where(ok, value, tile)
                    tile = tile.astype(BF)
                    s_ref[v * seams + x * SEAM : v * seams + (x + 1) * SEAM, :] = tile
                    base = v * si + x * pitch
                    choose(
                        slice(base, base + SEAM),
                        tile[:, :LANES],
                        tile[:, lanes - LANES : lanes],
                        even,
                    )
                    if x < span_x:
                        at = ((v * span_x + x) % (2 * span_x)) * span_z
                        own_rows = slice(at, at + span_z)
                        choose(
                            slice(base + SEAM, base + pitch),
                            source[own_rows, :LANES],
                            source[own_rows, lanes - LANES : lanes],
                            even_block,
                        )

        send_a, send_b, seam_rows = kernel_call(
            edge,
            [shape((3 * si, LANES), BF)] * 2 + [shape((3 * seams, mid), BF)],
            [bounds, block, cot_block] + got_z,
            smem=1,
        )
        got_a = lax.ppermute(send_a, "gy", pairs_y[0])
        got_b = lax.ppermute(send_b, "gy", pairs_y[1])

        def strips(bound, a_ref, b_ref, s_ref, g_ref, token_ref, o_ref, f_ref):
            del token_ref
            lane = lax.broadcasted_iota(jnp.int32, (si, LANES), 1)
            even = jnp.full(lane.shape, bound[7], jnp.int32) == 0

            def both(v):
                a = a_ref[v * si : (v + 1) * si, :].astype(F32)
                b = b_ref[v * si : (v + 1) * si, :].astype(F32)
                return jnp.where(even, b, a), jnp.where(even, a, b)

            low, high = both(0)
            o_ref[0:si, :] = jnp.where(lane < 2 * chan, high, low).astype(BF)
            low, high = both(1)
            at = strip_at[1]
            o_ref[at : at + si, :] = low.astype(BF)
            o_ref[at + si : at + 2 * si, :] = high.astype(BF)
            for v, first in enumerate((si, at + 2 * si)):
                for t in range(tiles):
                    o_ref[first + t * seams : first + (t + 1) * seams, :] = s_ref[
                        v * seams : (v + 1) * seams, t * LANES : (t + 1) * LANES
                    ]
            low, high = both(2)
            for x in range(span_x + 1):
                f_ref[x * pitch : x * pitch + SEAM, :] = s_ref[
                    2 * seams + x * SEAM : 2 * seams + (x + 1) * SEAM, :
                ]
                if x < span_x:
                    f_ref[x * pitch + SEAM : (x + 1) * pitch, :] = g_ref[
                        x * span_z : (x + 1) * span_z, :
                    ]
            f_ref[:, :LANES] = jnp.where(
                lane < 2 * chan, low, f_ref[:, :LANES].astype(F32)
            ).astype(BF)
            f_ref[:, mid - LANES :] = jnp.where(
                lane >= 2 * chan, high, f_ref[:, mid - LANES :].astype(F32)
            ).astype(BF)

        mine, cot_frame = kernel_call(
            strips,
            [shape((strip_rows, LANES), BF), shape((si, mid), BF)],
            [bounds, got_a, got_b, seam_rows, cot_block, token],
            smem=1,
        )
        return [
            from_low,
            block,
            from_high,
            lax.ppermute(mine, "gx", forward_x),
            mine,
            lax.ppermute(mine, "gx", backward_x),
        ], cot_frame

    def joiner(dest):
        waiting = {}

        def put(seam, columns, value):
            key = (seam, columns)
            if key in waiting:
                dest[seam : seam + SEAM, columns[0] : columns[1]] = waiting.pop(key) + value
            else:
                waiting[key] = value

        def finish():
            for (seam, columns), value in waiting.items():
                dest[seam : seam + SEAM, columns[0] : columns[1]] = value

        return put, finish

    def assemble(dest, v, pieces):
        blocks, strip_refs = pieces[:3], pieces[3:]
        lane = lax.broadcasted_iota(jnp.int32, (si, LANES), 1)
        put, finish = joiner(dest)
        dest[:, :LANES] = jnp.zeros((sw, LANES), BF)
        last = si - SEAM
        for b in range(3):
            base = b * span_x * pitch
            for x in range(span_x):
                at = base + SEAM + x * pitch
                rows = slice((v * span_x + x) * span_z, (v * span_x + x + 1) * span_z)
                dest[at : at + span_z, begin : begin + line] = blocks[b][rows, :]
            first = strip_at[v]
            if v == 0:
                ys = strip_refs[b][first : first + si, :].astype(F32)
                low = jnp.where(lane >= 2 * chan, ys, 0.0).astype(BF)
                high = jnp.where(lane < 2 * chan, ys, 0.0).astype(BF)
                first += si
            else:
                low = strip_refs[b][first : first + si, :]
                high = strip_refs[b][first + si : first + 2 * si, :]
                first += 2 * si
            for columns, value in (((LANES, begin), low), ((begin + line, wide), high)):
                dest[base + SEAM : base + last, columns[0] : columns[1]] = value[SEAM:last]
                put(base, columns, value[:SEAM])
                put(base + last, columns, value[last:])
            for t in range(tiles):
                at = first + t * seams
                columns = (begin + LANES * t, begin + LANES * (t + 1))
                for x in range(span_x + 1):
                    value = strip_refs[b][at + x * SEAM : at + (x + 1) * SEAM, :]
                    seam = base + x * pitch
                    if 0 < x < span_x:
                        dest[seam : seam + SEAM, columns[0] : columns[1]] = value
                    else:
                        put(seam, columns, value)
        finish()

    def assemble_delta(dest, frames):
        put, finish = joiner(dest)
        dest[:, mid:] = jnp.zeros((sw, LANES), BF)
        last = si - SEAM
        for b in range(3):
            base = b * span_x * pitch
            dest[base + SEAM : base + last, :mid] = frames[b][SEAM:last, :]
            put(base, (0, mid), frames[b][:SEAM, :])
            put(base + last, (0, mid), frames[b][last:, :])
        finish()


    def stat_shape(rows):
        return shape((world, rows, LANES), F32)

    def send(ref, sums, *parts):
        ref[:, 0:1, :] = jnp.broadcast_to(packed(sums, chan)[None], (world, 1, LANES))
        for i, part in enumerate(parts):
            for d in range(world):
                ref[d, 1 + i * hold : 1 + (i + 1) * hold, :] = part[d * hold : (d + 1) * hold, :]

    def moments(st_ref, row):
        mean = gathered(st_ref, row, chan) / voxels
        var = gathered(st_ref, row + 1, chan) / voxels - mean * mean
        return mean, lax.rsqrt(var + EPSILON)

    def add_up(sums, value, other):
        return (
            sums[0] + jnp.sum(value, axis=0, keepdims=True),
            sums[1] + jnp.sum(value * other, axis=0, keepdims=True),
        )

    def conv_one_of(first, groups, base, band, dest, c_ref, own_ref, to=None):
        fill_own(own_ref)
        band = band.fill(2)

        def step(g, sums):
            out = band_conv(dest, band, g + first, po, pitch)
            c_ref[:, lane_at(g)] = out
            if to is not None:
                column(c_ref, to[0], to[1], g).start()
            mine = jnp.where(own(own_ref, g, base), out[pitch : pitch + si], 0.0)
            return add_up(sums, mine, mine)

        return lax.fori_loop(0, groups, step, (zero(), zero()))

    def zero():
        return jnp.zeros((1, LANES), F32)

    def first_conv_b(w_ref, *refs):
        pieces, rest = refs[:6], refs[6:]
        c_ref, x_out, a_out, st_ref, m_ref, x_ref, a_ref, own_ref, *band, sems = rest
        band = Band(*band, w_ref, 0)
        copies = [
            pltpu.make_async_copy(a_ref, a_out, sems.at[0]),
            pltpu.make_async_copy(x_ref, x_out, sems.at[1]),
        ]
        assemble(a_ref, 0, pieces)
        copies[0].start()
        assemble(x_ref, 1, pieces)
        copies[1].start()
        send(st_ref, conv_one_of(0, b_groups, base_b, band, x_ref, c_ref, own_ref))
        plain_taps(x_ref, m_ref)
        for copy in copies:
            copy.wait()

    def first_conv_a(w_ref, after, x_far, c_out, st_ref, x_ref, c_ref, own_ref, band, part, wait, sem, sems):
        del after
        band = Band(band, part, wait, w_ref, 0)
        copy = pltpu.make_async_copy(x_far, x_ref, sem)
        copy.start()
        st_ref[...] = jnp.zeros(st_ref.shape, F32)
        copy.wait()
        to = (c_out, sems)
        rows = conv_one_of(1, outer_groups, base_a, band, x_ref, c_ref, own_ref, to)
        for k in range(2):
            st_ref[k : k + 1, :] = rows[k]
        columns(c_ref, c_out, sems)

    def column(source, dest, sems, g):
        return pltpu.make_async_copy(source.at[:, lane_at(g)], dest.at[:, lane_at(g)], sems.at[g])

    def columns(source, dest, sems):
        def wait(g, carry):
            column(source, dest, sems, g).wait()
            return carry

        lax.fori_loop(0, outer_groups, wait, 0)

    def conv_two_of(bound, c_ref, st_in, k, p_ref, h_ref, c2_ref, own_ref, in_ref, band, shifts, after=None):
        groups, base, out_groups, out_base, offset = shifts
        fill_own(own_ref)
        fill_inside(bound, in_ref, (bound[0], bound[1]))
        mean, rstd = moments(st_in, k)
        gain, bias = p_ref[0:1, :], p_ref[1:2, :]

        def act(g, carry):
            at = lane_at(g)
            z = gain * ((c_ref[:, at] - mean) * rstd) + bias
            h = jnp.where(inside(bound, in_ref, g, base), z * sigmoid(z), 0.0)
            h_ref[:, at] = h.astype(BF)
            return carry

        lax.fori_loop(0, groups, act, 0)
        if after is not None:
            after.start()
        band = band.fill(offset)

        def step(g, sums):
            out = band_conv(h_ref, band, g, pi, pitch)
            c2_ref[:, lane_at(g)] = out
            mine = jnp.where(own(own_ref, g, out_base), out, 0.0)
            return add_up(sums, mine, mine)

        return lax.fori_loop(0, out_groups, step, (zero(), zero()))

    def second_conv_b(bound, c_ref, w_ref, st_in, p_ref, more, m_ref, h_out, c2_ref, st_ref, token_ref, h_ref, own_ref, in_ref, band, part, wait, sem):
        band = Band(band, part, wait, w_ref, 1)
        token_ref[...] = jnp.zeros(token_ref.shape, F32)
        copy = pltpu.make_async_copy(h_ref, h_out, sem)
        shifts = (b_groups, base_b, outer_groups, base_two, 2)
        rows = conv_two_of(bound, c_ref, st_in, 0, p_ref, h_ref, c2_ref, own_ref, in_ref, band, shifts, copy)
        send(st_ref, list(rows) + [more[0:1, :], more[1:2, :]])
        for d in range(world):
            for k in range(2):
                row = min(d * hold // chan + k, m_ref.shape[0] - 1)
                st_ref[d, 1 + k : 2 + k, :] = m_ref[row : row + 1, :]
        copy.wait()

    def second_conv_a(bound, c_far, w_ref, st_in, p_ref, after, c2_ref, st_ref, c_ref, h_ref, own_ref, in_ref, band, part, wait, sem):
        del after
        band = Band(band, part, wait, w_ref, 1)
        shifts = (outer_groups, base_a, inner_groups, 0, 0)
        copy = pltpu.make_async_copy(c_far, c_ref, sem)
        copy.start()
        copy.wait()
        rows = conv_two_of(bound, c_ref, st_in, 2, p_ref, h_ref, c2_ref, own_ref, in_ref, band, shifts)
        st_ref[...] = jnp.concatenate(list(rows) + [jnp.zeros((6, LANES), F32)], axis=0)

    def early_taps(c_ref, st_in, x_far, after, t_ref, x_ref, acc, own_ref, sem):
        del after
        copy = pltpu.make_async_copy(x_far, x_ref, sem)
        copy.start()
        fill_own(own_ref)
        mean, rstd = moments(st_in, 0)
        acc[...] = jnp.zeros(acc.shape, F32)
        copy.wait()

        def step(g, carry):
            xhat = (c_ref[pl.ds(pitch, si), lane_at(g + 1)] - mean) * rstd
            mine = jnp.where(own(own_ref, g, base_one), xhat, 0.0)
            tap_products(mine, x_ref, pitch, g + 1, pitch, acc)
            return carry

        lax.fori_loop(0, outer_groups, step, 0)
        t_ref[...] = jnp.zeros(t_ref.shape, F32)
        fold_taps(acc, t_ref, 0, chan, 2)

    def plain_taps(x_ref, m_ref):
        m_ref[...] = jnp.zeros(m_ref.shape, F32)
        row = lax.broadcasted_iota(jnp.int32, (8, si), 0)
        at = lax.broadcasted_iota(jnp.int32, (8, si), 1)
        pick = jnp.zeros((8, si), F32)
        for x in range(span_x):
            for t in range(3):
                low = SEAM + x * pitch + t - 1
                pick = jnp.where((row == t) & (at >= low) & (at < low + span_z), 1.0, pick)
        pick = pick.astype(BF)
        for d in range(3):
            cols = jnp.dot(
                pick, x_ref[pl.ds((1 + d) * pitch, si), :], preferred_element_type=F32
            )
            for y in range(3):
                low = begin + (y - 1) * chan
                own_cols = cols[:, low : low + line]
                total = sum(own_cols[:, k * LANES : (k + 1) * LANES] for k in range(tiles))
                total = fold_lanes(total, chan)
                for t in range(3):
                    group, place = divmod((d * 3 + y) * 3 + t, per)
                    m_ref[group : group + 1, place * chan : (place + 1) * chan] = total[
                        t : t + 1, place * chan : (place + 1) * chan
                    ]

    def slope_two(c_ref, moment, p_ref, go_ref, at):
        mean, rstd = moment
        xhat = (c_ref[:, at] - mean) * rstd
        z = p_ref[2:3, :] * xhat + p_ref[3:4, :]
        s = sigmoid(z)
        d = go_ref[:, at].astype(F32) * (s * (1.0 + z * (1.0 - s)))
        return d, xhat

    def second_slope(c_ref, st_in, p_ref, go_ref, t_ref, st_ref, token_ref, own_ref):
        token_ref[...] = jnp.zeros(token_ref.shape, F32)
        fill_own(own_ref)
        moment = moments(st_in, 0)

        def step(g, sums):
            d, xhat = slope_two(c_ref, moment, p_ref, go_ref, lane_at(g))
            return add_up(sums, jnp.where(own(own_ref, g, base_two), d, 0.0), xhat)

        rows = lax.fori_loop(0, outer_groups, step, (zero(), zero()))
        send(st_ref, rows, t_ref)

    def second_delta(bound, c_ref, st_in, p_ref, go_ref, sums_in, after, d_ref, in_ref):
        del after
        fill_inside(bound, in_ref, (0, span_x))
        moment = moments(st_in, 0)
        scale = p_ref[2:3, :] * moment[1]
        sum_d, sum_x = gathered(sums_in, 0, chan) / voxels, gathered(sums_in, 1, chan) / voxels

        def step(g, carry):
            at = lane_at(g)
            d, xhat = slope_two(c_ref, moment, p_ref, go_ref, at)
            out = scale * (d - sum_d - xhat * sum_x)
            d_ref[:, at] = jnp.where(inside(bound, in_ref, g, base_two), out, 0.0).astype(BF)
            return carry

        lax.fori_loop(0, outer_groups, step, 0)

    def second_taps(d_ref, h_far, gw_ref, h_ref, acc, own_ref, sem):
        copy = pltpu.make_async_copy(h_far, h_ref, sem)
        copy.start()
        fill_own(own_ref)
        acc[...] = jnp.zeros(acc.shape, F32)
        gw_ref[...] = jnp.zeros(gw_ref.shape, F32)
        copy.wait()

        def taps(g, carry):
            mine = jnp.where(own(own_ref, g, base_two), d_ref[:, lane_at(g)].astype(F32), 0.0)
            tap_products(mine, h_ref, 0, g, pitch, acc)
            return carry

        lax.fori_loop(0, outer_groups, taps, 0)
        fold_taps(acc, gw_ref, 0, chan, 2)

    def first_slope(w_ref, c_ref, st_in, p_ref, more, gw_two, x_far, *refs):
        frames, rest = refs[:3], refs[3:]
        d1_out, st_ref, pad_ref, own_ref, *band, x_ref, acc, gw_ref, d1_ref, sem, sems = rest
        band = Band(*band, w_ref, 2)
        copy = pltpu.make_async_copy(x_far, x_ref, sem)
        copy.start()
        fill_own(own_ref)
        assemble_delta(pad_ref, frames)
        band = band.fill(0)
        mean, rstd = moments(st_in, 0)
        acc[...] = jnp.zeros(acc.shape, F32)
        gw_ref[...] = jnp.zeros(gw_ref.shape, F32)
        copy.wait()

        def step(g, sums):
            at = lane_at(g)
            xhat = (c_ref[:, lane_at(g + 1)] - mean) * rstd
            z = p_ref[0:1, :] * xhat + p_ref[1:2, :]
            s = sigmoid(z)
            d = band_conv(pad_ref, band, g, po, pitch) * (s * (1.0 + z * (1.0 - s)))
            d1_ref[:, at] = d
            column(d1_ref, d1_out, sems, g).start()
            mine = jnp.where(own(own_ref, g, base_one), d[pitch : pitch + si], 0.0)
            tap_products(mine, x_ref, pitch, g + 1, pitch, acc)
            return add_up(sums, mine, xhat[pitch : pitch + si])

        rows = lax.fori_loop(0, outer_groups, step, (zero(), zero()))
        fold_taps(acc, gw_ref, 0, chan, 2)
        send(st_ref, list(rows) + [more[0:1, :], more[1:2, :]], gw_ref, gw_two)
        columns(d1_ref, d1_out, sems)

    def first_delta(bound, s_far, c_ref, st_in, p_ref, sums_in, w_ref, after, dx_ref, s_ref, d_ref, o_ref, in_ref, band, part, wait, sem):
        del after
        band = Band(band, part, wait, w_ref, 3)
        copy = pltpu.make_async_copy(s_far, s_ref, sem)
        copy.start()
        fill_inside(bound, in_ref, (bound[0], bound[1]))
        band = band.fill(0)
        copy.wait()
        sum_d, sum_x = gathered(sums_in, 0, chan) / voxels, gathered(sums_in, 1, chan) / voxels
        mean, rstd = moments(st_in, 0)
        scale = p_ref[0:1, :] * rstd

        def step(g, carry):
            at = lane_at(g)
            xhat = (c_ref[:, lane_at(g + 1)] - mean) * rstd
            out = scale * (s_ref[:, at] - sum_d - xhat * sum_x)
            d_ref[:, at] = jnp.where(inside(bound, in_ref, g, base_one), out, 0.0).astype(BF)
            return carry

        lax.fori_loop(0, outer_groups, step, 0)

        def conv(g, carry):
            o_ref[:, lane_at(g)] = band_conv(d_ref, band, g, pi, pitch).astype(BF)
            return carry

        lax.fori_loop(0, inner_groups, conv, 0)
        order = order_matrix(chan, span_y, 0, line)
        for x in range(span_x):
            at = SEAM + x * pitch
            dx_ref[:, x] = native(o_ref[at : at + span_z, :], order)

    def mix(bound, st_in, p_ref, plain_ref, early_ref, late_ref, out_ref, token_ref):
        token_ref[...] = jnp.zeros(token_ref.shape, F32)
        sum_d, sum_x = gathered(late_ref, 0, chan) / voxels, gathered(late_ref, 1, chan) / voxels
        scale = p_ref[0:1, :] * moments(st_in, 0)[1]
        row = lax.broadcasted_iota(jnp.int32, (hold, LANES), 0) + bound[8] * hold
        lane = lax.broadcasted_iota(jnp.int32, (hold, LANES), 1)

        def of_row(value):
            return jnp.sum(jnp.where(lane == row % chan, value, 0.0), axis=1, keepdims=True)

        def part(ref, i):
            return jnp.sum(ref[:, 1 + i * hold : 1 + (i + 1) * hold, :], axis=0)

        plain = jnp.sum(plain_ref[:, 1:3, :], axis=0)
        plain = jnp.where(row // chan == bound[8] * hold // chan, plain[0:1, :], plain[1:2, :])
        one = of_row(scale) * (
            part(late_ref, 0) - of_row(sum_d) * plain - of_row(sum_x) * part(early_ref, 0)
        )
        out = jnp.concatenate([one, part(late_ref, 1)], axis=0) * factor
        spare = out_ref.shape[1] - out.shape[0]
        if spare:
            out = jnp.concatenate([out, jnp.zeros((spare, LANES), F32)], axis=0)
        out_ref[...] = jnp.broadcast_to(out.astype(BF)[None], out_ref.shape)

    def last(got_ref, one_ref, two_ref, flat):
        for i, out in enumerate((one_ref, two_ref)):
            for d in range(world):
                flat[d * hold : (d + 1) * hold, :] = got_ref[d, i * hold : (i + 1) * hold, :].astype(F32)
            for at in range(27):
                row, lane = divmod(at, per)
                block = flat[row * chan : (row + 1) * chan, lane * chan : (lane + 1) * chan]
                out[at // 9, at // 3 % 3, at % 3] = block

    def out_a(c_ref, st_in, st_two, p_ref, after, y_ref, n_ref, h_ref):
        del after
        for row, (ref, at) in enumerate(((st_in, 1), (st_in, 0), (st_two, 1), (st_two, 0))):
            n_ref[row : row + 1, :] = factor * gathered(ref, at, chan)[:, :chan]
        order = order_matrix(chan, span_y, 0, line)
        mean, rstd = moments(st_in, 2)

        def act(g, carry):
            at = lane_at(g)
            z = p_ref[2:3, :] * ((c_ref[:, at] - mean) * rstd) + p_ref[3:4, :]
            h_ref[:, at] = (z * sigmoid(z)).astype(BF)
            return carry

        lax.fori_loop(0, inner_groups, act, 0)
        for x in range(span_x):
            at = SEAM + x * pitch
            y_ref[:, x] = native(h_ref[at : at + span_z, :], order)


    vols, cot_block, tiles_z = kernel_call(
        turn_in,
        [
            shape((2 * flat_rows, line), BF),
            shape((flat_rows, mid), BF),
            shape((edges, 3 * span_x * SEAM, mid), BF),
        ],
        [bounds, x_a, x_b, grad_out],
        scratch=[
            pltpu.VMEM((3 * span_x, chan, span_y, span_z), BF),
            pltpu.SemaphoreType.DMA((3 * span_x,)),
        ],
        smem=1,
        far=(1, 2, 3),
    )
    pieces, cot = halo(vols, cot_block, tiles_z, params)
    wide_scratch = pltpu.VMEM((sw, wide), BF)
    one_copy = pltpu.SemaphoreType.DMA
    mid_scratch = pltpu.VMEM((so, mid), F32)
    group_copies = pltpu.SemaphoreType.DMA((outer_groups,))
    acc_scratch = pltpu.VMEM((3, 3 * LANES, 2 * LANES), F32)
    c1_b, pad_b, pad_a, stats, plain = kernel_call(
        first_conv_b,
        [shape((so, mid_b), F32)] + [shape((sw, wide), BF)] * 2 + [stat_shape(1), token_shape],
        [weights] + pieces,
        scratch=[
            wide_scratch,
            wide_scratch,
            own_scratch,
            *band_scratch,
            pltpu.SemaphoreType.DMA((2,)),
        ],
        far=(0,),
        far_out=(1, 2),
        home=(3,),
        work=1 << 30,
    )
    stats_one = exchange(stats)
    c1_a, local_a = kernel_call(
        first_conv_a,
        [shape((so, mid), F32), shape((8, LANES), F32)],
        [weights, plain, pad_a],
        scratch=[wide_scratch, mid_scratch, own_scratch, *band_scratch, one_copy, group_copies],
        far=(0, 2),
        far_out=(0,),
        work=1 << 32,
    )
    hidden_b, c2_b, stats, token = kernel_call(
        second_conv_b,
        [shape((so, mid_b), BF), shape((si, mid), F32), stat_shape(3), token_shape],
        [bounds, c1_b, weights, stats_one, params, local_a, plain],
        scratch=[pltpu.VMEM((so, mid_b), BF), own_scratch, in_scratch, *band_scratch, one_copy],
        smem=1,
        far_out=(0,),
        home=(2,),
        far=(2,),
        work=1 << 30,
    )
    stats_two = exchange(stats)
    (taps_early,) = kernel_call(
        early_taps,
        [shape((world * hold, LANES), F32)],
        [c1_b, stats_one, pad_b, token],
        scratch=[wide_scratch, acc_scratch, own_scratch, one_copy],
        far=(2,),
        work=1 << 32,
    )
    stats, token = kernel_call(
        second_slope,
        [stat_shape(1 + hold), token_shape],
        [c2_b, stats_two, params, cot, taps_early],
        scratch=[own_scratch],
        home=(0,),
        work=1 << 27,
    )
    sums_two = exchange(stats)
    c2_a, local_a = kernel_call(
        second_conv_a,
        [shape((si, line), F32), shape((8, LANES), F32)],
        [bounds, c1_a, weights, stats_two, params, token],
        scratch=[mid_scratch, pltpu.VMEM((so, mid), BF), own_scratch, in_scratch, *band_scratch, one_copy],
        smem=1,
        far=(1, 2),
        work=1 << 32,
    )
    (delta_two,) = kernel_call(
        second_delta,
        [shape((si, mid), BF)],
        [bounds, c2_b, stats_two, params, cot, sums_two, local_a],
        scratch=[pltpu.VMEM((si, LANES), F32)],
        smem=1,
        work=1 << 27,
    )
    (taps_two,) = kernel_call(
        second_taps,
        [shape((world * hold, LANES), F32)],
        [delta_two, hidden_b],
        scratch=[pltpu.VMEM((so, mid_b), BF), acc_scratch, own_scratch, one_copy],
        far=(1,),
        work=1 << 32,
    )
    forward_x, backward_x = neighbours("gx")
    frames = [
        lax.ppermute(delta_two, "gx", forward_x),
        delta_two,
        lax.ppermute(delta_two, "gx", backward_x),
    ]
    slope, stats = kernel_call(
        first_slope,
        [shape((so, mid), F32), stat_shape(1 + 2 * hold)],
        [weights, c1_b, stats_one, params, local_a, taps_two, pad_b] + frames,
        scratch=[
            pltpu.VMEM((sw, mid + LANES), BF),
            own_scratch,
            *band_scratch,
            wide_scratch,
            acc_scratch,
            pltpu.VMEM((world * hold, LANES), F32),
            mid_scratch,
            one_copy,
            group_copies,
        ],
        far=(0, 6),
        far_out=(0,),
        home=(1,),
        work=1 << 30,
    )
    sums_one = exchange(stats)
    whole, token = kernel_call(
        mix,
        [shape((world, -(-2 * hold // 8) * 8, LANES), BF), token_shape],
        [bounds, stats_one, params, stats_two, sums_two, sums_one],
        smem=1,
    )
    whole = exchange(whole)
    (dx_b,) = kernel_call(
        first_delta,
        [shape(x_a.shape, BF)],
        [bounds, slope, c1_b, stats_one, params, sums_one, weights, token],
        scratch=[
            mid_scratch,
            pltpu.VMEM((so, mid), BF),
            pltpu.VMEM((si, line), BF),
            in_scratch,
            *band_scratch,
            one_copy,
        ],
        smem=1,
        far=(1, 6),
        work=1 << 31,
    )
    y_a, grad_norm = kernel_call(
        out_a,
        [shape(x_a.shape, BF), shape((4, chan), F32)],
        [c2_a, sums_one, sums_two, params, token],
        scratch=[pltpu.VMEM((si, line), BF)],
        work=1 << 31,
    )
    weight_shape = shape((3, 3, 3, chan, chan), F32)
    grad_one, grad_two = kernel_call(
        last,
        [weight_shape, weight_shape],
        [whole],
        scratch=[pltpu.VMEM((world * hold, LANES), F32)],
    )
    return (y_a, dx_b, grad_one, grad_two, grad_norm)


def solution(mesh):
    block = P(None, "gx", "gy", "gz")
    placed = (block, block, P(), P(), P(), P(), P(), P(), block)

    return jax.shard_map(
        body,
        mesh=mesh,
        in_specs=placed,
        out_specs=(block, block, P(), P(), P()),
        check_vma=False,
    )
```

```python
import math

import jax
import jax.numpy as jnp
from jax import lax
from jax.experimental import pallas as pl
from jax.experimental.pallas import tpu as pltpu
from jax.sharding import PartitionSpec as P


EPSILON = 1e-05
AXES = ("gx", "gy", "gz")
LANES = 128
SEAM = 16
BF = jnp.bfloat16
F32 = jnp.float32
VM = pl.BlockSpec(memory_space=pltpu.VMEM)
SM = pl.BlockSpec(memory_space=pltpu.SMEM)
HB = pl.BlockSpec(memory_space=pltpu.HBM)


def kernel_call(body, out_shape, args, scratch=(), smem=0, work=0, far=(), far_out=(), home=()):
    args = [
        pltpu.with_memory_space_constraint(a, pltpu.HBM) if i in far else a
        for i, a in enumerate(args)
    ]
    out_shape = [
        pltpu.HBM(o.shape, o.dtype) if i in far_out or i in home else o
        for i, o in enumerate(out_shape)
    ]
    return pl.pallas_call(
        body,
        out_shape=out_shape,
        in_specs=[SM if i < smem else HB if i in far else VM for i in range(len(args))],
        out_specs=[HB if i in far_out else VM for i in range(len(out_shape))],
        scratch_shapes=list(scratch),
        cost_estimate=pl.CostEstimate(flops=work, bytes_accessed=1 << 20, transcendentals=0),
        compiler_params=pltpu.CompilerParams(vmem_limit_bytes=12 << 20),
    )(*args)


def shape(dims, kind):
    return jax.ShapeDtypeStruct(dims, kind)


def exchange(spread_rows):
    return lax.all_to_all(spread_rows, AXES, 0, 0)


def neighbours(axis):
    count = lax.axis_size(axis)
    forward = [(i, i + 1) for i in range(count - 1)]
    return forward, [(t, s) for s, t in forward]


def order_matrix(chan, rows, start, lanes):
    k = lax.broadcasted_iota(jnp.int32, (chan * rows, lanes), 0)
    n = lax.broadcasted_iota(jnp.int32, (chan * rows, lanes), 1)
    return (n == (k % rows) * chan + k // rows + start).astype(BF)


def lane_at(group):
    if isinstance(group, int):
        return slice(group * LANES, (group + 1) * LANES)
    return pl.ds(pl.multiple_of(group * LANES, LANES), LANES)


def band_conv(src, weight, group, planes, pitch):
    size = planes * pitch + SEAM
    at = pl.multiple_of(group * LANES, LANES)
    parts = [src[pl.ds(d * pitch, size), pl.ds(at, 2 * LANES)] for d in range(3)]
    out = jnp.dot(jnp.concatenate(parts, axis=1), weight[...], preferred_element_type=F32)
    return (
        pltpu.roll(out[:, :LANES], 1, 0)
        + out[:, LANES : 2 * LANES]
        + pltpu.roll(out[:, 2 * LANES :], size - 1, 0)
    )


def tap_products(groups, h_ref, start, first, pitch):
    size = groups[0].shape[0]
    left, right = [], []
    for g, rows in enumerate(groups):
        left.append(
            jnp.concatenate(
                [pltpu.roll(rows, size - 1, 0), rows, pltpu.roll(rows, 1, 0)], axis=1
            ).astype(BF)
        )
        at = (first + g) * LANES
        right.append(
            jnp.concatenate(
                [
                    h_ref[start + d * pitch : start + d * pitch + size, at : at + 2 * LANES]
                    for d in range(3)
                ],
                axis=1,
            )
        )
    return lax.dot_general(
        jnp.concatenate(left, axis=0),
        jnp.concatenate(right, axis=0),
        (((0,), (0,)), ((), ())),
        preferred_element_type=F32,
    )


def fold_taps(acc, out, first, chan, offset):
    per = LANES // chan
    for d in range(3):
        for t in range(3):
            rows = sum(
                acc[
                    t * LANES + j * chan : t * LANES + (j + 1) * chan,
                    d * 2 * LANES + (j + offset) * chan : d * 2 * LANES + (j + offset + 3) * chan,
                ]
                for j in range(per)
            )
            for y in range(3):
                row, lane = divmod((d * 3 + y) * 3 + t, per)
                out[
                    first + row * chan : first + (row + 1) * chan, lane * chan : (lane + 1) * chan
                ] = rows[:, y * chan : (y + 1) * chan].astype(out.dtype)


def fold_lanes(value, chan):
    step = chan
    while step < LANES:
        value = value + pltpu.roll(value, step, 1)
        step *= 2
    return value


def packed(sums, chan):
    lane = lax.broadcasted_iota(jnp.int32, (1, LANES), 1)
    out = jnp.zeros((1, LANES), F32)
    for k, value in enumerate(sums):
        out = jnp.where(lane // chan == k, fold_lanes(value, chan), out)
    return out


def gathered(ref, k, chan):
    total = jnp.sum(ref[:, 0, :], axis=0, keepdims=True)
    lane = lax.broadcasted_iota(jnp.int32, (1, LANES), 1)
    return fold_lanes(jnp.where(lane // chan == k, total, 0.0), chan)


def sigmoid(value):
    return 0.5 + 0.5 * jnp.tanh(0.5 * value)


def body(x_a, x_b, w_first, w_second, gain_first, bias_first, gain_second, bias_second, grad_out):
    chan, span_x, span_y, span_z = x_a.shape
    world = lax.axis_size("gx") * lax.axis_size("gy") * lax.axis_size("gz")
    voxels = float(span_x * span_y * span_z * world)
    factor = 1.0 / math.sqrt(voxels)
    per = LANES // chan
    line = span_y * chan
    tiles = line // LANES
    pitch = span_z + SEAM
    inner_groups = span_y // per
    outer_groups = inner_groups + 1
    b_groups = inner_groups + 2
    wide = line + 3 * LANES
    begin = 2 * LANES
    mid = outer_groups * LANES
    mid_b = b_groups * LANES
    base_b, base_a, base_two, base_one = -5, -1, -2, -1
    po, pi = span_x + 2, span_x
    so, si, sw = po * pitch + SEAM, pi * pitch + SEAM, (span_x + 4) * pitch + SEAM
    flat_rows = span_x * span_z
    seams = (span_x + 1) * SEAM
    packs = span_x * SEAM
    strip_at = (0, si + tiles * packs)
    strip_rows = strip_at[1] + 2 * si + tiles * packs
    swap = lax.axis_size("gz") == 2
    tap_rows = -(-27 // per) * chan
    hold = -(-tap_rows // world)
    edges = 1 if swap else 2

    def limits(axis, low, high, reach):
        at, count = lax.axis_index(axis), lax.axis_size(axis)
        return [
            jnp.where(at == 0, low, low - reach),
            jnp.where(at == count - 1, high, high + reach),
        ]

    bounds = jnp.stack(
        limits("gx", 1, span_x + 1, 1)
        + limits("gy", 0, span_y, 3)
        + limits("gz", 0, span_z, 3)
        + [lax.axis_index("gz"), lax.axis_index("gy") % 2, lax.axis_index(AXES)]
    ).astype(jnp.int32)


    def fill_inside(bound, ref, planes):
        row = lax.broadcasted_iota(jnp.int32, ref.shape, 0) + (pitch - SEAM + 4)
        plane = row // pitch - 1
        z = row % pitch - 4
        ok = (plane >= planes[0]) & (plane < planes[1]) & (z >= bound[4]) & (z < bound[5])
        ref[...] = ok.astype(F32)

    def inside(bound, ref, group, base):
        lane = lax.broadcasted_iota(jnp.int32, ref.shape, 1) + group * LANES
        y = lane // chan + base
        return (ref[...] > 0.5) & (y >= bound[2]) & (y < bound[3])

    def fill_own(ref):
        row = lax.broadcasted_iota(jnp.int32, (si, LANES), 0)
        ref[...] = ((row >= SEAM) & ((row - SEAM + pitch) % pitch < span_z)).astype(F32)

    def own(ref, group, base):
        lane = lax.broadcasted_iota(jnp.int32, (si, LANES), 1) + group * LANES
        y = lane // chan + base
        return (ref[...] > 0.5) & (y >= 0) & (y < span_y)

    own_scratch = pltpu.VMEM((si, LANES), F32)
    in_scratch = pltpu.VMEM((so, LANES), F32)


    def prepare(w1_ref, w2_ref, g1_ref, b1_ref, g2_ref, b2_ref, c_ref, p_ref, w1, w2, v, sems):
        copies = [
            pltpu.make_async_copy(source, dest, sems.at[i])
            for i, (source, dest) in enumerate(
                ((w1_ref, w1), (w2_ref, w2))
                + tuple((r, v.at[i : i + 1]) for i, r in enumerate((g1_ref, b1_ref, g2_ref, b2_ref)))
            )
        ]
        for copy in copies:
            copy.start()
        c_ref[...] = jnp.zeros(c_ref.shape, BF)
        p_ref[...] = jnp.zeros(p_ref.shape, F32)
        for copy in copies:
            copy.wait()
        for j in range(per):
            p_ref[0:4, j * chan : (j + 1) * chan] = v[0:4, 0:chan]
        for kind, (w, back) in enumerate(((w1, False), (w2, False), (w2, True), (w1, True))):
            for dx in range(3):
                for dy in range(3):
                    for dz in range(3):
                        if back:
                            block = w[2 - dx, 2 - dy, 2 - dz]
                        else:
                            block = w[dx, dy, dz].astype(F32).T.astype(BF)
                        row = ((kind * 3 + dx) * 3 + dy) * chan
                        c_ref[row : row + chan, dz * chan : (dz + 1) * chan] = block

    class Band:
        def __init__(self, band, part, sem, far, kind):
            self.band, self.part = band, part
            rows = 9 * chan
            self.copy = pltpu.make_async_copy(far.at[pl.ds(kind * rows, rows)], part, sem)
            self.copy.start()

        def fill(self, offset):
            self.band[...] = jnp.zeros(self.band.shape, BF)
            self.copy.wait()
            fill_band(self.band, self.part, offset)
            return self.band

    def fill_band(band, c_ref, offset):
        for dx in range(3):
            at = dx * 3 * chan
            for dz in range(3):
                block = c_ref[at : at + 3 * chan, dz * chan : (dz + 1) * chan]
                for j in range(per):
                    row = (dx * 2 * per + j + offset) * chan
                    lane = dz * LANES + j * chan
                    band[row : row + 3 * chan, lane : lane + chan] = block

    band_scratch = (
        pltpu.VMEM((6 * LANES, 3 * LANES), BF),
        pltpu.VMEM((9 * chan, LANES), BF),
        pltpu.SemaphoreType.DMA,
    )
    token_shape = shape((8, LANES), F32)
    vectors = (gain_first, bias_first, gain_second, bias_second)
    weights, params = kernel_call(
        prepare,
        [shape((4 * 9 * chan, LANES), BF), token_shape],
        [w_first, w_second] + [v.reshape(1, chan) for v in vectors],
        scratch=[
            pltpu.VMEM(w_first.shape, BF),
            pltpu.VMEM(w_second.shape, BF),
            pltpu.VMEM((8, chan), F32),
            pltpu.SemaphoreType.DMA((6,)),
        ],
        far=range(6),
        home=(0,),
        work=1 << 31,
    )


    def turned(block, order):
        return lax.dot_general(
            block.reshape(chan * span_y, span_z),
            order,
            (((0,), (0,)), ((), ())),
            preferred_element_type=F32,
        ).astype(BF)

    def native(value, order):
        return lax.dot_general(
            order, value, (((1,), (1,)), ((), ())), preferred_element_type=F32
        ).astype(BF).reshape(chan, span_y, span_z)

    def turn_in(bound, a_ref, b_ref, go_ref, t_ref, g_ref, z_ref, buf, sems):
        copies = [
            pltpu.make_async_copy(ref.at[:, x], buf.at[v * span_x + x], sems.at[v * span_x + x])
            for v, ref in enumerate((a_ref, b_ref, go_ref))
            for x in range(span_x)
        ]
        for copy in copies:
            copy.start()
        order = order_matrix(chan, span_y, 0, line)
        moved = order_matrix(chan, span_y, 2 * chan, mid)
        z_ref[...] = jnp.zeros(z_ref.shape, BF)
        for v in range(3):
            dest, lanes = (t_ref, line) if v < 2 else (g_ref, mid)
            for x in range(span_x):
                at = v * span_x + x
                row = (at % (2 * span_x)) * span_z
                copies[at].wait()
                dest[row : row + span_z, :] = turned(buf[at], order if v < 2 else moved)
                first = dest[row : row + SEAM, :]
                last = dest[row + span_z - SEAM : row + span_z, :]
                rows = slice(at * SEAM, (at + 1) * SEAM)
                if swap:
                    pick = jnp.full(first.shape, bound[6], jnp.int32) == 0
                    z_ref[0, rows, :lanes] = jnp.where(
                        pick, last.astype(F32), first.astype(F32)
                    ).astype(BF)
                else:
                    z_ref[0, rows, :lanes] = last
                    z_ref[1, rows, :lanes] = first


    def halo(block, cot_block, tiles_z, token):
        forward_x, backward_x = neighbours("gx")
        forward_z, backward_z = neighbours("gz")
        rows_y = lax.axis_size("gy")
        pairs_y = [
            [p for i in range(first, rows_y - 1, 2) for p in ((i, i + 1), (i + 1, i))]
            for first in range(2)
        ]
        if swap:
            got_z = [lax.ppermute(tiles_z[0], "gz", [(0, 1), (1, 0)])]
        else:
            got_z = [
                lax.ppermute(tiles_z[0], "gz", forward_z),
                lax.ppermute(tiles_z[1], "gz", backward_z),
            ]
        from_low = lax.ppermute(block, "gx", forward_x)
        from_high = lax.ppermute(block, "gx", backward_x)

        def edge(bound, t_ref, g_ref, *refs):
            got, (a_ref, b_ref, s_ref) = refs[:edges], refs[edges:]
            row = lax.broadcasted_iota(jnp.int32, (SEAM, mid), 0)
            even = jnp.full((SEAM, LANES), bound[7], jnp.int32) == 0
            even_block = jnp.full((span_z, LANES), bound[7], jnp.int32) == 0

            def choose(rows, low, high, ok):
                low, high = low.astype(F32), high.astype(F32)
                a_ref[rows, :] = jnp.where(ok, high, low).astype(BF)
                b_ref[rows, :] = jnp.where(ok, low, high).astype(BF)

            def tile_of(v, x):
                tile = jnp.zeros((SEAM, mid), F32)
                if x < span_x:
                    at = (v * span_x + x) * SEAM
                    value = got[0][at : at + SEAM, :].astype(F32)
                    ok = row >= SEAM - 4
                    if swap:
                        ok = ok & (jnp.full(row.shape, bound[6], jnp.int32) == 1)
                    tile = jnp.where(ok, value, tile)
                if x > 0:
                    at = (v * span_x + x - 1) * SEAM
                    value = got[-1][at : at + SEAM, :].astype(F32)
                    ok = row < 4
                    if swap:
                        ok = ok & (jnp.full(row.shape, bound[6], jnp.int32) == 0)
                    tile = jnp.where(ok, value, tile)
                tile = tile.astype(BF)
                s_ref[v * seams + x * SEAM : v * seams + (x + 1) * SEAM, :] = tile
                return tile

            def ends(value, v):
                lanes = line if v < 2 else mid
                return value[:, :LANES], value[:, lanes - LANES : lanes]

            def shared(values):
                (low, high), (cot_low, cot_high) = ends(values[0], 0), ends(values[1], 2)
                lane = lax.broadcasted_iota(jnp.int32, low.shape, 1)
                half = lane < 2 * chan
                return (
                    jnp.where(half, low.astype(F32), cot_low.astype(F32)),
                    jnp.where(half, cot_high.astype(F32), high.astype(F32)),
                )

            for x in range(span_x + 1):
                seam_tiles = [tile_of(v, x) for v in range(3)]
                base = x * pitch
                rows = slice(base, base + SEAM)
                choose(rows, *shared((seam_tiles[0], seam_tiles[2])), even)
                rows = slice(si + base, si + base + SEAM)
                choose(rows, *ends(seam_tiles[1], 1), even)
                if x < span_x:
                    plane = slice(x * span_z, (x + 1) * span_z)
                    rows = slice(base + SEAM, base + pitch)
                    choose(rows, *shared((t_ref[plane, :], g_ref[plane, :])), even_block)
                    plane = slice((span_x + x) * span_z, (span_x + x + 1) * span_z)
                    rows = slice(si + base + SEAM, si + base + pitch)
                    choose(rows, *ends(t_ref[plane, :], 1), even_block)

        send_a, send_b, seam_rows = kernel_call(
            edge,
            [shape((2 * si, LANES), BF)] * 2 + [shape((3 * seams, mid), BF)],
            [bounds, block, cot_block] + got_z,
            smem=1,
        )
        got_a = lax.ppermute(send_a, "gy", pairs_y[0])
        got_b = lax.ppermute(send_b, "gy", pairs_y[1])

        def strips(bound, a_ref, b_ref, s_ref, g_ref, token_ref, o_ref, f_ref):
            del token_ref
            lane = lax.broadcasted_iota(jnp.int32, (si, LANES), 1)
            even = jnp.full(lane.shape, bound[7], jnp.int32) == 0

            def both(v):
                a = a_ref[v * si : (v + 1) * si, :].astype(F32)
                b = b_ref[v * si : (v + 1) * si, :].astype(F32)
                return jnp.where(even, b, a), jnp.where(even, a, b)

            low, high = both(0)
            o_ref[0:si, :] = jnp.where(lane < 2 * chan, high, low).astype(BF)
            low, high = both(1)
            at = strip_at[1]
            o_ref[at : at + si, :] = low.astype(BF)
            o_ref[at + si : at + 2 * si, :] = high.astype(BF)
            for v, first in enumerate((si, at + 2 * si)):
                for t in range(tiles):
                    lanes = slice(t * LANES, (t + 1) * LANES)
                    at = first + t * packs
                    o_ref[at : at + SEAM, :] = (
                        s_ref[v * seams : v * seams + SEAM, lanes]
                        + s_ref[(v + 1) * seams - SEAM : (v + 1) * seams, lanes]
                    )
                    o_ref[at + SEAM : at + packs, :] = s_ref[
                        v * seams + SEAM : (v + 1) * seams - SEAM, lanes
                    ]
            low, high = both(0)
            for x in range(span_x + 1):
                f_ref[x * pitch : x * pitch + SEAM, :] = s_ref[
                    2 * seams + x * SEAM : 2 * seams + (x + 1) * SEAM, :
                ]
                if x < span_x:
                    f_ref[x * pitch + SEAM : (x + 1) * pitch, :] = g_ref[
                        x * span_z : (x + 1) * span_z, :
                    ]
            f_ref[:, :LANES] = jnp.where(
                lane < 2 * chan, low, f_ref[:, :LANES].astype(F32)
            ).astype(BF)
            f_ref[:, mid - LANES :] = jnp.where(
                lane >= 2 * chan, high, f_ref[:, mid - LANES :].astype(F32)
            ).astype(BF)

        mine, cot_frame = kernel_call(
            strips,
            [shape((strip_rows, LANES), BF), shape((si, mid), BF)],
            [bounds, got_a, got_b, seam_rows, cot_block, token],
            smem=1,
        )
        return [
            from_low,
            block,
            from_high,
            lax.ppermute(mine, "gx", forward_x),
            mine,
            lax.ppermute(mine, "gx", backward_x),
        ], cot_frame

    def joiner(dest):
        waiting = {}

        def put(seam, columns, value):
            key = (seam, columns)
            if key in waiting:
                dest[seam : seam + SEAM, columns[0] : columns[1]] = waiting.pop(key) + value
            else:
                waiting[key] = value

        def finish():
            for (seam, columns), value in waiting.items():
                dest[seam : seam + SEAM, columns[0] : columns[1]] = value

        return put, finish

    def assemble(dest, v, pieces):
        blocks, strip_refs = pieces[:3], pieces[3:]
        lane = lax.broadcasted_iota(jnp.int32, (si, LANES), 1)
        put, finish = joiner(dest)
        dest[:, :LANES] = jnp.zeros((sw, LANES), BF)
        last = si - SEAM
        for b in range(3):
            base = b * span_x * pitch
            for x in range(span_x):
                at = base + SEAM + x * pitch
                rows = slice((v * span_x + x) * span_z, (v * span_x + x + 1) * span_z)
                dest[at : at + span_z, begin : begin + line] = blocks[b][rows, :]
            first = strip_at[v]
            if v == 0:
                ys = strip_refs[b][first : first + si, :].astype(F32)
                low = jnp.where(lane >= 2 * chan, ys, 0.0).astype(BF)
                high = jnp.where(lane < 2 * chan, ys, 0.0).astype(BF)
                first += si
            else:
                low = strip_refs[b][first : first + si, :]
                high = strip_refs[b][first + si : first + 2 * si, :]
                first += 2 * si
            for columns, value in (((LANES, begin), low), ((begin + line, wide), high)):
                dest[base + SEAM : base + last, columns[0] : columns[1]] = value[SEAM:last]
                put(base, columns, value[:SEAM])
                put(base + last, columns, value[last:])
            for t in range(tiles):
                at = first + t * packs
                columns = (begin + LANES * t, begin + LANES * (t + 1))
                shared = strip_refs[b][at : at + SEAM, :].astype(F32)
                row = lax.broadcasted_iota(jnp.int32, shared.shape, 0)
                for x in range(span_x + 1):
                    if x == 0:
                        value = jnp.where(row >= SEAM - 4, shared, 0.0).astype(BF)
                    elif x == span_x:
                        value = jnp.where(row < 4, shared, 0.0).astype(BF)
                    else:
                        value = strip_refs[b][at + x * SEAM : at + (x + 1) * SEAM, :]
                    seam = base + x * pitch
                    if 0 < x < span_x:
                        dest[seam : seam + SEAM, columns[0] : columns[1]] = value
                    else:
                        put(seam, columns, value)
        finish()

    def assemble_delta(dest, frames):
        put, finish = joiner(dest)
        dest[:, mid:] = jnp.zeros((sw, LANES), BF)
        last = si - SEAM
        for b in range(3):
            base = b * span_x * pitch
            dest[base + SEAM : base + last, :mid] = frames[b][SEAM:last, :]
            put(base, (0, mid), frames[b][:SEAM, :])
            put(base + last, (0, mid), frames[b][last:, :])
        finish()


    def stat_shape(rows):
        return shape((world, rows, LANES), F32)

    def send(ref, sums, *parts):
        ref[:, 0:1, :] = jnp.broadcast_to(packed(sums, chan)[None], (world, 1, LANES))
        for i, part in enumerate(parts):
            for d in range(world):
                ref[d, 1 + i * hold : 1 + (i + 1) * hold, :] = part[d * hold : (d + 1) * hold, :]

    def moments(st_ref, row):
        mean = gathered(st_ref, row, chan) / voxels
        var = gathered(st_ref, row + 1, chan) / voxels - mean * mean
        return mean, lax.rsqrt(var + EPSILON)

    def add_up(sums, value, other):
        return (
            sums[0] + jnp.sum(value, axis=0, keepdims=True),
            sums[1] + jnp.sum(value * other, axis=0, keepdims=True),
        )

    def conv_one_of(first, groups, base, band, dest, c_ref, own_ref, to=None):
        fill_own(own_ref)
        band = band.fill(2)

        def step(g, sums):
            out = band_conv(dest, band, g + first, po, pitch)
            c_ref[:, lane_at(g)] = out
            if to is not None:
                column(c_ref, to[0], to[1], g).start()
            mine = jnp.where(own(own_ref, g, base), out[pitch : pitch + si], 0.0)
            return add_up(sums, mine, mine)

        return lax.fori_loop(0, groups, step, (zero(), zero()), unroll=True)

    def zero():
        return jnp.zeros((1, LANES), F32)

    def first_conv_b(w_ref, *refs):
        pieces, rest = refs[:6], refs[6:]
        c_ref, x_out, a_out, st_ref, m_ref, x_ref, a_ref, own_ref, *band, sems = rest
        band = Band(*band, w_ref, 0)
        copies = [
            pltpu.make_async_copy(a_ref, a_out, sems.at[0]),
            pltpu.make_async_copy(x_ref, x_out, sems.at[1]),
        ]
        assemble(a_ref, 0, pieces)
        copies[0].start()
        assemble(x_ref, 1, pieces)
        copies[1].start()
        send(st_ref, conv_one_of(0, b_groups, base_b, band, x_ref, c_ref, own_ref))
        plain_taps(x_ref, m_ref)
        for copy in copies:
            copy.wait()

    def first_conv_a(w_ref, after, x_far, c_out, st_ref, x_ref, c_ref, own_ref, band, part, wait, sem, sems):
        del after
        band = Band(band, part, wait, w_ref, 0)
        copy = pltpu.make_async_copy(x_far, x_ref, sem)
        copy.start()
        st_ref[...] = jnp.zeros(st_ref.shape, F32)
        copy.wait()
        to = (c_out, sems)
        rows = conv_one_of(1, outer_groups, base_a, band, x_ref, c_ref, own_ref, to)
        for k in range(2):
            st_ref[k : k + 1, :] = rows[k]
        columns(c_ref, c_out, sems)

    def column(source, dest, sems, g):
        return pltpu.make_async_copy(source.at[:, lane_at(g)], dest.at[:, lane_at(g)], sems.at[g])

    def columns(source, dest, sems):
        def wait(g, carry):
            column(source, dest, sems, g).wait()
            return carry

        lax.fori_loop(0, outer_groups, wait, 0, unroll=True)

    def conv_two_of(bound, c_ref, st_in, k, p_ref, h_ref, c2_ref, own_ref, in_ref, band, shifts, after=None):
        groups, base, out_groups, out_base, offset = shifts
        fill_own(own_ref)
        fill_inside(bound, in_ref, (bound[0], bound[1]))
        mean, rstd = moments(st_in, k)
        gain, bias = p_ref[0:1, :], p_ref[1:2, :]

        def act(g, carry):
            at = lane_at(g)
            z = gain * ((c_ref[:, at] - mean) * rstd) + bias
            h = jnp.where(inside(bound, in_ref, g, base), z * sigmoid(z), 0.0)
            h_ref[:, at] = h.astype(BF)
            return carry

        lax.fori_loop(0, groups, act, 0, unroll=True)
        if after is not None:
            after.start()
        band = band.fill(offset)

        def step(g, sums):
            out = band_conv(h_ref, band, g, pi, pitch)
            c2_ref[:, lane_at(g)] = out
            mine = jnp.where(own(own_ref, g, out_base), out, 0.0)
            return add_up(sums, mine, mine)

        return lax.fori_loop(0, out_groups, step, (zero(), zero()), unroll=True)

    def second_conv_b(bound, c_ref, w_ref, st_in, p_ref, more, m_ref, h_out, c2_ref, st_ref, token_ref, h_ref, own_ref, in_ref, band, part, wait, sem):
        band = Band(band, part, wait, w_ref, 1)
        token_ref[...] = jnp.zeros(token_ref.shape, F32)
        copy = pltpu.make_async_copy(h_ref, h_out, sem)
        shifts = (b_groups, base_b, outer_groups, base_two, 2)
        rows = conv_two_of(bound, c_ref, st_in, 0, p_ref, h_ref, c2_ref, own_ref, in_ref, band, shifts, copy)
        send(st_ref, list(rows) + [more[0:1, :], more[1:2, :]])
        for d in range(world):
            for k in range(2):
                row = min(d * hold // chan + k, m_ref.shape[0] - 1)
                st_ref[d, 1 + k : 2 + k, :] = m_ref[row : row + 1, :]
        copy.wait()

    def second_conv_a(bound, c_far, w_ref, st_in, p_ref, after, c2_ref, st_ref, c_ref, h_ref, own_ref, in_ref, band, part, wait, sem):
        del after
        band = Band(band, part, wait, w_ref, 1)
        shifts = (outer_groups, base_a, inner_groups, 0, 0)
        copy = pltpu.make_async_copy(c_far, c_ref, sem)
        copy.start()
        copy.wait()
        rows = conv_two_of(bound, c_ref, st_in, 2, p_ref, h_ref, c2_ref, own_ref, in_ref, band, shifts)
        st_ref[...] = jnp.concatenate(list(rows) + [jnp.zeros((6, LANES), F32)], axis=0)

    def early_taps(c_ref, st_in, x_far, after, t_ref, x_ref, acc, own_ref, sem):
        del after
        copy = pltpu.make_async_copy(x_far, x_ref, sem)
        copy.start()
        fill_own(own_ref)
        mean, rstd = moments(st_in, 0)
        copy.wait()
        groups = []
        for g in range(outer_groups):
            xhat = (c_ref[pl.ds(pitch, si), lane_at(g + 1)] - mean) * rstd
            groups.append(jnp.where(own(own_ref, g, base_one), xhat, 0.0))
        acc[...] = tap_products(groups, x_ref, pitch, 1, pitch)
        t_ref[...] = jnp.zeros(t_ref.shape, F32)
        fold_taps(acc, t_ref, 0, chan, 2)

    def plain_taps(x_ref, m_ref):
        m_ref[...] = jnp.zeros(m_ref.shape, F32)
        row = lax.broadcasted_iota(jnp.int32, (8, si), 0)
        at = lax.broadcasted_iota(jnp.int32, (8, si), 1)
        pick = jnp.zeros((8, si), F32)
        for x in range(span_x):
            for t in range(3):
                low = SEAM + x * pitch + t - 1
                pick = jnp.where((row == t) & (at >= low) & (at < low + span_z), 1.0, pick)
        pick = pick.astype(BF)
        for d in range(3):
            cols = jnp.dot(
                pick, x_ref[pl.ds((1 + d) * pitch, si), :], preferred_element_type=F32
            )
            for y in range(3):
                low = begin + (y - 1) * chan
                own_cols = cols[:, low : low + line]
                total = sum(own_cols[:, k * LANES : (k + 1) * LANES] for k in range(tiles))
                total = fold_lanes(total, chan)
                for t in range(3):
                    group, place = divmod((d * 3 + y) * 3 + t, per)
                    m_ref[group : group + 1, place * chan : (place + 1) * chan] = total[
                        t : t + 1, place * chan : (place + 1) * chan
                    ]

    def slope_two(c_ref, moment, p_ref, go_ref, at):
        mean, rstd = moment
        xhat = (c_ref[:, at] - mean) * rstd
        z = p_ref[2:3, :] * xhat + p_ref[3:4, :]
        s = sigmoid(z)
        d = go_ref[:, at].astype(F32) * (s * (1.0 + z * (1.0 - s)))
        return d, xhat

    def second_slope(c_ref, st_in, p_ref, go_ref, t_ref, st_ref, token_ref, own_ref):
        token_ref[...] = jnp.zeros(token_ref.shape, F32)
        fill_own(own_ref)
        moment = moments(st_in, 0)

        def step(g, sums):
            d, xhat = slope_two(c_ref, moment, p_ref, go_ref, lane_at(g))
            return add_up(sums, jnp.where(own(own_ref, g, base_two), d, 0.0), xhat)

        rows = lax.fori_loop(0, outer_groups, step, (zero(), zero()), unroll=True)
        send(st_ref, rows, t_ref)

    def second_delta(bound, c_ref, st_in, p_ref, go_ref, sums_in, after, d_ref, in_ref):
        del after
        fill_inside(bound, in_ref, (0, span_x))
        moment = moments(st_in, 0)
        scale = p_ref[2:3, :] * moment[1]
        sum_d, sum_x = gathered(sums_in, 0, chan) / voxels, gathered(sums_in, 1, chan) / voxels

        def step(g, carry):
            at = lane_at(g)
            d, xhat = slope_two(c_ref, moment, p_ref, go_ref, at)
            out = scale * (d - sum_d - xhat * sum_x)
            d_ref[:, at] = jnp.where(inside(bound, in_ref, g, base_two), out, 0.0).astype(BF)
            return carry

        lax.fori_loop(0, outer_groups, step, 0, unroll=True)

    def second_taps(d_ref, h_far, gw_ref, h_ref, acc, own_ref, sem):
        copy = pltpu.make_async_copy(h_far, h_ref, sem)
        copy.start()
        fill_own(own_ref)
        gw_ref[...] = jnp.zeros(gw_ref.shape, F32)
        copy.wait()
        groups = [
            jnp.where(own(own_ref, g, base_two), d_ref[:, lane_at(g)].astype(F32), 0.0)
            for g in range(outer_groups)
        ]
        acc[...] = tap_products(groups, h_ref, 0, 0, pitch)
        fold_taps(acc, gw_ref, 0, chan, 2)

    def first_slope(w_ref, c_ref, st_in, p_ref, more, gw_two, x_far, *refs):
        frames, rest = refs[:3], refs[3:]
        d1_out, st_ref, pad_ref, own_ref, *band, x_ref, acc, gw_ref, d1_ref, sem, sems = rest
        band = Band(*band, w_ref, 2)
        copy = pltpu.make_async_copy(x_far, x_ref, sem)
        copy.start()
        fill_own(own_ref)
        assemble_delta(pad_ref, frames)
        band = band.fill(0)
        mean, rstd = moments(st_in, 0)
        gw_ref[...] = jnp.zeros(gw_ref.shape, F32)
        copy.wait()
        groups = []

        def step(g, sums):
            at = lane_at(g)
            xhat = (c_ref[:, lane_at(g + 1)] - mean) * rstd
            z = p_ref[0:1, :] * xhat + p_ref[1:2, :]
            s = sigmoid(z)
            d = band_conv(pad_ref, band, g, po, pitch) * (s * (1.0 + z * (1.0 - s)))
            d1_ref[:, at] = d
            column(d1_ref, d1_out, sems, g).start()
            mine = jnp.where(own(own_ref, g, base_one), d[pitch : pitch + si], 0.0)
            groups.append(mine)
            return add_up(sums, mine, xhat[pitch : pitch + si])

        rows = (zero(), zero())
        for g in range(outer_groups):
            rows = step(g, rows)
        acc[...] = tap_products(groups, x_ref, pitch, 1, pitch)
        fold_taps(acc, gw_ref, 0, chan, 2)
        send(st_ref, list(rows) + [more[0:1, :], more[1:2, :]], gw_ref, gw_two)
        columns(d1_ref, d1_out, sems)

    def first_delta(bound, s_far, c_ref, st_in, p_ref, sums_in, w_ref, after, dx_ref, s_ref, d_ref, o_ref, in_ref, band, part, wait, sem):
        del after
        band = Band(band, part, wait, w_ref, 3)
        copy = pltpu.make_async_copy(s_far, s_ref, sem)
        copy.start()
        fill_inside(bound, in_ref, (bound[0], bound[1]))
        band = band.fill(0)
        copy.wait()
        sum_d, sum_x = gathered(sums_in, 0, chan) / voxels, gathered(sums_in, 1, chan) / voxels
        mean, rstd = moments(st_in, 0)
        scale = p_ref[0:1, :] * rstd

        def step(g, carry):
            at = lane_at(g)
            xhat = (c_ref[:, lane_at(g + 1)] - mean) * rstd
            out = scale * (s_ref[:, at] - sum_d - xhat * sum_x)
            d_ref[:, at] = jnp.where(inside(bound, in_ref, g, base_one), out, 0.0).astype(BF)
            return carry

        lax.fori_loop(0, outer_groups, step, 0, unroll=True)

        def conv(g, carry):
            o_ref[:, lane_at(g)] = band_conv(d_ref, band, g, pi, pitch).astype(BF)
            return carry

        lax.fori_loop(0, inner_groups, conv, 0, unroll=True)
        order = order_matrix(chan, span_y, 0, line)
        for x in range(span_x):
            at = SEAM + x * pitch
            dx_ref[:, x] = native(o_ref[at : at + span_z, :], order)

    def mix(bound, st_in, p_ref, plain_ref, early_ref, late_ref, out_ref, token_ref):
        token_ref[...] = jnp.zeros(token_ref.shape, F32)
        sum_d, sum_x = gathered(late_ref, 0, chan) / voxels, gathered(late_ref, 1, chan) / voxels
        scale = p_ref[0:1, :] * moments(st_in, 0)[1]
        row = lax.broadcasted_iota(jnp.int32, (hold, LANES), 0) + bound[8] * hold
        lane = lax.broadcasted_iota(jnp.int32, (hold, LANES), 1)

        def of_row(value):
            return jnp.sum(jnp.where(lane == row % chan, value, 0.0), axis=1, keepdims=True)

        def part(ref, i):
            return jnp.sum(ref[:, 1 + i * hold : 1 + (i + 1) * hold, :], axis=0)

        plain = jnp.sum(plain_ref[:, 1:3, :], axis=0)
        plain = jnp.where(row // chan == bound[8] * hold // chan, plain[0:1, :], plain[1:2, :])
        one = of_row(scale) * (
            part(late_ref, 0) - of_row(sum_d) * plain - of_row(sum_x) * part(early_ref, 0)
        )
        out = jnp.concatenate([one, part(late_ref, 1)], axis=0) * factor
        spare = out_ref.shape[1] - out.shape[0]
        if spare:
            out = jnp.concatenate([out, jnp.zeros((spare, LANES), F32)], axis=0)
        out_ref[...] = jnp.broadcast_to(out.astype(BF)[None], out_ref.shape)

    def last(got_ref, one_ref, two_ref, flat):
        for i, out in enumerate((one_ref, two_ref)):
            for d in range(world):
                flat[d * hold : (d + 1) * hold, :] = got_ref[d, i * hold : (i + 1) * hold, :].astype(F32)
            for at in range(27):
                row, lane = divmod(at, per)
                block = flat[row * chan : (row + 1) * chan, lane * chan : (lane + 1) * chan]
                out[at // 9, at // 3 % 3, at % 3] = block

    def out_a(c_ref, st_in, st_two, p_ref, after, y_ref, n_ref, h_ref):
        del after
        for row, (ref, at) in enumerate(((st_in, 1), (st_in, 0), (st_two, 1), (st_two, 0))):
            n_ref[row : row + 1, :] = factor * gathered(ref, at, chan)[:, :chan]
        order = order_matrix(chan, span_y, 0, line)
        mean, rstd = moments(st_in, 2)

        def act(g, carry):
            at = lane_at(g)
            z = p_ref[2:3, :] * ((c_ref[:, at] - mean) * rstd) + p_ref[3:4, :]
            h_ref[:, at] = (z * sigmoid(z)).astype(BF)
            return carry

        lax.fori_loop(0, inner_groups, act, 0, unroll=True)
        for x in range(span_x):
            at = SEAM + x * pitch
            y_ref[:, x] = native(h_ref[at : at + span_z, :], order)


    vols, cot_block, tiles_z = kernel_call(
        turn_in,
        [
            shape((2 * flat_rows, line), BF),
            shape((flat_rows, mid), BF),
            shape((edges, 3 * span_x * SEAM, mid), BF),
        ],
        [bounds, x_a, x_b, grad_out],
        scratch=[
            pltpu.VMEM((3 * span_x, chan, span_y, span_z), BF),
            pltpu.SemaphoreType.DMA((3 * span_x,)),
        ],
        smem=1,
        far=(1, 2, 3),
    )
    pieces, cot = halo(vols, cot_block, tiles_z, params)
    wide_scratch = pltpu.VMEM((sw, wide), BF)
    one_copy = pltpu.SemaphoreType.DMA
    mid_scratch = pltpu.VMEM((so, mid), F32)
    group_copies = pltpu.SemaphoreType.DMA((outer_groups,))
    acc_scratch = pltpu.VMEM((3 * LANES, 6 * LANES), F32)
    c1_b, pad_b, pad_a, stats, plain = kernel_call(
        first_conv_b,
        [shape((so, mid_b), F32)] + [shape((sw, wide), BF)] * 2 + [stat_shape(1), token_shape],
        [weights] + pieces,
        scratch=[
            wide_scratch,
            wide_scratch,
            own_scratch,
            *band_scratch,
            pltpu.SemaphoreType.DMA((2,)),
        ],
        far=(0,),
        far_out=(1, 2),
        home=(3,),
        work=1 << 30,
    )
    stats_one = exchange(stats)
    c1_a, local_a = kernel_call(
        first_conv_a,
        [shape((so, mid), F32), shape((8, LANES), F32)],
        [weights, plain, pad_a],
        scratch=[wide_scratch, mid_scratch, own_scratch, *band_scratch, one_copy, group_copies],
        far=(0, 2),
        far_out=(0,),
        work=1 << 32,
    )
    hidden_b, c2_b, stats, token = kernel_call(
        second_conv_b,
        [shape((so, mid_b), BF), shape((si, mid), F32), stat_shape(3), token_shape],
        [bounds, c1_b, weights, stats_one, params, local_a, plain],
        scratch=[pltpu.VMEM((so, mid_b), BF), own_scratch, in_scratch, *band_scratch, one_copy],
        smem=1,
        far_out=(0,),
        home=(2,),
        far=(2,),
        work=1 << 30,
    )
    stats_two = exchange(stats)
    (taps_early,) = kernel_call(
        early_taps,
        [shape((world * hold, LANES), F32)],
        [c1_b, stats_one, pad_b, token],
        scratch=[wide_scratch, acc_scratch, own_scratch, one_copy],
        far=(2,),
        work=1 << 32,
    )
    stats, token = kernel_call(
        second_slope,
        [stat_shape(1 + hold), token_shape],
        [c2_b, stats_two, params, cot, taps_early],
        scratch=[own_scratch],
        home=(0,),
        work=1 << 27,
    )
    sums_two = exchange(stats)
    c2_a, local_a = kernel_call(
        second_conv_a,
        [shape((si, line), F32), shape((8, LANES), F32)],
        [bounds, c1_a, weights, stats_two, params, token],
        scratch=[mid_scratch, pltpu.VMEM((so, mid), BF), own_scratch, in_scratch, *band_scratch, one_copy],
        smem=1,
        far=(1, 2),
        home=(0,),
        work=1 << 32,
    )
    (delta_two,) = kernel_call(
        second_delta,
        [shape((si, mid), BF)],
        [bounds, c2_b, stats_two, params, cot, sums_two, local_a],
        scratch=[pltpu.VMEM((si, LANES), F32)],
        smem=1,
        work=1 << 27,
    )
    (taps_two,) = kernel_call(
        second_taps,
        [shape((world * hold, LANES), F32)],
        [delta_two, hidden_b],
        scratch=[pltpu.VMEM((so, mid_b), BF), acc_scratch, own_scratch, one_copy],
        far=(1,),
        work=1 << 32,
    )
    forward_x, backward_x = neighbours("gx")
    frames = [
        lax.ppermute(delta_two, "gx", forward_x),
        delta_two,
        lax.ppermute(delta_two, "gx", backward_x),
    ]
    slope, stats = kernel_call(
        first_slope,
        [shape((so, mid), F32), stat_shape(1 + 2 * hold)],
        [weights, c1_b, stats_one, params, local_a, taps_two, pad_b] + frames,
        scratch=[
            pltpu.VMEM((sw, mid + LANES), BF),
            own_scratch,
            *band_scratch,
            wide_scratch,
            acc_scratch,
            pltpu.VMEM((world * hold, LANES), F32),
            mid_scratch,
            one_copy,
            group_copies,
        ],
        far=(0, 6),
        far_out=(0,),
        home=(1,),
        work=1 << 30,
    )
    sums_one = exchange(stats)
    whole, token = kernel_call(
        mix,
        [shape((world, -(-2 * hold // 8) * 8, LANES), BF), token_shape],
        [bounds, stats_one, params, stats_two, sums_two, sums_one],
        smem=1,
    )
    whole = exchange(whole)
    (dx_b,) = kernel_call(
        first_delta,
        [shape(x_a.shape, BF)],
        [bounds, slope, c1_b, stats_one, params, sums_one, weights, token],
        scratch=[
            mid_scratch,
            pltpu.VMEM((so, mid), BF),
            pltpu.VMEM((si, line), BF),
            in_scratch,
            *band_scratch,
            one_copy,
        ],
        smem=1,
        far=(1, 6),
        work=1 << 31,
    )
    y_a, grad_norm = kernel_call(
        out_a,
        [shape(x_a.shape, BF), shape((4, chan), F32)],
        [c2_a, sums_one, sums_two, params, token],
        scratch=[pltpu.VMEM((si, line), BF)],
        work=1 << 31,
    )
    weight_shape = shape((3, 3, 3, chan, chan), F32)
    grad_one, grad_two = kernel_call(
        last,
        [weight_shape, weight_shape],
        [whole],
        scratch=[pltpu.VMEM((world * hold, LANES), F32)],
    )
    return (y_a, dx_b, grad_one, grad_two, grad_norm)


def solution(mesh):
    block = P(None, "gx", "gy", "gz")
    placed = (block, block, P(), P(), P(), P(), P(), P(), block)

    return jax.shard_map(
        body,
        mesh=mesh,
        in_specs=placed,
        out_specs=(block, block, P(), P(), P()),
        check_vma=False,
    )
```

```python
import math

import jax
import jax.numpy as jnp
from jax import lax
from jax.experimental import pallas as pl
from jax.experimental.pallas import tpu as pltpu
from jax.sharding import PartitionSpec as P


EPSILON = 1e-05
AXES = ("gx", "gy", "gz")
LANES = 128
SEAM = 16
BF = jnp.bfloat16
F32 = jnp.float32
VM = pl.BlockSpec(memory_space=pltpu.VMEM)
SM = pl.BlockSpec(memory_space=pltpu.SMEM)
HB = pl.BlockSpec(memory_space=pltpu.HBM)


def kernel_call(body, out_shape, args, scratch=(), smem=0, work=0, far=(), far_out=(), home=()):
    args = [
        pltpu.with_memory_space_constraint(a, pltpu.HBM) if i in far else a
        for i, a in enumerate(args)
    ]
    out_shape = [
        pltpu.HBM(o.shape, o.dtype) if i in far_out or i in home else o
        for i, o in enumerate(out_shape)
    ]
    return pl.pallas_call(
        body,
        out_shape=out_shape,
        in_specs=[SM if i < smem else HB if i in far else VM for i in range(len(args))],
        out_specs=[HB if i in far_out else VM for i in range(len(out_shape))],
        scratch_shapes=list(scratch),
        cost_estimate=pl.CostEstimate(flops=work, bytes_accessed=1 << 20, transcendentals=0),
        compiler_params=pltpu.CompilerParams(vmem_limit_bytes=12 << 20),
    )(*args)


def shape(dims, kind):
    return jax.ShapeDtypeStruct(dims, kind)


def exchange(spread_rows):
    return lax.all_to_all(spread_rows, AXES, 0, 0)


def neighbours(axis):
    count = lax.axis_size(axis)
    forward = [(i, i + 1) for i in range(count - 1)]
    return forward, [(t, s) for s, t in forward]


def order_matrix(chan, rows, start, lanes):
    k = lax.broadcasted_iota(jnp.int32, (chan * rows, lanes), 0)
    n = lax.broadcasted_iota(jnp.int32, (chan * rows, lanes), 1)
    return (n == (k % rows) * chan + k // rows + start).astype(BF)


def lane_at(group):
    if isinstance(group, int):
        return slice(group * LANES, (group + 1) * LANES)
    return pl.ds(pl.multiple_of(group * LANES, LANES), LANES)


def band_conv(src, weight, group, planes, pitch):
    size = planes * pitch + SEAM
    at = pl.multiple_of(group * LANES, LANES)
    parts = [src[pl.ds(d * pitch, size), pl.ds(at, 2 * LANES)] for d in range(3)]
    out = jnp.dot(jnp.concatenate(parts, axis=1), weight[...], preferred_element_type=F32)
    return (
        pltpu.roll(out[:, :LANES], 1, 0)
        + out[:, LANES : 2 * LANES]
        + pltpu.roll(out[:, 2 * LANES :], size - 1, 0)
    )


def tap_products(groups, h_ref, start, first, pitch):
    size = groups[0].shape[0]
    left, right = [], []
    for g, rows in enumerate(groups):
        left.append(
            jnp.concatenate(
                [pltpu.roll(rows, size - 1, 0), rows, pltpu.roll(rows, 1, 0)], axis=1
            ).astype(BF)
        )
        at = (first + g) * LANES
        right.append(
            jnp.concatenate(
                [
                    h_ref[start + d * pitch : start + d * pitch + size, at : at + 2 * LANES]
                    for d in range(3)
                ],
                axis=1,
            )
        )
    return lax.dot_general(
        jnp.concatenate(left, axis=0),
        jnp.concatenate(right, axis=0),
        (((0,), (0,)), ((), ())),
        preferred_element_type=F32,
    )


def fold_taps(acc, out, first, chan, offset):
    per = LANES // chan
    for d in range(3):
        for t in range(3):
            rows = sum(
                acc[
                    t * LANES + j * chan : t * LANES + (j + 1) * chan,
                    d * 2 * LANES + (j + offset) * chan : d * 2 * LANES + (j + offset + 3) * chan,
                ]
                for j in range(per)
            )
            for y in range(3):
                row, lane = divmod((d * 3 + y) * 3 + t, per)
                out[
                    first + row * chan : first + (row + 1) * chan, lane * chan : (lane + 1) * chan
                ] = rows[:, y * chan : (y + 1) * chan].astype(out.dtype)


def fold_lanes(value, chan):
    step = chan
    while step < LANES:
        value = value + pltpu.roll(value, step, 1)
        step *= 2
    return value


def packed(sums, chan):
    lane = lax.broadcasted_iota(jnp.int32, (1, LANES), 1)
    out = jnp.zeros((1, LANES), F32)
    for k, value in enumerate(sums):
        out = jnp.where(lane // chan == k, fold_lanes(value, chan), out)
    return out


def gathered(ref, k, chan):
    total = jnp.sum(ref[:, 0, :], axis=0, keepdims=True)
    lane = lax.broadcasted_iota(jnp.int32, (1, LANES), 1)
    return fold_lanes(jnp.where(lane // chan == k, total, 0.0), chan)


def sigmoid(value):
    return 0.5 + 0.5 * jnp.tanh(0.5 * value)


def body(x_a, x_b, w_first, w_second, gain_first, bias_first, gain_second, bias_second, grad_out):
    chan, span_x, span_y, span_z = x_a.shape
    world = lax.axis_size("gx") * lax.axis_size("gy") * lax.axis_size("gz")
    voxels = float(span_x * span_y * span_z * world)
    factor = 1.0 / math.sqrt(voxels)
    per = LANES // chan
    line = span_y * chan
    tiles = line // LANES
    pitch = span_z + SEAM
    inner_groups = span_y // per
    outer_groups = inner_groups + 1
    b_groups = inner_groups + 2
    wide = line + 3 * LANES
    begin = 2 * LANES
    mid = outer_groups * LANES
    mid_b = b_groups * LANES
    base_b, base_a, base_two, base_one = -5, -1, -2, -1
    po, pi = span_x + 2, span_x
    so, si, sw = po * pitch + SEAM, pi * pitch + SEAM, (span_x + 4) * pitch + SEAM
    flat_rows = span_x * span_z
    seams = (span_x + 1) * SEAM
    packs = span_x * SEAM
    strip_at = (0, si + tiles * packs)
    strip_rows = strip_at[1] + 2 * si + tiles * packs
    swap = lax.axis_size("gz") == 2
    tap_rows = -(-27 // per) * chan
    hold = -(-tap_rows // world)
    edges = 1 if swap else 2

    def limits(axis, low, high, reach):
        at, count = lax.axis_index(axis), lax.axis_size(axis)
        return [
            jnp.where(at == 0, low, low - reach),
            jnp.where(at == count - 1, high, high + reach),
        ]

    bounds = jnp.stack(
        limits("gx", 1, span_x + 1, 1)
        + limits("gy", 0, span_y, 3)
        + limits("gz", 0, span_z, 3)
        + [lax.axis_index("gz"), lax.axis_index("gy") % 2, lax.axis_index(AXES)]
    ).astype(jnp.int32)


    def fill_inside(bound, ref, planes):
        row = lax.broadcasted_iota(jnp.int32, (pitch, LANES), 0)
        near = ((row >= SEAM - 4) & (row >= bound[4] + SEAM)).astype(F32)
        far = ((row < SEAM - 4) & (row < bound[5] - span_z)).astype(F32)
        count = ref.shape[0] // pitch

        def valid(p):
            if p < 0 or p >= count:
                return jnp.float32(0.0)
            return jnp.where((p >= planes[0]) & (p < planes[1]), 1.0, 0.0).astype(F32)

        for p in range(count):
            ref[p * pitch : (p + 1) * pitch, :] = near * valid(p) + far * valid(p - 1)
        ref[count * pitch :, :] = far[:SEAM] * valid(count - 1)

    def rows_of(group, base):
        return (lax.broadcasted_iota(jnp.int32, (1, LANES), 1) + group * LANES) // chan + base

    def inside(bound, ref, group, base):
        y = rows_of(group, base)
        return ref[...] * ((y >= bound[2]) & (y < bound[3])).astype(F32) > 0.5

    def fill_own(ref):
        ref[...] = jnp.zeros(ref.shape, F32)
        for x in range(span_x):
            at = SEAM + x * pitch
            ref[at : at + span_z, :] = jnp.ones((span_z, LANES), F32)

    def own(ref, group, base):
        y = rows_of(group, base)
        return ref[...] * ((y >= 0) & (y < span_y)).astype(F32) > 0.5

    own_scratch = pltpu.VMEM((si, LANES), F32)
    in_scratch = pltpu.VMEM((so, LANES), F32)


    def prepare(w1_ref, w2_ref, g1_ref, b1_ref, g2_ref, b2_ref, c_ref, p_ref, w1, w2, v, sems):
        copies = [
            pltpu.make_async_copy(source, dest, sems.at[i])
            for i, (source, dest) in enumerate(
                ((w1_ref, w1), (w2_ref, w2))
                + tuple((r, v.at[i : i + 1]) for i, r in enumerate((g1_ref, b1_ref, g2_ref, b2_ref)))
            )
        ]
        for copy in copies:
            copy.start()
        c_ref[...] = jnp.zeros(c_ref.shape, BF)
        p_ref[...] = jnp.zeros(p_ref.shape, F32)
        for copy in copies:
            copy.wait()
        for j in range(per):
            p_ref[0:4, j * chan : (j + 1) * chan] = v[0:4, 0:chan]
        for kind, (w, back) in enumerate(((w1, False), (w2, False), (w2, True), (w1, True))):
            for dx in range(3):
                for dy in range(3):
                    for dz in range(3):
                        if back:
                            block = w[2 - dx, 2 - dy, 2 - dz]
                        else:
                            block = w[dx, dy, dz].astype(F32).T.astype(BF)
                        row = ((kind * 3 + dx) * 3 + dy) * chan
                        c_ref[row : row + chan, dz * chan : (dz + 1) * chan] = block

    class Band:
        def __init__(self, band, part, sem, far, kind):
            self.band, self.part = band, part
            rows = 9 * chan
            self.copy = pltpu.make_async_copy(far.at[pl.ds(kind * rows, rows)], part, sem)
            self.copy.start()

        def fill(self, offset):
            self.band[...] = jnp.zeros(self.band.shape, BF)
            self.copy.wait()
            fill_band(self.band, self.part, offset)
            return self.band

    def fill_band(band, c_ref, offset):
        for dx in range(3):
            at = dx * 3 * chan
            for dz in range(3):
                block = c_ref[at : at + 3 * chan, dz * chan : (dz + 1) * chan]
                for j in range(per):
                    row = (dx * 2 * per + j + offset) * chan
                    lane = dz * LANES + j * chan
                    band[row : row + 3 * chan, lane : lane + chan] = block

    band_scratch = (
        pltpu.VMEM((6 * LANES, 3 * LANES), BF),
        pltpu.VMEM((9 * chan, LANES), BF),
        pltpu.SemaphoreType.DMA,
    )
    token_shape = shape((8, LANES), F32)
    vectors = (gain_first, bias_first, gain_second, bias_second)
    weights, params = kernel_call(
        prepare,
        [shape((4 * 9 * chan, LANES), BF), token_shape],
        [w_first, w_second] + [v.reshape(1, chan) for v in vectors],
        scratch=[
            pltpu.VMEM(w_first.shape, BF),
            pltpu.VMEM(w_second.shape, BF),
            pltpu.VMEM((8, chan), F32),
            pltpu.SemaphoreType.DMA((6,)),
        ],
        far=range(6),
        home=(0,),
        work=1 << 31,
    )


    def turned(planes, order):
        return lax.dot_general(
            jnp.concatenate([p.reshape(chan * span_y, span_z) for p in planes], axis=1),
            order,
            (((0,), (0,)), ((), ())),
            preferred_element_type=F32,
        ).astype(BF)

    def native(value, order):
        return lax.dot_general(
            order, value, (((1,), (1,)), ((), ())), preferred_element_type=F32
        ).astype(BF).reshape(chan, span_y, span_z)

    def turn_in(bound, a_ref, b_ref, go_ref, t_ref, g_ref, z_ref, buf, sems):
        copies = [
            pltpu.make_async_copy(ref.at[:, x], buf.at[v * span_x + x], sems.at[v * span_x + x])
            for v, ref in enumerate((a_ref, b_ref, go_ref))
            for x in range(span_x)
        ]
        for copy in copies:
            copy.start()
        order = order_matrix(chan, span_y, 0, line)
        moved = order_matrix(chan, span_y, 2 * chan, mid)
        z_ref[...] = jnp.zeros(z_ref.shape, BF)
        for planes, dest, matrix in (
            (range(2 * span_x), t_ref, order),
            (range(2 * span_x, 3 * span_x), g_ref, moved),
        ):
            for at in planes:
                copies[at].wait()
            dest[...] = turned([buf[at] for at in planes], matrix)
            lanes = dest.shape[1]
            for at in planes:
                row = (at % (2 * span_x)) * span_z
                first = dest[row : row + SEAM, :]
                last = dest[row + span_z - SEAM : row + span_z, :]
                rows = slice(at * SEAM, (at + 1) * SEAM)
                if swap:
                    pick = jnp.full(first.shape, bound[6], jnp.int32) == 0
                    z_ref[0, rows, :lanes] = jnp.where(
                        pick, last.astype(F32), first.astype(F32)
                    ).astype(BF)
                else:
                    z_ref[0, rows, :lanes] = last
                    z_ref[1, rows, :lanes] = first


    def halo(block, cot_block, tiles_z, token):
        forward_x, backward_x = neighbours("gx")
        forward_z, backward_z = neighbours("gz")
        rows_y = lax.axis_size("gy")
        pairs_y = [
            [p for i in range(first, rows_y - 1, 2) for p in ((i, i + 1), (i + 1, i))]
            for first in range(2)
        ]
        if swap:
            got_z = [lax.ppermute(tiles_z[0], "gz", [(0, 1), (1, 0)])]
        else:
            got_z = [
                lax.ppermute(tiles_z[0], "gz", forward_z),
                lax.ppermute(tiles_z[1], "gz", backward_z),
            ]
        from_low = lax.ppermute(block, "gx", forward_x)
        from_high = lax.ppermute(block, "gx", backward_x)

        def edge(bound, t_ref, g_ref, *refs):
            got, (a_ref, b_ref, s_ref) = refs[:edges], refs[edges:]
            row = lax.broadcasted_iota(jnp.int32, (SEAM, mid), 0)
            even = jnp.full((SEAM, LANES), bound[7], jnp.int32) == 0
            even_block = jnp.full((span_z, LANES), bound[7], jnp.int32) == 0

            def choose(rows, low, high, ok):
                low, high = low.astype(F32), high.astype(F32)
                a_ref[rows, :] = jnp.where(ok, high, low).astype(BF)
                b_ref[rows, :] = jnp.where(ok, low, high).astype(BF)

            def tile_of(v, x):
                tile = jnp.zeros((SEAM, mid), F32)
                if x < span_x:
                    at = (v * span_x + x) * SEAM
                    value = got[0][at : at + SEAM, :].astype(F32)
                    ok = row >= SEAM - 4
                    if swap:
                        ok = ok & (jnp.full(row.shape, bound[6], jnp.int32) == 1)
                    tile = jnp.where(ok, value, tile)
                if x > 0:
                    at = (v * span_x + x - 1) * SEAM
                    value = got[-1][at : at + SEAM, :].astype(F32)
                    ok = row < 4
                    if swap:
                        ok = ok & (jnp.full(row.shape, bound[6], jnp.int32) == 0)
                    tile = jnp.where(ok, value, tile)
                tile = tile.astype(BF)
                s_ref[v * seams + x * SEAM : v * seams + (x + 1) * SEAM, :] = tile
                return tile

            def ends(value, v):
                lanes = line if v < 2 else mid
                return value[:, :LANES], value[:, lanes - LANES : lanes]

            def shared(values):
                (low, high), (cot_low, cot_high) = ends(values[0], 0), ends(values[1], 2)
                lane = lax.broadcasted_iota(jnp.int32, low.shape, 1)
                half = lane < 2 * chan
                return (
                    jnp.where(half, low.astype(F32), cot_low.astype(F32)),
                    jnp.where(half, cot_high.astype(F32), high.astype(F32)),
                )

            for x in range(span_x + 1):
                seam_tiles = [tile_of(v, x) for v in range(3)]
                base = x * pitch
                rows = slice(base, base + SEAM)
                choose(rows, *shared((seam_tiles[0], seam_tiles[2])), even)
                rows = slice(si + base, si + base + SEAM)
                choose(rows, *ends(seam_tiles[1], 1), even)
                if x < span_x:
                    plane = slice(x * span_z, (x + 1) * span_z)
                    rows = slice(base + SEAM, base + pitch)
                    choose(rows, *shared((t_ref[plane, :], g_ref[plane, :])), even_block)
                    plane = slice((span_x + x) * span_z, (span_x + x + 1) * span_z)
                    rows = slice(si + base + SEAM, si + base + pitch)
                    choose(rows, *ends(t_ref[plane, :], 1), even_block)

        send_a, send_b, seam_rows = kernel_call(
            edge,
            [shape((2 * si, LANES), BF)] * 2 + [shape((3 * seams, mid), BF)],
            [bounds, block, cot_block] + got_z,
            smem=1,
        )
        got_a = lax.ppermute(send_a, "gy", pairs_y[0])
        got_b = lax.ppermute(send_b, "gy", pairs_y[1])

        def strips(bound, a_ref, b_ref, s_ref, g_ref, token_ref, o_ref, f_ref):
            del token_ref
            lane = lax.broadcasted_iota(jnp.int32, (si, LANES), 1)
            even = jnp.full(lane.shape, bound[7], jnp.int32) == 0

            def both(v):
                a = a_ref[v * si : (v + 1) * si, :].astype(F32)
                b = b_ref[v * si : (v + 1) * si, :].astype(F32)
                return jnp.where(even, b, a), jnp.where(even, a, b)

            low, high = both(0)
            o_ref[0:si, :] = jnp.where(lane < 2 * chan, high, low).astype(BF)
            low, high = both(1)
            at = strip_at[1]
            o_ref[at : at + si, :] = low.astype(BF)
            o_ref[at + si : at + 2 * si, :] = high.astype(BF)
            for v, first in enumerate((si, at + 2 * si)):
                for t in range(tiles):
                    lanes = slice(t * LANES, (t + 1) * LANES)
                    at = first + t * packs
                    o_ref[at : at + SEAM, :] = (
                        s_ref[v * seams : v * seams + SEAM, lanes]
                        + s_ref[(v + 1) * seams - SEAM : (v + 1) * seams, lanes]
                    )
                    o_ref[at + SEAM : at + packs, :] = s_ref[
                        v * seams + SEAM : (v + 1) * seams - SEAM, lanes
                    ]
            low, high = both(0)
            for x in range(span_x + 1):
                f_ref[x * pitch : x * pitch + SEAM, :] = s_ref[
                    2 * seams + x * SEAM : 2 * seams + (x + 1) * SEAM, :
                ]
                if x < span_x:
                    f_ref[x * pitch + SEAM : (x + 1) * pitch, :] = g_ref[
                        x * span_z : (x + 1) * span_z, :
                    ]
            f_ref[:, :LANES] = jnp.where(
                lane < 2 * chan, low, f_ref[:, :LANES].astype(F32)
            ).astype(BF)
            f_ref[:, mid - LANES :] = jnp.where(
                lane >= 2 * chan, high, f_ref[:, mid - LANES :].astype(F32)
            ).astype(BF)

        mine, cot_frame = kernel_call(
            strips,
            [shape((strip_rows, LANES), BF), shape((si, mid), BF)],
            [bounds, got_a, got_b, seam_rows, cot_block, token],
            smem=1,
        )
        return [
            from_low,
            block,
            from_high,
            lax.ppermute(mine, "gx", forward_x),
            mine,
            lax.ppermute(mine, "gx", backward_x),
        ], cot_frame

    def joiner(dest):
        waiting = {}

        def put(seam, columns, value):
            key = (seam, columns)
            if key in waiting:
                dest[seam : seam + SEAM, columns[0] : columns[1]] = waiting.pop(key) + value
            else:
                waiting[key] = value

        def finish():
            for (seam, columns), value in waiting.items():
                dest[seam : seam + SEAM, columns[0] : columns[1]] = value

        return put, finish

    def assemble(dest, v, pieces):
        blocks, strip_refs = pieces[:3], pieces[3:]
        lane = lax.broadcasted_iota(jnp.int32, (si, LANES), 1)
        put, finish = joiner(dest)
        dest[:, :LANES] = jnp.zeros((sw, LANES), BF)
        last = si - SEAM
        for b in range(3):
            base = b * span_x * pitch
            for x in range(span_x):
                at = base + SEAM + x * pitch
                rows = slice((v * span_x + x) * span_z, (v * span_x + x + 1) * span_z)
                dest[at : at + span_z, begin : begin + line] = blocks[b][rows, :]
            first = strip_at[v]
            if v == 0:
                ys = strip_refs[b][first : first + si, :].astype(F32)
                low = jnp.where(lane >= 2 * chan, ys, 0.0).astype(BF)
                high = jnp.where(lane < 2 * chan, ys, 0.0).astype(BF)
                first += si
            else:
                low = strip_refs[b][first : first + si, :]
                high = strip_refs[b][first + si : first + 2 * si, :]
                first += 2 * si
            for columns, value in (((LANES, begin), low), ((begin + line, wide), high)):
                dest[base + SEAM : base + last, columns[0] : columns[1]] = value[SEAM:last]
                put(base, columns, value[:SEAM])
                put(base + last, columns, value[last:])
            for t in range(tiles):
                at = first + t * packs
                columns = (begin + LANES * t, begin + LANES * (t + 1))
                shared = strip_refs[b][at : at + SEAM, :].astype(F32)
                row = lax.broadcasted_iota(jnp.int32, shared.shape, 0)
                for x in range(span_x + 1):
                    if x == 0:
                        value = jnp.where(row >= SEAM - 4, shared, 0.0).astype(BF)
                    elif x == span_x:
                        value = jnp.where(row < 4, shared, 0.0).astype(BF)
                    else:
                        value = strip_refs[b][at + x * SEAM : at + (x + 1) * SEAM, :]
                    seam = base + x * pitch
                    if 0 < x < span_x:
                        dest[seam : seam + SEAM, columns[0] : columns[1]] = value
                    else:
                        put(seam, columns, value)
        finish()

    def below(frame, band, group):
        now, later = windows(frame, group)
        zeros = jnp.zeros((si - (later.shape[0] - pitch), 2 * LANES), BF)
        lhs = jnp.concatenate([now, jnp.concatenate([later[pitch:], zeros], axis=0)], axis=1)
        return spread_dz(jnp.dot(lhs, band[0 : 4 * LANES, :], preferred_element_type=F32))

    def above(frame, band, group):
        now, later = windows(frame, group)
        zeros = jnp.zeros((pitch, 2 * LANES), BF)
        lhs = jnp.concatenate([jnp.concatenate([zeros, later[: si - pitch]], axis=0), now], axis=1)
        return spread_dz(jnp.dot(lhs, band[2 * LANES :, :], preferred_element_type=F32))

    def windows(frame, group):
        value = frame[:, lane_at(group)]
        if (group + 1) * LANES < mid:
            more = frame[:, lane_at(group + 1)]
        else:
            more = jnp.zeros(value.shape, BF)
        value = jnp.concatenate([value, more], axis=1)
        return value, value

    def spread_dz(out):
        size = out.shape[0]
        return (
            pltpu.roll(out[:, :LANES], 1, 0)
            + out[:, LANES : 2 * LANES]
            + pltpu.roll(out[:, 2 * LANES :], size - 1, 0)
        )

    def halves(first, second):
        cut = si - SEAM // 2
        return jnp.concatenate([first[:cut], second[SEAM // 2 :]], axis=0)


    def stat_shape(rows):
        return shape((world, rows, LANES), F32)

    def send(ref, sums, *parts):
        ref[:, 0:1, :] = jnp.broadcast_to(packed(sums, chan)[None], (world, 1, LANES))
        for i, part in enumerate(parts):
            for d in range(world):
                ref[d, 1 + i * hold : 1 + (i + 1) * hold, :] = part[d * hold : (d + 1) * hold, :]

    def moments(st_ref, row):
        mean = gathered(st_ref, row, chan) / voxels
        var = gathered(st_ref, row + 1, chan) / voxels - mean * mean
        return mean, lax.rsqrt(var + EPSILON)

    def add_up(sums, value, other):
        return (
            sums[0] + jnp.sum(value, axis=0, keepdims=True),
            sums[1] + jnp.sum(value * other, axis=0, keepdims=True),
        )

    def conv_one_of(first, groups, base, band, dest, c_ref, own_ref, to=None):
        fill_own(own_ref)
        band = band.fill(2)

        def step(g, sums):
            out = band_conv(dest, band, g + first, po, pitch)
            c_ref[:, lane_at(g)] = out
            if to is not None:
                column(c_ref, to[0], to[1], g).start()
            mine = jnp.where(own(own_ref, g, base), out[pitch : pitch + si], 0.0)
            return add_up(sums, mine, mine)

        return lax.fori_loop(0, groups, step, (zero(), zero()), unroll=True)

    def zero():
        return jnp.zeros((1, LANES), F32)

    def first_conv_b(w_ref, *refs):
        pieces, rest = refs[:6], refs[6:]
        c_ref, x_out, a_out, st_ref, m_ref, x_ref, a_ref, own_ref, *band, sems = rest
        band = Band(*band, w_ref, 0)
        copies = [
            pltpu.make_async_copy(a_ref, a_out, sems.at[0]),
            pltpu.make_async_copy(x_ref, x_out, sems.at[1]),
        ]
        assemble(a_ref, 0, pieces)
        copies[0].start()
        assemble(x_ref, 1, pieces)
        copies[1].start()
        send(st_ref, conv_one_of(0, b_groups, base_b, band, x_ref, c_ref, own_ref))
        plain_taps(x_ref, m_ref)
        for copy in copies:
            copy.wait()

    def first_conv_a(w_ref, after, x_far, c_out, st_ref, x_ref, c_ref, own_ref, band, part, wait, sem, sems):
        del after
        band = Band(band, part, wait, w_ref, 0)
        copy = pltpu.make_async_copy(x_far, x_ref, sem)
        copy.start()
        st_ref[...] = jnp.zeros(st_ref.shape, F32)
        copy.wait()
        to = (c_out, sems)
        rows = conv_one_of(1, outer_groups, base_a, band, x_ref, c_ref, own_ref, to)
        for k in range(2):
            st_ref[k : k + 1, :] = rows[k]
        columns(c_ref, c_out, sems)

    def column(source, dest, sems, g):
        return pltpu.make_async_copy(source.at[:, lane_at(g)], dest.at[:, lane_at(g)], sems.at[g])

    def columns(source, dest, sems):
        def wait(g, carry):
            column(source, dest, sems, g).wait()
            return carry

        lax.fori_loop(0, outer_groups, wait, 0, unroll=True)

    def conv_two_of(bound, c_ref, st_in, k, p_ref, h_ref, c2_ref, own_ref, in_ref, band, shifts, after=None):
        groups, base, out_groups, out_base, offset = shifts
        fill_own(own_ref)
        fill_inside(bound, in_ref, (bound[0], bound[1]))
        mean, rstd = moments(st_in, k)
        gain, bias = p_ref[0:1, :], p_ref[1:2, :]

        def act(g, carry):
            at = lane_at(g)
            z = gain * ((c_ref[:, at] - mean) * rstd) + bias
            h = jnp.where(inside(bound, in_ref, g, base), z * sigmoid(z), 0.0)
            h_ref[:, at] = h.astype(BF)
            return carry

        lax.fori_loop(0, groups, act, 0, unroll=True)
        if after is not None:
            after.start()
        band = band.fill(offset)

        def step(g, sums):
            out = band_conv(h_ref, band, g, pi, pitch)
            c2_ref[:, lane_at(g)] = out
            mine = jnp.where(own(own_ref, g, out_base), out, 0.0)
            return add_up(sums, mine, mine)

        return lax.fori_loop(0, out_groups, step, (zero(), zero()), unroll=True)

    def second_conv_b(bound, c_ref, w_ref, st_in, p_ref, more, m_ref, h_out, c2_ref, st_ref, token_ref, h_ref, own_ref, in_ref, band, part, wait, sem):
        band = Band(band, part, wait, w_ref, 1)
        token_ref[...] = jnp.zeros(token_ref.shape, F32)
        copy = pltpu.make_async_copy(h_ref, h_out, sem)
        shifts = (b_groups, base_b, outer_groups, base_two, 2)
        rows = conv_two_of(bound, c_ref, st_in, 0, p_ref, h_ref, c2_ref, own_ref, in_ref, band, shifts, copy)
        send(st_ref, list(rows) + [more[0:1, :], more[1:2, :]])
        for d in range(world):
            for k in range(2):
                row = min(d * hold // chan + k, m_ref.shape[0] - 1)
                st_ref[d, 1 + k : 2 + k, :] = m_ref[row : row + 1, :]
        copy.wait()

    def second_conv_a(bound, c_far, w_ref, st_in, p_ref, after, c2_ref, st_ref, c_ref, h_ref, own_ref, in_ref, band, part, wait, sem):
        del after
        band = Band(band, part, wait, w_ref, 1)
        shifts = (outer_groups, base_a, inner_groups, 0, 0)
        copy = pltpu.make_async_copy(c_far, c_ref, sem)
        copy.start()
        copy.wait()
        rows = conv_two_of(bound, c_ref, st_in, 2, p_ref, h_ref, c2_ref, own_ref, in_ref, band, shifts)
        st_ref[...] = jnp.concatenate(list(rows) + [jnp.zeros((6, LANES), F32)], axis=0)

    def early_taps(c_ref, st_in, x_far, after, t_ref, x_ref, acc, own_ref, sem):
        del after
        copy = pltpu.make_async_copy(x_far, x_ref, sem)
        copy.start()
        fill_own(own_ref)
        mean, rstd = moments(st_in, 0)
        copy.wait()
        groups = []
        for g in range(outer_groups):
            xhat = (c_ref[pl.ds(pitch, si), lane_at(g + 1)] - mean) * rstd
            groups.append(jnp.where(own(own_ref, g, base_one), xhat, 0.0))
        acc[...] = tap_products(groups, x_ref, pitch, 1, pitch)
        t_ref[...] = jnp.zeros(t_ref.shape, F32)
        fold_taps(acc, t_ref, 0, chan, 2)

    def plain_taps(x_ref, m_ref):
        m_ref[...] = jnp.zeros(m_ref.shape, F32)
        row = lax.broadcasted_iota(jnp.int32, (8, si), 0)
        at = lax.broadcasted_iota(jnp.int32, (8, si), 1)
        pick = jnp.zeros((8, si), F32)
        for x in range(span_x):
            for t in range(3):
                low = SEAM + x * pitch + t - 1
                pick = jnp.where((row == t) & (at >= low) & (at < low + span_z), 1.0, pick)
        pick = pick.astype(BF)
        for d in range(3):
            cols = jnp.dot(
                pick, x_ref[pl.ds((1 + d) * pitch, si), :], preferred_element_type=F32
            )
            for y in range(3):
                low = begin + (y - 1) * chan
                own_cols = cols[:, low : low + line]
                total = sum(own_cols[:, k * LANES : (k + 1) * LANES] for k in range(tiles))
                total = fold_lanes(total, chan)
                for t in range(3):
                    group, place = divmod((d * 3 + y) * 3 + t, per)
                    m_ref[group : group + 1, place * chan : (place + 1) * chan] = total[
                        t : t + 1, place * chan : (place + 1) * chan
                    ]

    def slope_two(c_ref, moment, p_ref, go_ref, at):
        mean, rstd = moment
        xhat = (c_ref[:, at] - mean) * rstd
        z = p_ref[2:3, :] * xhat + p_ref[3:4, :]
        s = sigmoid(z)
        d = go_ref[:, at].astype(F32) * (s * (1.0 + z * (1.0 - s)))
        return d, xhat

    def second_slope(c_ref, st_in, p_ref, go_ref, t_ref, st_ref, token_ref, own_ref):
        token_ref[...] = jnp.zeros(token_ref.shape, F32)
        fill_own(own_ref)
        moment = moments(st_in, 0)

        def step(g, sums):
            d, xhat = slope_two(c_ref, moment, p_ref, go_ref, lane_at(g))
            return add_up(sums, jnp.where(own(own_ref, g, base_two), d, 0.0), xhat)

        rows = lax.fori_loop(0, outer_groups, step, (zero(), zero()), unroll=True)
        send(st_ref, rows, t_ref)

    def second_delta(bound, c_ref, st_in, p_ref, go_ref, sums_in, after, d_ref, in_ref):
        del after
        fill_inside(bound, in_ref, (0, span_x))
        moment = moments(st_in, 0)
        scale = p_ref[2:3, :] * moment[1]
        sum_d, sum_x = gathered(sums_in, 0, chan) / voxels, gathered(sums_in, 1, chan) / voxels

        def step(g, carry):
            at = lane_at(g)
            d, xhat = slope_two(c_ref, moment, p_ref, go_ref, at)
            out = scale * (d - sum_d - xhat * sum_x)
            d_ref[:, at] = jnp.where(inside(bound, in_ref, g, base_two), out, 0.0).astype(BF)
            return carry

        lax.fori_loop(0, outer_groups, step, 0, unroll=True)

    def second_taps(d_ref, h_far, gw_ref, h_ref, acc, own_ref, sem):
        copy = pltpu.make_async_copy(h_far, h_ref, sem)
        copy.start()
        fill_own(own_ref)
        gw_ref[...] = jnp.zeros(gw_ref.shape, F32)
        copy.wait()
        groups = [
            jnp.where(own(own_ref, g, base_two), d_ref[:, lane_at(g)].astype(F32), 0.0)
            for g in range(outer_groups)
        ]
        acc[...] = tap_products(groups, h_ref, 0, 0, pitch)
        fold_taps(acc, gw_ref, 0, chan, 2)

    def own_upstream(w_ref, d_ref, after, e_ref, band, part, wait):
        del after
        band = Band(band, part, wait, w_ref, 2).fill(0)
        for g in range(outer_groups):
            e_ref[:, lane_at(g)] = halves(above(d_ref, band, g), below(d_ref, band, g))

    def first_slope(w_ref, c_ref, st_in, p_ref, more, gw_two, x_far, low_ref, high_ref, e_ref, *rest):
        d1_out, st_ref, own_ref, *band, x_ref, acc, gw_ref, d1_ref, sem, sems = rest
        band = Band(*band, w_ref, 2)
        copy = pltpu.make_async_copy(x_far, x_ref, sem)
        copy.start()
        fill_own(own_ref)
        band = band.fill(0)
        mean, rstd = moments(st_in, 0)
        gw_ref[...] = jnp.zeros(gw_ref.shape, F32)
        copy.wait()
        groups = []

        def step(g, sums):
            at = lane_at(g)
            xhat = (c_ref[:, lane_at(g + 1)] - mean) * rstd
            z = p_ref[0:1, :] * xhat + p_ref[1:2, :]
            s = sigmoid(z)
            e = e_ref[:, at] + halves(below(low_ref, band, g), above(high_ref, band, g))
            d = e * (s * (1.0 + z * (1.0 - s)))
            d1_ref[:, at] = d
            column(d1_ref, d1_out, sems, g).start()
            mine = jnp.where(own(own_ref, g, base_one), d[pitch : pitch + si], 0.0)
            groups.append(mine)
            return add_up(sums, mine, xhat[pitch : pitch + si])

        rows = (zero(), zero())
        for g in range(outer_groups):
            rows = step(g, rows)
        acc[...] = tap_products(groups, x_ref, pitch, 1, pitch)
        fold_taps(acc, gw_ref, 0, chan, 2)
        send(st_ref, list(rows) + [more[0:1, :], more[1:2, :]], gw_ref, gw_two)
        columns(d1_ref, d1_out, sems)

    def first_delta(bound, s_far, c_ref, st_in, p_ref, sums_in, w_ref, after, dx_ref, s_ref, d_ref, o_ref, in_ref, band, part, wait, sem):
        del after
        band = Band(band, part, wait, w_ref, 3)
        copy = pltpu.make_async_copy(s_far, s_ref, sem)
        copy.start()
        fill_inside(bound, in_ref, (bound[0], bound[1]))
        band = band.fill(0)
        copy.wait()
        sum_d, sum_x = gathered(sums_in, 0, chan) / voxels, gathered(sums_in, 1, chan) / voxels
        mean, rstd = moments(st_in, 0)
        scale = p_ref[0:1, :] * rstd

        def step(g, carry):
            at = lane_at(g)
            xhat = (c_ref[:, lane_at(g + 1)] - mean) * rstd
            out = scale * (s_ref[:, at] - sum_d - xhat * sum_x)
            d_ref[:, at] = jnp.where(inside(bound, in_ref, g, base_one), out, 0.0).astype(BF)
            return carry

        lax.fori_loop(0, outer_groups, step, 0, unroll=True)

        def conv(g, carry):
            o_ref[:, lane_at(g)] = band_conv(d_ref, band, g, pi, pitch).astype(BF)
            return carry

        lax.fori_loop(0, inner_groups, conv, 0, unroll=True)
        order = order_matrix(chan, span_y, 0, line)
        for x in range(span_x):
            at = SEAM + x * pitch
            dx_ref[:, x] = native(o_ref[at : at + span_z, :], order)

    def mix(bound, st_in, p_ref, plain_ref, early_ref, late_ref, out_ref, token_ref):
        token_ref[...] = jnp.zeros(token_ref.shape, F32)
        sum_d, sum_x = gathered(late_ref, 0, chan) / voxels, gathered(late_ref, 1, chan) / voxels
        scale = p_ref[0:1, :] * moments(st_in, 0)[1]
        row = lax.broadcasted_iota(jnp.int32, (hold, LANES), 0) + bound[8] * hold
        lane = lax.broadcasted_iota(jnp.int32, (hold, LANES), 1)

        def of_row(value):
            return jnp.sum(jnp.where(lane == row % chan, value, 0.0), axis=1, keepdims=True)

        def part(ref, i):
            return jnp.sum(ref[:, 1 + i * hold : 1 + (i + 1) * hold, :], axis=0)

        plain = jnp.sum(plain_ref[:, 1:3, :], axis=0)
        plain = jnp.where(row // chan == bound[8] * hold // chan, plain[0:1, :], plain[1:2, :])
        one = of_row(scale) * (
            part(late_ref, 0) - of_row(sum_d) * plain - of_row(sum_x) * part(early_ref, 0)
        )
        out = jnp.concatenate([one, part(late_ref, 1)], axis=0) * factor
        spare = out_ref.shape[1] - out.shape[0]
        if spare:
            out = jnp.concatenate([out, jnp.zeros((spare, LANES), F32)], axis=0)
        out_ref[...] = jnp.broadcast_to(out.astype(BF)[None], out_ref.shape)

    def last(got_ref, one_ref, two_ref, flat):
        for i, out in enumerate((one_ref, two_ref)):
            for d in range(world):
                flat[d * hold : (d + 1) * hold, :] = got_ref[d, i * hold : (i + 1) * hold, :].astype(F32)
            for at in range(27):
                row, lane = divmod(at, per)
                block = flat[row * chan : (row + 1) * chan, lane * chan : (lane + 1) * chan]
                out[at // 9, at // 3 % 3, at % 3] = block

    def out_a(c_ref, st_in, st_two, p_ref, after, y_ref, n_ref, h_ref):
        del after
        for row, (ref, at) in enumerate(((st_in, 1), (st_in, 0), (st_two, 1), (st_two, 0))):
            n_ref[row : row + 1, :] = factor * gathered(ref, at, chan)[:, :chan]
        order = order_matrix(chan, span_y, 0, line)
        mean, rstd = moments(st_in, 2)

        def act(g, carry):
            at = lane_at(g)
            z = p_ref[2:3, :] * ((c_ref[:, at] - mean) * rstd) + p_ref[3:4, :]
            h_ref[:, at] = (z * sigmoid(z)).astype(BF)
            return carry

        lax.fori_loop(0, inner_groups, act, 0, unroll=True)
        for x in range(span_x):
            at = SEAM + x * pitch
            y_ref[:, x] = native(h_ref[at : at + span_z, :], order)


    vols, cot_block, tiles_z = kernel_call(
        turn_in,
        [
            shape((2 * flat_rows, line), BF),
            shape((flat_rows, mid), BF),
            shape((edges, 3 * span_x * SEAM, mid), BF),
        ],
        [bounds, x_a, x_b, grad_out],
        scratch=[
            pltpu.VMEM((3 * span_x, chan, span_y, span_z), BF),
            pltpu.SemaphoreType.DMA((3 * span_x,)),
        ],
        smem=1,
        far=(1, 2, 3),
    )
    pieces, cot = halo(vols, cot_block, tiles_z, params)
    wide_scratch = pltpu.VMEM((sw, wide), BF)
    one_copy = pltpu.SemaphoreType.DMA
    mid_scratch = pltpu.VMEM((so, mid), F32)
    group_copies = pltpu.SemaphoreType.DMA((outer_groups,))
    acc_scratch = pltpu.VMEM((3 * LANES, 6 * LANES), F32)
    c1_b, pad_b, pad_a, stats, plain = kernel_call(
        first_conv_b,
        [shape((so, mid_b), F32)] + [shape((sw, wide), BF)] * 2 + [stat_shape(1), token_shape],
        [weights] + pieces,
        scratch=[
            wide_scratch,
            wide_scratch,
            own_scratch,
            *band_scratch,
            pltpu.SemaphoreType.DMA((2,)),
        ],
        far=(0,),
        far_out=(1, 2),
        home=(3,),
        work=1 << 30,
    )
    stats_one = exchange(stats)
    c1_a, local_a = kernel_call(
        first_conv_a,
        [shape((so, mid), F32), shape((8, LANES), F32)],
        [weights, plain, pad_a],
        scratch=[wide_scratch, mid_scratch, own_scratch, *band_scratch, one_copy, group_copies],
        far=(0, 2),
        far_out=(0,),
        work=1 << 32,
    )
    hidden_b, c2_b, stats, token = kernel_call(
        second_conv_b,
        [shape((so, mid_b), BF), shape((si, mid), F32), stat_shape(3), token_shape],
        [bounds, c1_b, weights, stats_one, params, local_a, plain],
        scratch=[pltpu.VMEM((so, mid_b), BF), own_scratch, in_scratch, *band_scratch, one_copy],
        smem=1,
        far_out=(0,),
        home=(2,),
        far=(2,),
        work=1 << 30,
    )
    stats_two = exchange(stats)
    (taps_early,) = kernel_call(
        early_taps,
        [shape((world * hold, LANES), F32)],
        [c1_b, stats_one, pad_b, token],
        scratch=[wide_scratch, acc_scratch, own_scratch, one_copy],
        far=(2,),
        work=1 << 32,
    )
    stats, token = kernel_call(
        second_slope,
        [stat_shape(1 + hold), token_shape],
        [c2_b, stats_two, params, cot, taps_early],
        scratch=[own_scratch],
        home=(0,),
        work=1 << 27,
    )
    sums_two = exchange(stats)
    c2_a, local_a = kernel_call(
        second_conv_a,
        [shape((si, line), F32), shape((8, LANES), F32)],
        [bounds, c1_a, weights, stats_two, params, token],
        scratch=[mid_scratch, pltpu.VMEM((so, mid), BF), own_scratch, in_scratch, *band_scratch, one_copy],
        smem=1,
        far=(1, 2),
        home=(0,),
        work=1 << 32,
    )
    (delta_two,) = kernel_call(
        second_delta,
        [shape((si, mid), BF)],
        [bounds, c2_b, stats_two, params, cot, sums_two, local_a],
        scratch=[pltpu.VMEM((si, LANES), F32)],
        smem=1,
        work=1 << 27,
    )
    (taps_two,) = kernel_call(
        second_taps,
        [shape((world * hold, LANES), F32)],
        [delta_two, hidden_b],
        scratch=[pltpu.VMEM((so, mid_b), BF), acc_scratch, own_scratch, one_copy],
        far=(1,),
        work=1 << 32,
    )
    forward_x, backward_x = neighbours("gx")
    frames = [
        lax.ppermute(delta_two, "gx", forward_x),
        lax.ppermute(delta_two, "gx", backward_x),
    ]
    (upstream,) = kernel_call(
        own_upstream,
        [shape((so, mid), F32)],
        [weights, delta_two, taps_two],
        scratch=list(band_scratch),
        far=(0,),
        work=1 << 32,
    )
    slope, stats = kernel_call(
        first_slope,
        [shape((so, mid), F32), stat_shape(1 + 2 * hold)],
        [weights, c1_b, stats_one, params, local_a, taps_two, pad_b] + frames + [upstream],
        scratch=[
            own_scratch,
            *band_scratch,
            wide_scratch,
            acc_scratch,
            pltpu.VMEM((world * hold, LANES), F32),
            mid_scratch,
            one_copy,
            group_copies,
        ],
        far=(0, 6),
        far_out=(0,),
        home=(1,),
        work=1 << 30,
    )
    sums_one = exchange(stats)
    whole, token = kernel_call(
        mix,
        [shape((world, -(-2 * hold // 8) * 8, LANES), BF), token_shape],
        [bounds, stats_one, params, stats_two, sums_two, sums_one],
        smem=1,
    )
    whole = exchange(whole)
    (dx_b,) = kernel_call(
        first_delta,
        [shape(x_a.shape, BF)],
        [bounds, slope, c1_b, stats_one, params, sums_one, weights, token],
        scratch=[
            mid_scratch,
            pltpu.VMEM((so, mid), BF),
            pltpu.VMEM((si, line), BF),
            in_scratch,
            *band_scratch,
            one_copy,
        ],
        smem=1,
        far=(1, 6),
        work=1 << 31,
    )
    y_a, grad_norm = kernel_call(
        out_a,
        [shape(x_a.shape, BF), shape((4, chan), F32)],
        [c2_a, sums_one, sums_two, params, token],
        scratch=[pltpu.VMEM((si, line), BF)],
        work=1 << 31,
    )
    weight_shape = shape((3, 3, 3, chan, chan), F32)
    grad_one, grad_two = kernel_call(
        last,
        [weight_shape, weight_shape],
        [whole],
        scratch=[pltpu.VMEM((world * hold, LANES), F32)],
    )
    return (y_a, dx_b, grad_one, grad_two, grad_norm)


def solution(mesh):
    block = P(None, "gx", "gy", "gz")
    placed = (block, block, P(), P(), P(), P(), P(), P(), block)

    return jax.shard_map(
        body,
        mesh=mesh,
        in_specs=placed,
        out_specs=(block, block, P(), P(), P()),
        check_vma=False,
    )
```

```python
import math

import jax
import jax.numpy as jnp
from jax import lax
from jax.experimental import pallas as pl
from jax.experimental.pallas import tpu as pltpu
from jax.sharding import PartitionSpec as P


EPSILON = 1e-05
AXES = ("gx", "gy", "gz")
LANES = 128
SEAM = 16
BF = jnp.bfloat16
F32 = jnp.float32
VM = pl.BlockSpec(memory_space=pltpu.VMEM)
SM = pl.BlockSpec(memory_space=pltpu.SMEM)
HB = pl.BlockSpec(memory_space=pltpu.HBM)


def kernel_call(body, out_shape, args, scratch=(), smem=0, work=0, far=(), far_out=(), home=()):
    args = [
        pltpu.with_memory_space_constraint(a, pltpu.HBM) if i in far else a
        for i, a in enumerate(args)
    ]
    out_shape = [
        pltpu.HBM(o.shape, o.dtype) if i in far_out or i in home else o
        for i, o in enumerate(out_shape)
    ]
    return pl.pallas_call(
        body,
        out_shape=out_shape,
        in_specs=[SM if i < smem else HB if i in far else VM for i in range(len(args))],
        out_specs=[HB if i in far_out else VM for i in range(len(out_shape))],
        scratch_shapes=list(scratch),
        cost_estimate=pl.CostEstimate(flops=work, bytes_accessed=1 << 20, transcendentals=0),
        compiler_params=pltpu.CompilerParams(vmem_limit_bytes=12 << 20),
    )(*args)


def shape(dims, kind):
    return jax.ShapeDtypeStruct(dims, kind)


def exchange(spread_rows):
    return lax.all_to_all(spread_rows, AXES, 0, 0)


def neighbours(axis):
    count = lax.axis_size(axis)
    forward = [(i, i + 1) for i in range(count - 1)]
    return forward, [(t, s) for s, t in forward]


def order_matrix(chan, rows, start, lanes):
    k = lax.broadcasted_iota(jnp.int32, (chan * rows, lanes), 0)
    n = lax.broadcasted_iota(jnp.int32, (chan * rows, lanes), 1)
    return (n == (k % rows) * chan + k // rows + start).astype(BF)


def lane_at(group):
    if isinstance(group, int):
        return slice(group * LANES, (group + 1) * LANES)
    return pl.ds(pl.multiple_of(group * LANES, LANES), LANES)


def band_conv(src, weight, group, planes, pitch):
    size = planes * pitch + SEAM
    at = pl.multiple_of(group * LANES, LANES)
    parts = [src[pl.ds(d * pitch, size), pl.ds(at, 2 * LANES)] for d in range(3)]
    out = jnp.dot(jnp.concatenate(parts, axis=1), weight[...], preferred_element_type=F32)
    return (
        pltpu.roll(out[:, :LANES], 1, 0)
        + out[:, LANES : 2 * LANES]
        + pltpu.roll(out[:, 2 * LANES :], size - 1, 0)
    )


def tap_products(groups, h_ref, start, first, pitch):
    size = groups[0].shape[0]
    left, right = [], []
    for g, rows in enumerate(groups):
        left.append(
            jnp.concatenate(
                [pltpu.roll(rows, size - 1, 0), rows, pltpu.roll(rows, 1, 0)], axis=1
            ).astype(BF)
        )
        at = (first + g) * LANES
        right.append(
            jnp.concatenate(
                [
                    h_ref[start + d * pitch : start + d * pitch + size, at : at + 2 * LANES]
                    for d in range(3)
                ],
                axis=1,
            )
        )
    return lax.dot_general(
        jnp.concatenate(left, axis=0),
        jnp.concatenate(right, axis=0),
        (((0,), (0,)), ((), ())),
        preferred_element_type=F32,
    )


def fold_taps(acc, out, first, chan, offset):
    per = LANES // chan
    for d in range(3):
        for t in range(3):
            rows = sum(
                acc[
                    t * LANES + j * chan : t * LANES + (j + 1) * chan,
                    d * 2 * LANES + (j + offset) * chan : d * 2 * LANES + (j + offset + 3) * chan,
                ]
                for j in range(per)
            )
            for y in range(3):
                row, lane = divmod((d * 3 + y) * 3 + t, per)
                out[
                    first + row * chan : first + (row + 1) * chan, lane * chan : (lane + 1) * chan
                ] = rows[:, y * chan : (y + 1) * chan].astype(out.dtype)


def fold_lanes(value, chan):
    step = chan
    while step < LANES:
        value = value + pltpu.roll(value, step, 1)
        step *= 2
    return value


def packed(sums, chan):
    lane = lax.broadcasted_iota(jnp.int32, (1, LANES), 1)
    out = jnp.zeros((1, LANES), F32)
    for k, value in enumerate(sums):
        out = jnp.where(lane // chan == k, fold_lanes(value, chan), out)
    return out


def gathered(ref, k, chan):
    total = jnp.sum(ref[:, 0, :], axis=0, keepdims=True)
    lane = lax.broadcasted_iota(jnp.int32, (1, LANES), 1)
    return fold_lanes(jnp.where(lane // chan == k, total, 0.0), chan)


def sigmoid(value):
    return 0.5 + 0.5 * jnp.tanh(0.5 * value)


def body(x_a, x_b, w_first, w_second, gain_first, bias_first, gain_second, bias_second, grad_out):
    chan, span_x, span_y, span_z = x_a.shape
    world = lax.axis_size("gx") * lax.axis_size("gy") * lax.axis_size("gz")
    voxels = float(span_x * span_y * span_z * world)
    factor = 1.0 / math.sqrt(voxels)
    per = LANES // chan
    line = span_y * chan
    tiles = line // LANES
    pitch = span_z + SEAM
    inner_groups = span_y // per
    outer_groups = inner_groups + 1
    b_groups = inner_groups + 2
    wide = line + 3 * LANES
    begin = 2 * LANES
    mid = outer_groups * LANES
    mid_b = b_groups * LANES
    base_b, base_a, base_two, base_one = -5, -1, -2, -1
    po, pi = span_x + 2, span_x
    so, si, sw = po * pitch + SEAM, pi * pitch + SEAM, (span_x + 4) * pitch + SEAM
    flat_rows = span_x * span_z
    seams = (span_x + 1) * SEAM
    packs = span_x * SEAM
    strip_at = (0, si + tiles * packs)
    strip_rows = strip_at[1] + 2 * si + tiles * packs
    swap = lax.axis_size("gz") == 2
    tap_rows = -(-27 // per) * chan
    hold = -(-tap_rows // world)
    edges = 1 if swap else 2

    def limits(axis, low, high, reach):
        at, count = lax.axis_index(axis), lax.axis_size(axis)
        return [
            jnp.where(at == 0, low, low - reach),
            jnp.where(at == count - 1, high, high + reach),
        ]

    bounds = jnp.stack(
        limits("gx", 1, span_x + 1, 1)
        + limits("gy", 0, span_y, 3)
        + limits("gz", 0, span_z, 3)
        + [lax.axis_index("gz"), lax.axis_index("gy") % 2, lax.axis_index(AXES)]
    ).astype(jnp.int32)


    def fill_inside(bound, ref, planes):
        row = lax.broadcasted_iota(jnp.int32, (pitch, LANES), 0)
        near = ((row >= SEAM - 4) & (row >= bound[4] + SEAM)).astype(F32)
        far = ((row < SEAM - 4) & (row < bound[5] - span_z)).astype(F32)
        count = ref.shape[0] // pitch

        def valid(p):
            if p < 0 or p >= count:
                return jnp.float32(0.0)
            return jnp.where((p >= planes[0]) & (p < planes[1]), 1.0, 0.0).astype(F32)

        for p in range(count):
            ref[p * pitch : (p + 1) * pitch, :] = near * valid(p) + far * valid(p - 1)
        ref[count * pitch :, :] = far[:SEAM] * valid(count - 1)

    def rows_of(group, base):
        return (lax.broadcasted_iota(jnp.int32, (1, LANES), 1) + group * LANES) // chan + base

    def inside(bound, ref, group, base):
        y = rows_of(group, base)
        return ref[...] * ((y >= bound[2]) & (y < bound[3])).astype(F32) > 0.5

    def fill_own(ref):
        ref[...] = jnp.zeros(ref.shape, F32)
        for x in range(span_x):
            at = SEAM + x * pitch
            ref[at : at + span_z, :] = jnp.ones((span_z, LANES), F32)

    def own(ref, group, base):
        y = rows_of(group, base)
        return ref[...] * ((y >= 0) & (y < span_y)).astype(F32) > 0.5

    own_scratch = pltpu.VMEM((si, LANES), F32)
    in_scratch = pltpu.VMEM((so, LANES), F32)


    def prepare(w1_ref, w2_ref, g1_ref, b1_ref, g2_ref, b2_ref, c_ref, p_ref, w1, w2, v, sems):
        copies = [
            pltpu.make_async_copy(source, dest, sems.at[i])
            for i, (source, dest) in enumerate(
                ((w1_ref, w1), (w2_ref, w2))
                + tuple((r, v.at[i : i + 1]) for i, r in enumerate((g1_ref, b1_ref, g2_ref, b2_ref)))
            )
        ]
        for copy in copies:
            copy.start()
        c_ref[...] = jnp.zeros(c_ref.shape, BF)
        p_ref[...] = jnp.zeros(p_ref.shape, F32)
        for copy in copies:
            copy.wait()
        for j in range(per):
            p_ref[0:4, j * chan : (j + 1) * chan] = v[0:4, 0:chan]
        for kind, (w, back) in enumerate(((w1, False), (w2, False), (w2, True), (w1, True))):
            for dx in range(3):
                for dy in range(3):
                    for dz in range(3):
                        if back:
                            block = w[2 - dx, 2 - dy, 2 - dz]
                        else:
                            block = w[dx, dy, dz].astype(F32).T.astype(BF)
                        row = ((kind * 3 + dx) * 3 + dy) * chan
                        c_ref[row : row + chan, dz * chan : (dz + 1) * chan] = block

    class Band:
        def __init__(self, band, part, sem, far, kind):
            self.band, self.part = band, part
            rows = 9 * chan
            self.copy = pltpu.make_async_copy(far.at[pl.ds(kind * rows, rows)], part, sem)
            self.copy.start()

        def fill(self, offset):
            self.band[...] = jnp.zeros(self.band.shape, BF)
            self.copy.wait()
            fill_band(self.band, self.part, offset)
            return self.band

    def fill_band(band, c_ref, offset):
        for dx in range(3):
            at = dx * 3 * chan
            for dz in range(3):
                block = c_ref[at : at + 3 * chan, dz * chan : (dz + 1) * chan]
                for j in range(per):
                    row = (dx * 2 * per + j + offset) * chan
                    lane = dz * LANES + j * chan
                    band[row : row + 3 * chan, lane : lane + chan] = block

    band_scratch = (
        pltpu.VMEM((6 * LANES, 3 * LANES), BF),
        pltpu.VMEM((9 * chan, LANES), BF),
        pltpu.SemaphoreType.DMA,
    )
    token_shape = shape((8, LANES), F32)
    vectors = (gain_first, bias_first, gain_second, bias_second)
    weights, params = kernel_call(
        prepare,
        [shape((4 * 9 * chan, LANES), BF), token_shape],
        [w_first, w_second] + [v.reshape(1, chan) for v in vectors],
        scratch=[
            pltpu.VMEM(w_first.shape, BF),
            pltpu.VMEM(w_second.shape, BF),
            pltpu.VMEM((8, chan), F32),
            pltpu.SemaphoreType.DMA((6,)),
        ],
        far=range(6),
        home=(0,),
        work=1 << 31,
    )


    def turned(planes, order):
        return lax.dot_general(
            jnp.concatenate([p.reshape(chan * span_y, span_z) for p in planes], axis=1),
            order,
            (((0,), (0,)), ((), ())),
            preferred_element_type=F32,
        ).astype(BF)

    def native(value, order):
        return lax.dot_general(
            order, value, (((1,), (1,)), ((), ())), preferred_element_type=F32
        ).astype(BF).reshape(chan, span_y, span_z)

    def turn_in(bound, a_ref, b_ref, go_ref, t_ref, g_ref, z_ref, buf, sems):
        copies = [
            pltpu.make_async_copy(ref.at[:, x], buf.at[v * span_x + x], sems.at[v * span_x + x])
            for v, ref in enumerate((a_ref, b_ref, go_ref))
            for x in range(span_x)
        ]
        for copy in copies:
            copy.start()
        order = order_matrix(chan, span_y, 0, line)
        moved = order_matrix(chan, span_y, 2 * chan, mid)
        z_ref[...] = jnp.zeros(z_ref.shape, BF)
        for planes, dest, matrix in (
            (range(2 * span_x), t_ref, order),
            (range(2 * span_x, 3 * span_x), g_ref, moved),
        ):
            for at in planes:
                copies[at].wait()
            dest[...] = turned([buf[at] for at in planes], matrix)
            lanes = dest.shape[1]
            for at in planes:
                row = (at % (2 * span_x)) * span_z
                first = dest[row : row + SEAM, :]
                last = dest[row + span_z - SEAM : row + span_z, :]
                rows = slice(at * SEAM, (at + 1) * SEAM)
                if swap:
                    pick = jnp.full(first.shape, bound[6], jnp.int32) == 0
                    z_ref[0, rows, :lanes] = jnp.where(
                        pick, last.astype(F32), first.astype(F32)
                    ).astype(BF)
                else:
                    z_ref[0, rows, :lanes] = last
                    z_ref[1, rows, :lanes] = first


    def halo(block, cot_block, tiles_z, token):
        forward_x, backward_x = neighbours("gx")
        forward_z, backward_z = neighbours("gz")
        rows_y = lax.axis_size("gy")
        pairs_y = [
            [p for i in range(first, rows_y - 1, 2) for p in ((i, i + 1), (i + 1, i))]
            for first in range(2)
        ]
        if swap:
            got_z = [lax.ppermute(tiles_z[0], "gz", [(0, 1), (1, 0)])]
        else:
            got_z = [
                lax.ppermute(tiles_z[0], "gz", forward_z),
                lax.ppermute(tiles_z[1], "gz", backward_z),
            ]
        from_low = lax.ppermute(block, "gx", forward_x)
        from_high = lax.ppermute(block, "gx", backward_x)

        def edge(bound, t_ref, g_ref, *refs):
            got, (a_ref, b_ref, s_ref) = refs[:edges], refs[edges:]
            row = lax.broadcasted_iota(jnp.int32, (SEAM, mid), 0)
            even = jnp.full((SEAM, LANES), bound[7], jnp.int32) == 0
            even_block = jnp.full((span_z, LANES), bound[7], jnp.int32) == 0

            def choose(rows, low, high, ok):
                low, high = low.astype(F32), high.astype(F32)
                a_ref[rows, :] = jnp.where(ok, high, low).astype(BF)
                b_ref[rows, :] = jnp.where(ok, low, high).astype(BF)

            def tile_of(v, x):
                tile = jnp.zeros((SEAM, mid), F32)
                if x < span_x:
                    at = (v * span_x + x) * SEAM
                    value = got[0][at : at + SEAM, :].astype(F32)
                    ok = row >= SEAM - 4
                    if swap:
                        ok = ok & (jnp.full(row.shape, bound[6], jnp.int32) == 1)
                    tile = jnp.where(ok, value, tile)
                if x > 0:
                    at = (v * span_x + x - 1) * SEAM
                    value = got[-1][at : at + SEAM, :].astype(F32)
                    ok = row < 4
                    if swap:
                        ok = ok & (jnp.full(row.shape, bound[6], jnp.int32) == 0)
                    tile = jnp.where(ok, value, tile)
                tile = tile.astype(BF)
                s_ref[v * seams + x * SEAM : v * seams + (x + 1) * SEAM, :] = tile
                return tile

            def ends(value, v):
                lanes = line if v < 2 else mid
                return value[:, :LANES], value[:, lanes - LANES : lanes]

            def shared(values):
                (low, high), (cot_low, cot_high) = ends(values[0], 0), ends(values[1], 2)
                lane = lax.broadcasted_iota(jnp.int32, low.shape, 1)
                half = lane < 2 * chan
                return (
                    jnp.where(half, low.astype(F32), cot_low.astype(F32)),
                    jnp.where(half, cot_high.astype(F32), high.astype(F32)),
                )

            for x in range(span_x + 1):
                seam_tiles = [tile_of(v, x) for v in range(3)]
                base = x * pitch
                rows = slice(base, base + SEAM)
                choose(rows, *shared((seam_tiles[0], seam_tiles[2])), even)
                rows = slice(si + base, si + base + SEAM)
                choose(rows, *ends(seam_tiles[1], 1), even)
                if x < span_x:
                    plane = slice(x * span_z, (x + 1) * span_z)
                    rows = slice(base + SEAM, base + pitch)
                    choose(rows, *shared((t_ref[plane, :], g_ref[plane, :])), even_block)
                    plane = slice((span_x + x) * span_z, (span_x + x + 1) * span_z)
                    rows = slice(si + base + SEAM, si + base + pitch)
                    choose(rows, *ends(t_ref[plane, :], 1), even_block)

        send_a, send_b, seam_rows = kernel_call(
            edge,
            [shape((2 * si, LANES), BF)] * 2 + [shape((3 * seams, mid), BF)],
            [bounds, block, cot_block] + got_z,
            smem=1,
        )
        got_a = lax.ppermute(send_a, "gy", pairs_y[0])
        got_b = lax.ppermute(send_b, "gy", pairs_y[1])

        def strips(bound, a_ref, b_ref, s_ref, g_ref, token_ref, o_ref, f_ref):
            del token_ref
            lane = lax.broadcasted_iota(jnp.int32, (si, LANES), 1)
            even = jnp.full(lane.shape, bound[7], jnp.int32) == 0

            def both(v):
                a = a_ref[v * si : (v + 1) * si, :].astype(F32)
                b = b_ref[v * si : (v + 1) * si, :].astype(F32)
                return jnp.where(even, b, a), jnp.where(even, a, b)

            low, high = both(0)
            o_ref[0:si, :] = jnp.where(lane < 2 * chan, high, low).astype(BF)
            low, high = both(1)
            at = strip_at[1]
            o_ref[at : at + si, :] = low.astype(BF)
            o_ref[at + si : at + 2 * si, :] = high.astype(BF)
            for v, first in enumerate((si, at + 2 * si)):
                for t in range(tiles):
                    lanes = slice(t * LANES, (t + 1) * LANES)
                    at = first + t * packs
                    o_ref[at : at + SEAM, :] = (
                        s_ref[v * seams : v * seams + SEAM, lanes]
                        + s_ref[(v + 1) * seams - SEAM : (v + 1) * seams, lanes]
                    )
                    o_ref[at + SEAM : at + packs, :] = s_ref[
                        v * seams + SEAM : (v + 1) * seams - SEAM, lanes
                    ]
            low, high = both(0)
            for x in range(span_x + 1):
                f_ref[x * pitch : x * pitch + SEAM, :] = s_ref[
                    2 * seams + x * SEAM : 2 * seams + (x + 1) * SEAM, :
                ]
                if x < span_x:
                    f_ref[x * pitch + SEAM : (x + 1) * pitch, :] = g_ref[
                        x * span_z : (x + 1) * span_z, :
                    ]
            f_ref[:, :LANES] = jnp.where(
                lane < 2 * chan, low, f_ref[:, :LANES].astype(F32)
            ).astype(BF)
            f_ref[:, mid - LANES :] = jnp.where(
                lane >= 2 * chan, high, f_ref[:, mid - LANES :].astype(F32)
            ).astype(BF)

        mine, cot_frame = kernel_call(
            strips,
            [shape((strip_rows, LANES), BF), shape((si, mid), BF)],
            [bounds, got_a, got_b, seam_rows, cot_block, token],
            smem=1,
        )
        return [
            from_low,
            block,
            from_high,
            lax.ppermute(mine, "gx", forward_x),
            mine,
            lax.ppermute(mine, "gx", backward_x),
        ], cot_frame

    def joiner(dest):
        waiting = {}

        def put(seam, columns, value):
            key = (seam, columns)
            if key in waiting:
                dest[seam : seam + SEAM, columns[0] : columns[1]] = waiting.pop(key) + value
            else:
                waiting[key] = value

        def finish():
            for (seam, columns), value in waiting.items():
                dest[seam : seam + SEAM, columns[0] : columns[1]] = value

        return put, finish

    def assemble(dest, v, pieces):
        blocks, strip_refs = pieces[:3], pieces[3:]
        lane = lax.broadcasted_iota(jnp.int32, (si, LANES), 1)
        put, finish = joiner(dest)
        dest[:, :LANES] = jnp.zeros((sw, LANES), BF)
        last = si - SEAM
        for b in range(3):
            base = b * span_x * pitch
            for x in range(span_x):
                at = base + SEAM + x * pitch
                rows = slice((v * span_x + x) * span_z, (v * span_x + x + 1) * span_z)
                dest[at : at + span_z, begin : begin + line] = blocks[b][rows, :]
            first = strip_at[v]
            if v == 0:
                ys = strip_refs[b][first : first + si, :].astype(F32)
                low = jnp.where(lane >= 2 * chan, ys, 0.0).astype(BF)
                high = jnp.where(lane < 2 * chan, ys, 0.0).astype(BF)
                first += si
            else:
                low = strip_refs[b][first : first + si, :]
                high = strip_refs[b][first + si : first + 2 * si, :]
                first += 2 * si
            for columns, value in (((LANES, begin), low), ((begin + line, wide), high)):
                dest[base + SEAM : base + last, columns[0] : columns[1]] = value[SEAM:last]
                put(base, columns, value[:SEAM])
                put(base + last, columns, value[last:])
            for t in range(tiles):
                at = first + t * packs
                columns = (begin + LANES * t, begin + LANES * (t + 1))
                shared = strip_refs[b][at : at + SEAM, :].astype(F32)
                row = lax.broadcasted_iota(jnp.int32, shared.shape, 0)
                for x in range(span_x + 1):
                    if x == 0:
                        value = jnp.where(row >= SEAM - 4, shared, 0.0).astype(BF)
                    elif x == span_x:
                        value = jnp.where(row < 4, shared, 0.0).astype(BF)
                    else:
                        value = strip_refs[b][at + x * SEAM : at + (x + 1) * SEAM, :]
                    seam = base + x * pitch
                    if 0 < x < span_x:
                        dest[seam : seam + SEAM, columns[0] : columns[1]] = value
                    else:
                        put(seam, columns, value)
        finish()

    def below(frame, band, group):
        now, later = windows(frame, group)
        zeros = jnp.zeros((si - (later.shape[0] - pitch), 2 * LANES), BF)
        lhs = jnp.concatenate([now, jnp.concatenate([later[pitch:], zeros], axis=0)], axis=1)
        return spread_dz(jnp.dot(lhs, band[0 : 4 * LANES, :], preferred_element_type=F32))

    def above(frame, band, group):
        now, later = windows(frame, group)
        zeros = jnp.zeros((pitch, 2 * LANES), BF)
        lhs = jnp.concatenate([jnp.concatenate([zeros, later[: si - pitch]], axis=0), now], axis=1)
        return spread_dz(jnp.dot(lhs, band[2 * LANES :, :], preferred_element_type=F32))

    def windows(frame, group):
        value = frame[:, lane_at(group)]
        if (group + 1) * LANES < mid:
            more = frame[:, lane_at(group + 1)]
        else:
            more = jnp.zeros(value.shape, BF)
        value = jnp.concatenate([value, more], axis=1)
        return value, value

    def spread_dz(out):
        size = out.shape[0]
        return (
            pltpu.roll(out[:, :LANES], 1, 0)
            + out[:, LANES : 2 * LANES]
            + pltpu.roll(out[:, 2 * LANES :], size - 1, 0)
        )

    def halves(first, second):
        cut = si - SEAM // 2
        return jnp.concatenate([first[:cut], second[SEAM // 2 :]], axis=0)


    def stat_shape(rows):
        return shape((world, rows, LANES), F32)

    def send(ref, sums, *parts):
        ref[:, 0:1, :] = jnp.broadcast_to(packed(sums, chan)[None], (world, 1, LANES))
        for i, part in enumerate(parts):
            for d in range(world):
                ref[d, 1 + i * hold : 1 + (i + 1) * hold, :] = part[d * hold : (d + 1) * hold, :]

    def moments(st_ref, row):
        mean = gathered(st_ref, row, chan) / voxels
        var = gathered(st_ref, row + 1, chan) / voxels - mean * mean
        return mean, lax.rsqrt(var + EPSILON)

    def add_up(sums, value, other):
        return (
            sums[0] + jnp.sum(value, axis=0, keepdims=True),
            sums[1] + jnp.sum(value * other, axis=0, keepdims=True),
        )

    def conv_one_of(first, groups, base, band, dest, c_ref, own_ref, to=None):
        fill_own(own_ref)
        band = band.fill(2)

        def step(g, sums):
            out = band_conv(dest, band, g + first, po, pitch)
            c_ref[:, lane_at(g)] = out
            if to is not None:
                column(c_ref, to[0], to[1], g).start()
            mine = jnp.where(own(own_ref, g, base), out[pitch : pitch + si], 0.0)
            return add_up(sums, mine, mine)

        return lax.fori_loop(0, groups, step, (zero(), zero()), unroll=True)

    def zero():
        return jnp.zeros((1, LANES), F32)

    def first_conv_b(w_ref, *refs):
        pieces, rest = refs[:6], refs[6:]
        c_ref, x_out, a_out, st_ref, m_ref, x_ref, a_ref, own_ref, *band, sems = rest
        band = Band(*band, w_ref, 0)
        copies = [
            pltpu.make_async_copy(a_ref, a_out, sems.at[0]),
            pltpu.make_async_copy(x_ref, x_out, sems.at[1]),
        ]
        assemble(a_ref, 0, pieces)
        copies[0].start()
        assemble(x_ref, 1, pieces)
        copies[1].start()
        send(st_ref, conv_one_of(0, b_groups, base_b, band, x_ref, c_ref, own_ref))
        plain_taps(x_ref, m_ref)
        for copy in copies:
            copy.wait()

    def first_conv_a(w_ref, after, x_far, c_out, st_ref, x_ref, c_ref, own_ref, band, part, wait, sem, sems):
        del after
        band = Band(band, part, wait, w_ref, 0)
        copy = pltpu.make_async_copy(x_far, x_ref, sem)
        copy.start()
        st_ref[...] = jnp.zeros(st_ref.shape, F32)
        copy.wait()
        to = (c_out, sems)
        rows = conv_one_of(1, outer_groups, base_a, band, x_ref, c_ref, own_ref, to)
        for k in range(2):
            st_ref[k : k + 1, :] = rows[k]
        columns(c_ref, c_out, sems)

    def column(source, dest, sems, g):
        return pltpu.make_async_copy(source.at[:, lane_at(g)], dest.at[:, lane_at(g)], sems.at[g])

    def columns(source, dest, sems):
        def wait(g, carry):
            column(source, dest, sems, g).wait()
            return carry

        lax.fori_loop(0, outer_groups, wait, 0, unroll=True)

    def conv_two_of(bound, c_ref, st_in, k, p_ref, h_ref, c2_ref, own_ref, in_ref, band, shifts, after=None):
        groups, base, out_groups, out_base, offset = shifts
        fill_own(own_ref)
        fill_inside(bound, in_ref, (bound[0], bound[1]))
        mean, rstd = moments(st_in, k)
        gain, bias = p_ref[0:1, :], p_ref[1:2, :]

        def act(g, carry):
            at = lane_at(g)
            z = gain * ((c_ref[:, at] - mean) * rstd) + bias
            h = jnp.where(inside(bound, in_ref, g, base), z * sigmoid(z), 0.0)
            h_ref[:, at] = h.astype(BF)
            return carry

        lax.fori_loop(0, groups, act, 0, unroll=True)
        if after is not None:
            after.start()
        band = band.fill(offset)

        def step(g, sums):
            out = band_conv(h_ref, band, g, pi, pitch)
            c2_ref[:, lane_at(g)] = out
            mine = jnp.where(own(own_ref, g, out_base), out, 0.0)
            return add_up(sums, mine, mine)

        return lax.fori_loop(0, out_groups, step, (zero(), zero()), unroll=True)

    def second_conv_b(bound, c_ref, w_ref, st_in, p_ref, more, m_ref, h_out, c2_ref, st_ref, token_ref, h_ref, own_ref, in_ref, band, part, wait, sem):
        band = Band(band, part, wait, w_ref, 1)
        token_ref[...] = jnp.zeros(token_ref.shape, F32)
        copy = pltpu.make_async_copy(h_ref, h_out, sem)
        shifts = (b_groups, base_b, outer_groups, base_two, 2)
        rows = conv_two_of(bound, c_ref, st_in, 0, p_ref, h_ref, c2_ref, own_ref, in_ref, band, shifts, copy)
        send(st_ref, list(rows) + [more[0:1, :], more[1:2, :]])
        for d in range(world):
            for k in range(2):
                row = min(d * hold // chan + k, m_ref.shape[0] - 1)
                st_ref[d, 1 + k : 2 + k, :] = m_ref[row : row + 1, :]
        copy.wait()

    def second_conv_a(bound, c_far, w_ref, st_in, p_ref, after, c2_ref, st_ref, c_ref, h_ref, own_ref, in_ref, band, part, wait, sem):
        del after
        band = Band(band, part, wait, w_ref, 1)
        shifts = (outer_groups, base_a, inner_groups, 0, 0)
        copy = pltpu.make_async_copy(c_far, c_ref, sem)
        copy.start()
        copy.wait()
        rows = conv_two_of(bound, c_ref, st_in, 2, p_ref, h_ref, c2_ref, own_ref, in_ref, band, shifts)
        st_ref[...] = jnp.concatenate(list(rows) + [jnp.zeros((6, LANES), F32)], axis=0)

    def early_taps(c_ref, st_in, x_far, after, t_ref, x_ref, acc, own_ref, sem):
        del after
        copy = pltpu.make_async_copy(x_far, x_ref, sem)
        copy.start()
        fill_own(own_ref)
        mean, rstd = moments(st_in, 0)
        copy.wait()
        groups = []
        for g in range(outer_groups):
            xhat = (c_ref[pl.ds(pitch, si), lane_at(g + 1)] - mean) * rstd
            groups.append(jnp.where(own(own_ref, g, base_one), xhat, 0.0))
        acc[...] = tap_products(groups, x_ref, pitch, 1, pitch)
        t_ref[...] = jnp.zeros(t_ref.shape, F32)
        fold_taps(acc, t_ref, 0, chan, 2)

    def plain_taps(x_ref, m_ref):
        m_ref[...] = jnp.zeros(m_ref.shape, F32)
        row = lax.broadcasted_iota(jnp.int32, (8, si), 0)
        at = lax.broadcasted_iota(jnp.int32, (8, si), 1)
        pick = jnp.zeros((8, si), F32)
        for x in range(span_x):
            for t in range(3):
                low = SEAM + x * pitch + t - 1
                pick = jnp.where((row == t) & (at >= low) & (at < low + span_z), 1.0, pick)
        pick = pick.astype(BF)
        for d in range(3):
            cols = jnp.dot(
                pick, x_ref[pl.ds((1 + d) * pitch, si), :], preferred_element_type=F32
            )
            for y in range(3):
                low = begin + (y - 1) * chan
                own_cols = cols[:, low : low + line]
                total = sum(own_cols[:, k * LANES : (k + 1) * LANES] for k in range(tiles))
                total = fold_lanes(total, chan)
                for t in range(3):
                    group, place = divmod((d * 3 + y) * 3 + t, per)
                    m_ref[group : group + 1, place * chan : (place + 1) * chan] = total[
                        t : t + 1, place * chan : (place + 1) * chan
                    ]

    def slope_two(c_ref, moment, p_ref, go_ref, at):
        mean, rstd = moment
        xhat = (c_ref[:, at] - mean) * rstd
        z = p_ref[2:3, :] * xhat + p_ref[3:4, :]
        s = sigmoid(z)
        d = go_ref[:, at].astype(F32) * (s * (1.0 + z * (1.0 - s)))
        return d, xhat

    def second_slope(c_ref, st_in, p_ref, go_ref, t_ref, st_ref, token_ref, own_ref):
        token_ref[...] = jnp.zeros(token_ref.shape, F32)
        fill_own(own_ref)
        moment = moments(st_in, 0)

        def step(g, sums):
            d, xhat = slope_two(c_ref, moment, p_ref, go_ref, lane_at(g))
            return add_up(sums, jnp.where(own(own_ref, g, base_two), d, 0.0), xhat)

        rows = lax.fori_loop(0, outer_groups, step, (zero(), zero()), unroll=True)
        send(st_ref, rows, t_ref)

    def second_delta(bound, c_ref, st_in, p_ref, go_ref, sums_in, after, d_ref, in_ref):
        del after
        fill_inside(bound, in_ref, (0, span_x))
        moment = moments(st_in, 0)
        scale = p_ref[2:3, :] * moment[1]
        sum_d, sum_x = gathered(sums_in, 0, chan) / voxels, gathered(sums_in, 1, chan) / voxels

        def step(g, carry):
            at = lane_at(g)
            d, xhat = slope_two(c_ref, moment, p_ref, go_ref, at)
            out = scale * (d - sum_d - xhat * sum_x)
            d_ref[:, at] = jnp.where(inside(bound, in_ref, g, base_two), out, 0.0).astype(BF)
            return carry

        lax.fori_loop(0, outer_groups, step, 0, unroll=True)

    def second_taps(d_ref, h_far, gw_ref, h_ref, acc, own_ref, sem):
        copy = pltpu.make_async_copy(h_far, h_ref, sem)
        copy.start()
        fill_own(own_ref)
        gw_ref[...] = jnp.zeros(gw_ref.shape, F32)
        copy.wait()
        groups = [
            jnp.where(own(own_ref, g, base_two), d_ref[:, lane_at(g)].astype(F32), 0.0)
            for g in range(outer_groups)
        ]
        acc[...] = tap_products(groups, h_ref, 0, 0, pitch)
        fold_taps(acc, gw_ref, 0, chan, 2)

    one = pitch + SEAM

    def own_upstream(w_ref, d_ref, after, e_ref, low_ref, high_ref, band, part, wait):
        del after
        band = Band(band, part, wait, w_ref, 2).fill(0)
        for g in range(outer_groups):
            e = halves(above(d_ref, band, g), below(d_ref, band, g))
            e_ref[:, lane_at(g)] = e[pitch : pitch + si]
            low_ref[:, lane_at(g)] = e[:one]
            high_ref[:, lane_at(g)] = e[so - one :]

    def slope_one(c_rows, moment, p_ref):
        mean, rstd = moment
        xhat = (c_rows - mean) * rstd
        z = p_ref[0:1, :] * xhat + p_ref[1:2, :]
        s = sigmoid(z)
        return s * (1.0 + z * (1.0 - s)), xhat

    def first_slope(w_ref, c_ref, st_in, p_ref, more, x_far, gw_two, low_ref, high_ref, e_ref, *rest):
        d1_out, st_ref, token_ref, own_ref, *band, x_ref, acc, gw_ref, d1_ref, wait, sems = rest
        token_ref[...] = jnp.zeros(token_ref.shape, F32)
        band = Band(*band, w_ref, 2)
        copy = pltpu.make_async_copy(x_far, x_ref, wait)
        copy.start()
        fill_own(own_ref)
        band = band.fill(0)
        moment = moments(st_in, 0)
        gw_ref[...] = jnp.zeros(gw_ref.shape, F32)
        groups, sums = [], (zero(), zero())
        cut = one - SEAM // 2
        for g in range(outer_groups):
            slope, xhat = slope_one(c_ref[pitch : pitch + si, lane_at(g + 1)], moment, p_ref)
            low = windows(low_ref, g)[0][si - one :]
            high = windows(high_ref, g)[0][:one]
            low = spread_dz(jnp.dot(low, band[: 2 * LANES, :], preferred_element_type=F32))
            high = spread_dz(jnp.dot(high, band[4 * LANES :, :], preferred_element_type=F32))
            more_e = [low[:cut], high[SEAM // 2 :]]
            if span_x > 2:
                more_e.insert(1, jnp.zeros((si - 2 * cut, LANES), F32))
            d = (e_ref[:, lane_at(g)] + jnp.concatenate(more_e, axis=0)) * slope
            d1_ref[:, lane_at(g)] = d
            column(d1_ref, d1_out, sems, g).start()
            mine = jnp.where(own(own_ref, g, base_one), d, 0.0)
            groups.append(mine)
            sums = add_up(sums, mine, xhat)
        copy.wait()
        acc[...] = tap_products(groups, x_ref, pitch, 1, pitch)
        fold_taps(acc, gw_ref, 0, chan, 2)
        send(st_ref, list(sums) + [more[0:1, :], more[1:2, :]], gw_ref, gw_two)
        columns(d1_ref, d1_out, sems)

    def outer_slope(w_ref, c_ref, st_in, p_ref, low_ref, high_ref, low_e, high_e, after, low_out, high_out, band, part, wait, e_ref, waits):
        del after
        band = Band(band, part, wait, w_ref, 2)
        copies = [
            pltpu.make_async_copy(low_e, e_ref.at[0], waits.at[0]),
            pltpu.make_async_copy(high_e, e_ref.at[1], waits.at[1]),
        ]
        for copy in copies:
            copy.start()
        band = band.fill(0)
        moment = moments(st_in, 0)
        for copy in copies:
            copy.wait()
        for g in range(outer_groups):
            for side, (ref, out, row, weight) in enumerate(
                ((low_ref, low_out, 0, 0), (high_ref, high_out, so - one, 2 * LANES))
            ):
                frame = windows(ref, g)[0]
                if side == 0:
                    frame = frame[si - one - pitch :]
                else:
                    frame = frame[: one + pitch]
                lhs = jnp.concatenate([frame[:one], frame[pitch:]], axis=1)
                e = spread_dz(
                    jnp.dot(lhs, band[weight : weight + 4 * LANES, :], preferred_element_type=F32)
                )
                slope, _ = slope_one(c_ref[row : row + one, lane_at(g + 1)], moment, p_ref)
                out[:, lane_at(g)] = (e_ref[side, :, lane_at(g)] + e) * slope

    def first_delta(bound, s_far, c_ref, st_in, p_ref, sums_in, w_ref, after, low_far, high_far, dx_ref, s_ref, d_ref, o_ref, in_ref, band, part, wait, sems):
        del after
        band = Band(band, part, wait, w_ref, 3)
        half = SEAM // 2
        first, second = pitch + half, so - pitch - half
        copies = [
            pltpu.make_async_copy(
                low_far.at[pl.ds(0, first)], s_ref.at[pl.ds(0, first)], sems.at[0]
            ),
            pltpu.make_async_copy(
                s_far.at[pl.ds(half, second - first)],
                s_ref.at[pl.ds(first, second - first)],
                sems.at[1],
            ),
            pltpu.make_async_copy(
                high_far.at[pl.ds(half, so - second)], s_ref.at[pl.ds(second, so - second)], sems.at[2]
            ),
        ]
        for copy in copies:
            copy.start()
        fill_inside(bound, in_ref, (bound[0], bound[1]))
        band = band.fill(0)
        for copy in copies:
            copy.wait()
        sum_d, sum_x = gathered(sums_in, 0, chan) / voxels, gathered(sums_in, 1, chan) / voxels
        mean, rstd = moments(st_in, 0)
        scale = p_ref[0:1, :] * rstd

        def step(g, carry):
            at = lane_at(g)
            xhat = (c_ref[:, lane_at(g + 1)] - mean) * rstd
            out = scale * (s_ref[:, at] - sum_d - xhat * sum_x)
            d_ref[:, at] = jnp.where(inside(bound, in_ref, g, base_one), out, 0.0).astype(BF)
            return carry

        lax.fori_loop(0, outer_groups, step, 0, unroll=True)

        def conv(g, carry):
            o_ref[:, lane_at(g)] = band_conv(d_ref, band, g, pi, pitch).astype(BF)
            return carry

        lax.fori_loop(0, inner_groups, conv, 0, unroll=True)
        order = order_matrix(chan, span_y, 0, line)
        for x in range(span_x):
            at = SEAM + x * pitch
            dx_ref[:, x] = native(o_ref[at : at + span_z, :], order)

    def mix(bound, st_in, p_ref, plain_ref, early_ref, late_ref, out_ref, token_ref):
        token_ref[...] = jnp.zeros(token_ref.shape, F32)
        sum_d, sum_x = gathered(late_ref, 0, chan) / voxels, gathered(late_ref, 1, chan) / voxels
        scale = p_ref[0:1, :] * moments(st_in, 0)[1]
        row = lax.broadcasted_iota(jnp.int32, (hold, LANES), 0) + bound[8] * hold
        lane = lax.broadcasted_iota(jnp.int32, (hold, LANES), 1)

        def of_row(value):
            return jnp.sum(jnp.where(lane == row % chan, value, 0.0), axis=1, keepdims=True)

        def part(ref, i):
            return jnp.sum(ref[:, 1 + i * hold : 1 + (i + 1) * hold, :], axis=0)

        plain = jnp.sum(plain_ref[:, 1:3, :], axis=0)
        plain = jnp.where(row // chan == bound[8] * hold // chan, plain[0:1, :], plain[1:2, :])
        one = of_row(scale) * (
            part(late_ref, 0) - of_row(sum_d) * plain - of_row(sum_x) * part(early_ref, 0)
        )
        out = jnp.concatenate([one, part(late_ref, 1)], axis=0) * factor
        spare = out_ref.shape[1] - out.shape[0]
        if spare:
            out = jnp.concatenate([out, jnp.zeros((spare, LANES), F32)], axis=0)
        out_ref[...] = jnp.broadcast_to(out.astype(BF)[None], out_ref.shape)

    def last(got_ref, one_ref, two_ref, flat):
        for i, out in enumerate((one_ref, two_ref)):
            for d in range(world):
                flat[d * hold : (d + 1) * hold, :] = got_ref[d, i * hold : (i + 1) * hold, :].astype(F32)
            for at in range(27):
                row, lane = divmod(at, per)
                block = flat[row * chan : (row + 1) * chan, lane * chan : (lane + 1) * chan]
                out[at // 9, at // 3 % 3, at % 3] = block

    def out_a(c_ref, st_in, st_two, p_ref, after, y_ref, n_ref, h_ref):
        del after
        for row, (ref, at) in enumerate(((st_in, 1), (st_in, 0), (st_two, 1), (st_two, 0))):
            n_ref[row : row + 1, :] = factor * gathered(ref, at, chan)[:, :chan]
        order = order_matrix(chan, span_y, 0, line)
        mean, rstd = moments(st_in, 2)

        def act(g, carry):
            at = lane_at(g)
            z = p_ref[2:3, :] * ((c_ref[:, at] - mean) * rstd) + p_ref[3:4, :]
            h_ref[:, at] = (z * sigmoid(z)).astype(BF)
            return carry

        lax.fori_loop(0, inner_groups, act, 0, unroll=True)
        for x in range(span_x):
            at = SEAM + x * pitch
            y_ref[:, x] = native(h_ref[at : at + span_z, :], order)


    vols, cot_block, tiles_z = kernel_call(
        turn_in,
        [
            shape((2 * flat_rows, line), BF),
            shape((flat_rows, mid), BF),
            shape((edges, 3 * span_x * SEAM, mid), BF),
        ],
        [bounds, x_a, x_b, grad_out],
        scratch=[
            pltpu.VMEM((3 * span_x, chan, span_y, span_z), BF),
            pltpu.SemaphoreType.DMA((3 * span_x,)),
        ],
        smem=1,
        far=(1, 2, 3),
    )
    pieces, cot = halo(vols, cot_block, tiles_z, params)
    wide_scratch = pltpu.VMEM((sw, wide), BF)
    one_copy = pltpu.SemaphoreType.DMA
    mid_scratch = pltpu.VMEM((so, mid), F32)
    group_copies = pltpu.SemaphoreType.DMA((outer_groups,))
    acc_scratch = pltpu.VMEM((3 * LANES, 6 * LANES), F32)
    c1_b, pad_b, pad_a, stats, plain = kernel_call(
        first_conv_b,
        [shape((so, mid_b), F32)] + [shape((sw, wide), BF)] * 2 + [stat_shape(1), token_shape],
        [weights] + pieces,
        scratch=[
            wide_scratch,
            wide_scratch,
            own_scratch,
            *band_scratch,
            pltpu.SemaphoreType.DMA((2,)),
        ],
        far=(0,),
        far_out=(1, 2),
        home=(3,),
        work=1 << 30,
    )
    stats_one = exchange(stats)
    c1_a, local_a = kernel_call(
        first_conv_a,
        [shape((so, mid), F32), shape((8, LANES), F32)],
        [weights, plain, pad_a],
        scratch=[wide_scratch, mid_scratch, own_scratch, *band_scratch, one_copy, group_copies],
        far=(0, 2),
        far_out=(0,),
        work=1 << 32,
    )
    hidden_b, c2_b, stats, token = kernel_call(
        second_conv_b,
        [shape((so, mid_b), BF), shape((si, mid), F32), stat_shape(3), token_shape],
        [bounds, c1_b, weights, stats_one, params, local_a, plain],
        scratch=[pltpu.VMEM((so, mid_b), BF), own_scratch, in_scratch, *band_scratch, one_copy],
        smem=1,
        far_out=(0,),
        home=(2,),
        far=(2,),
        work=1 << 30,
    )
    stats_two = exchange(stats)
    (taps_early,) = kernel_call(
        early_taps,
        [shape((world * hold, LANES), F32)],
        [c1_b, stats_one, pad_b, token],
        scratch=[wide_scratch, acc_scratch, own_scratch, one_copy],
        far=(2,),
        work=1 << 32,
    )
    stats, token = kernel_call(
        second_slope,
        [stat_shape(1 + hold), token_shape],
        [c2_b, stats_two, params, cot, taps_early],
        scratch=[own_scratch],
        home=(0,),
        work=1 << 27,
    )
    sums_two = exchange(stats)
    c2_a, local_a = kernel_call(
        second_conv_a,
        [shape((si, line), F32), shape((8, LANES), F32)],
        [bounds, c1_a, weights, stats_two, params, token],
        scratch=[mid_scratch, pltpu.VMEM((so, mid), BF), own_scratch, in_scratch, *band_scratch, one_copy],
        smem=1,
        far=(1, 2),
        home=(0,),
        work=1 << 32,
    )
    (delta_two,) = kernel_call(
        second_delta,
        [shape((si, mid), BF)],
        [bounds, c2_b, stats_two, params, cot, sums_two, local_a],
        scratch=[pltpu.VMEM((si, LANES), F32)],
        smem=1,
        work=1 << 27,
    )
    (taps_two,) = kernel_call(
        second_taps,
        [shape((world * hold, LANES), F32)],
        [delta_two, hidden_b],
        scratch=[pltpu.VMEM((so, mid_b), BF), acc_scratch, own_scratch, one_copy],
        far=(1,),
        work=1 << 32,
    )
    forward_x, backward_x = neighbours("gx")
    frames = [
        lax.ppermute(delta_two, "gx", forward_x),
        lax.ppermute(delta_two, "gx", backward_x),
    ]
    side_shape = shape((one, mid), F32)
    upstream, low_part, high_part = kernel_call(
        own_upstream,
        [shape((si, mid), F32), side_shape, side_shape],
        [weights, delta_two, taps_two],
        scratch=list(band_scratch),
        far=(0,),
        home=(1, 2),
        work=1 << 32,
    )
    frame_scratch = pltpu.VMEM((si, mid), F32)
    slope, stats, token = kernel_call(
        first_slope,
        [shape((si, mid), F32), stat_shape(1 + 2 * hold), token_shape],
        [weights, c1_b, stats_one, params, local_a, pad_b, taps_two] + frames + [upstream],
        scratch=[
            own_scratch,
            *band_scratch,
            wide_scratch,
            acc_scratch,
            pltpu.VMEM((world * hold, LANES), F32),
            frame_scratch,
            one_copy,
            group_copies,
        ],
        far=(0, 5),
        far_out=(0,),
        home=(1,),
        work=1 << 30,
    )
    sums_one = exchange(stats)
    side_low, side_high = kernel_call(
        outer_slope,
        [side_shape, side_shape],
        [weights, c1_b, stats_one, params] + frames + [low_part, high_part, token],
        scratch=[
            *band_scratch,
            pltpu.VMEM((2, one, mid), F32),
            pltpu.SemaphoreType.DMA((2,)),
        ],
        far=(0, 6, 7),
        home=(0, 1),
        work=1 << 32,
    )
    whole, token = kernel_call(
        mix,
        [shape((world, -(-2 * hold // 8) * 8, LANES), BF), token_shape],
        [bounds, stats_one, params, stats_two, sums_two, sums_one],
        smem=1,
    )
    whole = exchange(whole)
    (dx_b,) = kernel_call(
        first_delta,
        [shape(x_a.shape, BF)],
        [bounds, slope, c1_b, stats_one, params, sums_one, weights, token, side_low, side_high],
        scratch=[
            mid_scratch,
            pltpu.VMEM((so, mid), BF),
            pltpu.VMEM((si, line), BF),
            in_scratch,
            *band_scratch,
            pltpu.SemaphoreType.DMA((3,)),
        ],
        smem=1,
        far=(1, 6, 8, 9),
        work=1 << 31,
    )
    y_a, grad_norm = kernel_call(
        out_a,
        [shape(x_a.shape, BF), shape((4, chan), F32)],
        [c2_a, sums_one, sums_two, params, token],
        scratch=[pltpu.VMEM((si, line), BF)],
        work=1 << 31,
    )
    weight_shape = shape((3, 3, 3, chan, chan), F32)
    grad_one, grad_two = kernel_call(
        last,
        [weight_shape, weight_shape],
        [whole],
        scratch=[pltpu.VMEM((world * hold, LANES), F32)],
    )
    return (y_a, dx_b, grad_one, grad_two, grad_norm)


def solution(mesh):
    block = P(None, "gx", "gy", "gz")
    placed = (block, block, P(), P(), P(), P(), P(), P(), block)

    return jax.shard_map(
        body,
        mesh=mesh,
        in_specs=placed,
        out_specs=(block, block, P(), P(), P()),
        check_vma=False,
    )
```
